128 devices in a mesh: gx: 16 (over z, y), gy: 8 (over x, core).
Axes of the slice: x: 4, y: 4, z: 4, core: 2. Of those that a mesh axis runs over, the one named last changes fastest.
Arguments:
- velocity_u: float32 [4, 2560, 2048], P(None, 'gy', 'gx'), may hold values from -6 to 6
- velocity_v: float32 [4, 2560, 2048], P(None, 'gy', 'gx'), may hold values from -6 to 6
- tracer: float32 [4, 2560, 2048], P(None, 'gy', 'gx'), may hold values from -6 to 6
- pressure_old: float32 [2560, 2048], P('gy', 'gx'), may hold values from -6 to 6
- depth: float32 [2560, 2048], P('gy', 'gx'), may hold values from 0.5 to 2
- helm: float32 [2560, 2048], P('gy', 'gx'), may hold values from 0.05 to 0.5
- land_mask: int32 [2560, 2048], P('gy', 'gx'), may hold values from 0 to 1, as said below
- clinic_map: int32 [64, 16], replicated, may hold values from 0 to 1, as said below
- tropic_map: int32 [64, 16], replicated, may hold values from -1 to 95, as said below
Outputs:
- velocity_u_new: float32 [4, 2560, 2048], P(None, 'gy', 'gx')
- velocity_v_new: float32 [4, 2560, 2048], P(None, 'gy', 'gx')
- tracer_new: float32 [4, 2560, 2048], P(None, 'gy', 'gx')
- pressure: float32 [2560, 2048], P('gy', 'gx')
The draws below stay inside these ranges and needn't reach their ends.
Inputs may be any that keep to these rules, and one draw needn't show every extreme that they name: `land_mask`: rows 0 and 2559 are land; every column of a block whose tropic_map entry is -1 is land; every other block has an ocean column. `clinic_map`: 1 exactly on the blocks whose tropic_map entry is not -1. `tropic_map`: A quarter of the blocks of every device's clinic domain are -1. Another value t places the block in slot t % 6 of the device with gx index t // 6 and the gy index of the device that holds the block's rows; no slot is named twice. The blocks of one device's clinic domain place at most 1 block on any one device, and this bound is reached; every device receives at most 6 blocks, and this bound is reached.
All inputs are finite; a program needn't handle non-finite values.
Results may differ from the reference program's by a relative error of at most 0.00026.
Values sent between devices are 32-bit elements; how exact they have to be, the bound alone decides.
A program may use at most 64 MiB of HBM per device.

```python
import math
import jax
import jax.numpy as jnp

KZ = 4
BX = 128
BY = 40
ITERS = 4
NX = 2048
NY = 2560
BPX = 1
BPY = 8
NSUB = 8
KEEP = 6
CAP = 1
NBX = 16
NBY = 64


def block_plan(key):
    base = jax.random.fold_in(key, 4242)
    key_order = jax.random.fold_in(base, 1)
    key_shift = jax.random.fold_in(base, 2)
    key_slots = jax.random.fold_in(base, 3)
    bands = NBY // BPY
    columns = NBX // BPX
    local = jnp.arange(NSUB)
    scores = jax.random.randint(key_order, (bands, columns, NSUB), 0, 1 << 20) * NSUB + local
    order = jnp.argsort(scores, axis=-1)
    ranking = jnp.argsort(order, axis=-1)
    kept = ranking < KEEP
    offset = ranking // CAP
    within = ranking % CAP
    shift = jax.random.randint(key_shift, (bands, 1, 1), 0, columns)
    source = jnp.arange(columns).reshape(1, columns, 1)
    target = (source + shift + offset) % columns
    slot = jnp.where(kept, offset * CAP + within, 0)
    slot_scores = jax.random.randint(key_slots, (bands, columns, KEEP), 0, 1 << 20) * KEEP + jnp.arange(KEEP)
    shuffle = jnp.argsort(slot_scores, axis=-1)
    band_index = jnp.broadcast_to(jnp.arange(bands).reshape(bands, 1, 1), target.shape)
    placed = shuffle[band_index, target, slot]
    value = jnp.where(kept, target * KEEP + placed, -1)
    return value.reshape(bands, columns, BPY, BPX).transpose(0, 2, 1, 3).reshape(NBY, NBX).astype(jnp.int32)


def draw_tropic_map(key, part):
    return block_plan(key)


def draw_clinic_map(key, part):
    return (block_plan(key) >= 0).astype(jnp.int32)


def draw_land_mask(key, part):
    plan = block_plan(key)
    kept = jnp.repeat(jnp.repeat(plan >= 0, BY, axis=0), BX, axis=1)
    landed = jax.random.randint(jax.random.fold_in(key, 99), (NY, NX), 0, 100) < 15
    rows = jnp.arange(NY).reshape(NY, 1)
    cols = jnp.arange(NX).reshape(1, NX)
    centre = (rows % BY == BY // 2) & (cols % BX == BX // 2)
    ocean = kept & (jnp.logical_not(landed) | centre)
    border = (rows == 0) | (rows == NY - 1)
    ocean = ocean & jnp.logical_not(border)
    return ocean.astype(jnp.int32)


def block_levels(own_key, extent, shards, least, high):
    factor_of, own = 1.0, jax.random.fold_in(own_key, 6)
    for dim, shards_of in shards:
        steps = jnp.exp(jax.random.uniform(jax.random.fold_in(own, dim), (shards_of,), jnp.float32, least / len(shards), high / len(shards)))
        factor_of = factor_of * jnp.repeat(steps, extent[dim] // shards_of).reshape([-1 if axis == dim else 1 for axis in range(len(extent))])
    return factor_of


def centred(own_key, extent, scale, most, pieces=(), held_as=jnp.bfloat16):
    factor_of = block_levels(own_key, extent, pieces, -0.22, 0.18) if pieces else 1.0
    drawn = jax.random.normal(own_key, extent, jnp.float32) * scale * factor_of
    return jnp.minimum(jnp.maximum(drawn, -most), most).astype(held_as)


def setup_inputs(seed: int = 0) -> dict:
    streams_of = jax.random.split(jax.random.key(seed), 10)
    velocity_u = centred(streams_of[0], (KZ, NY, NX), 1.0, 6.0, ((1, 8), (2, 16)), jnp.float32)
    velocity_v = centred(streams_of[1], (KZ, NY, NX), 1.0, 6.0, ((1, 8), (2, 16)), jnp.float32)
    tracer = centred(streams_of[2], (KZ, NY, NX), 1.0, 6.0, ((1, 8), (2, 16)), jnp.float32)
    pressure_old = centred(streams_of[3], (NY, NX), 1.0, 6.0, ((0, 8), (1, 16)), jnp.float32)
    depth = jnp.clip(jnp.exp(math.log(2.0) - 1.3862944 * jax.random.uniform(streams_of[4], (NY, NX), jnp.float32) ** block_levels(streams_of[4], (NY, NX), ((0, 8), (1, 16)), -0.2, 0.2)), 0.5, 2.0)
    helm = jnp.clip(jnp.exp(math.log(0.5) - 2.3025851 * jax.random.uniform(streams_of[5], (NY, NX), jnp.float32) ** block_levels(streams_of[5], (NY, NX), ((0, 8), (1, 16)), -0.2, 0.2)), 0.05, 0.5)
    land_mask = draw_land_mask(jax.random.fold_in(streams_of[9], 71), 0)
    clinic_map = draw_clinic_map(jax.random.fold_in(streams_of[9], 71), 0)
    tropic_map = draw_tropic_map(jax.random.fold_in(streams_of[9], 71), 0)
    return {"velocity_u": velocity_u, "velocity_v": velocity_v, "tracer": tracer, "pressure_old": pressure_old, "depth": depth, "helm": helm, "land_mask": land_mask, "clinic_map": clinic_map, "tropic_map": tropic_map}


def mixing(field):
    diff = field[1:] - field[:-1]
    zero = jnp.zeros_like(field[:1])
    return jnp.concatenate([diff, zero], 0) - jnp.concatenate([zero, diff], 0)


def east(a):
    return jnp.roll(a, -1, axis=-1)


def west(a):
    return jnp.roll(a, 1, axis=-1)


def north(a):
    return jnp.roll(a, -1, axis=-2)


def south(a):
    return jnp.roll(a, 1, axis=-2)


def reference(velocity_u, velocity_v, tracer, pressure_old, depth, helm, land_mask, clinic_map, tropic_map):
    f32 = jnp.float32

    def spread(blocks):
        return jnp.repeat(jnp.repeat(blocks, BY, axis=0), BX, axis=1)

    ocean = land_mask.astype(f32)
    domain = spread((tropic_map >= 0).astype(f32))
    active = spread(clinic_map.astype(f32))
    solve_mask = ocean * domain
    wet = depth * solve_mask
    face_e = jnp.minimum(wet, east(wet))
    face_w = jnp.minimum(wet, west(wet))
    face_n = jnp.minimum(wet, north(wet))
    face_s = jnp.minimum(wet, south(wet))

    def diffuse(a):
        return face_e * (east(a) - a) + face_w * (west(a) - a) + face_n * (north(a) - a) + face_s * (south(a) - a)

    latitude = jnp.arange(NY).astype(f32)
    coriolis = (0.2 + 0.6 * ((latitude + 0.5) / NY)).reshape(NY, 1)
    u_star = velocity_u + 0.2 * (0.5 * mixing(velocity_u) + 0.5 * diffuse(velocity_u) + coriolis * velocity_v)
    v_star = velocity_v + 0.2 * (0.5 * mixing(velocity_v) + 0.5 * diffuse(velocity_v) - coriolis * velocity_u)
    tracer_raw = tracer + 0.2 * (0.5 * mixing(tracer) + 0.5 * diffuse(tracer)
                                 - 0.5 * (velocity_u * (east(tracer) - west(tracer)) + velocity_v * (north(tracer) - south(tracer))))
    thick = ((2 * jnp.arange(KZ) + 1).astype(f32) / (KZ * KZ)).reshape(KZ, 1, 1)
    east_flow = wet * jnp.sum(thick * u_star, 0)
    north_flow = wet * jnp.sum(thick * v_star, 0)
    forcing = solve_mask * (-(east_flow - west(east_flow)) - (north_flow - south(north_flow)))
    diagonal = helm + face_e + face_w + face_n + face_s

    def operate(x):
        return diagonal * x - face_e * east(x) - face_w * west(x) - face_n * north(x) - face_s * south(x)

    solution = solve_mask * pressure_old
    residual = forcing - operate(solution)
    precond = residual / diagonal
    direction = precond
    rz_now = jnp.sum(residual * precond)
    for step in range(ITERS):
        image = operate(direction)
        alpha = rz_now / jnp.sum(direction * image)
        solution = solution + alpha * direction
        residual = residual - alpha * image
        if step + 1 < ITERS:
            precond = residual / diagonal
            rz_next = jnp.sum(residual * precond)
            direction = precond + (rz_next / rz_now) * direction
            rz_now = rz_next
    grad_x = east(solution) - solution
    grad_y = north(solution) - solution
    keep = active * ocean
    u_new = keep * (u_star - 1.0 * grad_x) + (1.0 - active) * velocity_u
    v_new = keep * (v_star - 1.0 * grad_y) + (1.0 - active) * velocity_v
    t_new = keep * tracer_raw + (1.0 - active) * tracer
    return u_new, v_new, t_new, solution
```

```python
import functools

import jax
import jax.numpy as jnp
from jax import lax
from jax.experimental import pallas as pl
from jax.experimental.pallas import tpu as pltpu
from jax.sharding import PartitionSpec as P

MESH = pl.DeviceIdType.MESH
F32 = jnp.float32

LEVELS, ROWS, COLS, BY, NY = 4, 320, 128, 40, 2560
BLOCKS, NBY = ROWS // BY, 64
THICK = [(2 * k + 1) / (LEVELS * LEVELS) for k in range(LEVELS)]

OFF = 16
EXT_ROWS = ROWS + 2 * OFF
LOW, HIGH = OFF - 8, OFF + ROWS + 8
STEP = 48
FIELDS = 7
WET, HELM, X0, UB, UH, VB, VH = range(FIELDS)
PLANES = 3 * LEVELS
NX_DEV, NY_DEV = 16, 8

VMEM_LIMIT = 54 * 1024 * 1024
RED_STAGES = ("all",)


def peers(kind):
    gx, gy = lax.axis_index("gx"), lax.axis_index("gy")
    if kind == "halo":
        return [
            (lax.rem(gx + i, NX_DEV), lax.rem(gy + j, NY_DEV))
            for i in (0, 1, NX_DEV - 1)
            for j in (0, 1, NY_DEV - 1)
            if i or j
        ]
    if kind == "plane":
        base = gx // 4 * 4
        return [
            (base + lax.rem(lax.rem(gx, 4) + i, 4), lax.rem(gy + j, NY_DEV))
            for i in range(4)
            for j in range(NY_DEV)
            if i or j
        ]
    if kind == "z":
        return [(lax.rem(gx + 4 * j, NX_DEV), gy) for j in range(1, 4)]
    return [
        (lax.rem(gx + i, NX_DEV), lax.rem(gy + j, NY_DEV))
        for i in range(NX_DEV)
        for j in range(NY_DEV)
        if i or j
    ]


COUNT = {"all": 127, "plane": 31, "z": 3}


def lanes(rows):
    return lax.broadcasted_iota(jnp.int32, (rows, COLS), 1)


def beside(ref, r, n, both=True):
    lane = lanes(n)
    first, last = lane == 0, lane == COLS - 1
    c0, c1 = ref[0, r : r + n, :], ref[1, r : r + n, :]
    e0, e1 = pltpu.roll(c0, COLS - 1, 1), pltpu.roll(c1, COLS - 1, 1)
    w0, w1 = pltpu.roll(c0, 1, 1), pltpu.roll(c1, 1, 1)
    out = [
        (
            c0,
            jnp.where(last, e1, e0),
            jnp.where(first, w1, w0),
            ref[0, r + 1 : r + 1 + n, :],
            ref[0, r - 1 : r - 1 + n, :],
        )
    ]
    if both:
        out.append(
            (
                c1,
                jnp.where(last, e0, e1),
                jnp.where(first, w0, w1),
                ref[1, r + 1 : r + 1 + n, :],
                ref[1, r - 1 : r - 1 + n, :],
            )
        )
    return out


def west_of(ref, r, n):
    first = lanes(n) == 0
    c0, c1 = ref[0, r : r + n, :], ref[1, r : r + n, :]
    w0, w1 = pltpu.roll(c0, 1, 1), pltpu.roll(c1, 1, 1)
    return (c0, jnp.where(first, w1, w0)), (c1, jnp.where(first, w0, w1))


def eights(x):
    return jnp.sum(x.reshape(x.shape[0] // 8, 8, COLS), axis=0)


def coefficients(sums):
    m = [sums[0], sums[1]]
    for k in range(2, 8):
        m.append(2.0 * sums[k] - m[k % 2])
    g = [[0.5 * (m[i + j] + m[abs(i - j)]) for j in range(5) if i + j < 8] for i in range(4)]

    def image(i, j):
        if j == 0:
            return g[i][1]
        return 0.5 * (g[i][j + 1] + g[i][j - 1])

    a = [[g[i][j] - image(i, j) for j in range(i + 1)] for i in range(4)]
    low = [[None] * 4 for _ in range(4)]
    inv, piv = [], []
    for j in range(4):
        pivot = a[j][j]
        for k in range(j):
            pivot = pivot - low[j][k] * low[j][k] * piv[k]
        good = pivot > 1e-6 * a[j][j]
        piv.append(jnp.where(good, pivot, 0.0))
        inv.append(jnp.where(good, 1.0 / jnp.where(good, pivot, 1.0), 0.0))
        for i in range(j + 1, 4):
            s = a[i][j]
            for k in range(j):
                s = s - low[i][k] * low[j][k] * piv[k]
            low[i][j] = s * inv[j]
    y = []
    for i in range(4):
        s = m[i]
        for k in range(i):
            s = s - low[i][k] * y[k]
        y.append(s)
    c = [None] * 4
    for i in reversed(range(4)):
        s = y[i] * inv[i]
        for k in range(i + 1, 4):
            s = s - low[k][i] * c[k]
        c[i] = s
    return c


def ocean_kernel(
    u_hbm, v_hbm, t_hbm, p_hbm, depth_hbm, helm_hbm, land_hbm, clinic_hbm, tropic_hbm,
    u_out, v_out, t_out, p_out,
    uvt, pold, depth, land, cmap, tmap, act, dom,
    ext, pack, pack_t, got_t, got, corner,
    rim, rim_t, rim_got, rim_m, rim_back, edge, edge_got,
    face, rdiag, gain, diag, flow, basis, part,
    in_sem, send_sem, recv_sem, rsend_sem, rrecv_sem, *red,
):
    gx, gy = lax.axis_index("gx"), lax.axis_index("gy")
    east, west = lax.rem(gx + 1, NX_DEV), lax.rem(gx + NX_DEV - 1, NX_DEV)
    north, south = lax.rem(gy + 1, NY_DEV), lax.rem(gy + NY_DEV - 1, NY_DEV)
    own = pl.ds(OFF, ROWS)

    loads = [
        pltpu.make_async_copy(u_hbm, uvt.at[0:4, 8 : 8 + ROWS, :], in_sem.at[0]),
        pltpu.make_async_copy(v_hbm, uvt.at[4:8, 8 : 8 + ROWS, :], in_sem.at[1]),
        pltpu.make_async_copy(p_hbm, pold, in_sem.at[2]),
        pltpu.make_async_copy(depth_hbm, depth, in_sem.at[3]),
        pltpu.make_async_copy(land_hbm, land, in_sem.at[4]),
        pltpu.make_async_copy(clinic_hbm, cmap, in_sem.at[5]),
        pltpu.make_async_copy(tropic_hbm, tmap, in_sem.at[6]),
        pltpu.make_async_copy(helm_hbm, ext.at[HELM, 0, OFF : OFF + ROWS, :], in_sem.at[7]),
        pltpu.make_async_copy(t_hbm, uvt.at[8:12, 8 : 8 + ROWS, :], in_sem.at[8]),
    ]
    for load in loads:
        load.start()

    barrier = pltpu.get_barrier_semaphore()
    greeted = []
    for kind in RED_STAGES if RED_STAGES == ("all",) else RED_STAGES + ("halo",):
        greeted += peers(kind)
    for peer in greeted:
        pl.semaphore_signal(barrier, inc=1, device_id=peer, device_id_type=MESH)

    pack[ROWS:, :] = jnp.zeros((pack.shape[0] - ROWS, COLS), F32)
    for load in loads[:8]:
        load.wait()

    shape = (NX_DEV, NBY)
    mine = lax.broadcasted_iota(jnp.int32, shape, 0) == gx
    shape = (BLOCKS, NBY)
    wanted = lax.broadcasted_iota(jnp.int32, shape, 1) == lax.broadcasted_iota(jnp.int32, shape, 0) + gy * BLOCKS

    def per_block(flags):
        line = jnp.sum(jnp.where(mine, flags, 0.0), axis=0, keepdims=True)
        column = jnp.sum(jnp.where(wanted, line, 0.0), axis=1, keepdims=True)
        return jnp.broadcast_to(column, (BLOCKS, COLS))

    act[...] = per_block(cmap[...].astype(F32))
    dom[...] = per_block(jnp.where(tmap[...] >= 0, 1.0, 0.0))

    def coriolis(b):
        row = lax.broadcasted_iota(jnp.int32, (BY, COLS), 0) + (gy * ROWS + b * BY)
        return 0.2 + 0.6 * ((row.astype(F32) + 0.5) / NY)

    group = lanes(BY) // 16
    for b in range(BLOCKS):
        r = b * BY
        rows = slice(r, r + BY)
        solve = land[rows, :].astype(F32) * dom[b : b + 1, :]
        wet = depth[rows, :] * solve
        u = [uvt[k, 8 + r : 8 + r + BY, :] for k in range(LEVELS)]
        v = [uvt[LEVELS + k, 8 + r : 8 + r + BY, :] for k in range(LEVELS)]
        u_bar = sum(THICK[k] * u[k] for k in range(LEVELS))
        v_bar = sum(THICK[k] * v[k] for k in range(LEVELS))
        cor = 0.2 * coriolis(b)
        mix = 0.1 * (THICK[1] - THICK[0])
        u_hat = u_bar + mix * (u[0] - u[3]) + cor * v_bar
        v_hat = v_bar + mix * (v[0] - v[3]) - cor * u_bar
        fields = [wet, ext[HELM, 0, OFF + r : OFF + r + BY, :], solve * pold[rows, :], u_bar, u_hat, v_bar, v_hat]
        packed = None
        for f, value in enumerate(fields):
            if f != HELM:
                ext[f, 0, OFF + r : OFF + r + BY, :] = value
            moved = pltpu.roll(value, 8 + 16 * f, 1)
            packed = moved if packed is None else jnp.where(group == f, moved, packed)
        pack[rows, :] = packed
    for c in range(3):
        pack_t[:, :, :, 128 * c : 128 * (c + 1)] = pack[128 * c : 128 * (c + 1), :].T.reshape(8, 2, 8, COLS)

    def send(src, dst, k, to):
        copy = pltpu.make_async_remote_copy(
            src_ref=src, dst_ref=dst, send_sem=send_sem.at[k], recv_sem=recv_sem.at[k], device_id=to, device_id_type=MESH
        )
        copy.start()
        return copy

    pl.semaphore_wait(barrier, len(greeted))
    halo = [
        send(pack_t.at[0:7, 0], got_t.at[0:7, 0], 0, (east, gy)),
        send(pack_t.at[0:7, 1], got_t.at[0:7, 1], 1, (west, gy)),
        send(ext.at[:, 0, OFF + ROWS - 8 : OFF + ROWS, :], ext.at[:, 0, LOW:OFF, :], 2, (gx, north)),
        send(ext.at[:, 0, OFF : OFF + 8, :], ext.at[:, 0, OFF + ROWS : HIGH, :], 3, (gx, south)),
        send(pack.at[ROWS - 8 : ROWS, :], corner.at[0], 4, (east, north)),
        send(pack.at[ROWS - 8 : ROWS, :], corner.at[1], 5, (west, north)),
        send(pack.at[0:8, :], corner.at[2], 6, (east, south)),
        send(pack.at[0:8, :], corner.at[3], 7, (west, south)),
    ]

    loads[8].wait()
    pair = lanes(BY) // 2
    for b in range(BLOCKS):
        r = b * BY
        packed = None
        for q in range(PLANES):
            moved = pltpu.roll(uvt[q, 8 + r : 8 + r + BY, :], 2 * q + 1, 1)
            packed = moved if packed is None else jnp.where(pair == q, moved, packed)
        rim[r : r + BY, :] = packed
    rim[ROWS:, :] = jnp.zeros((rim.shape[0] - ROWS, COLS), F32)
    for c in range(3):
        rim_t[:, 128 * c : 128 * (c + 1)] = rim[128 * c : 128 * (c + 1), :].T[: 2 * PLANES, :]
    for q in range(PLANES):
        edge[0, q : q + 1, :] = uvt[q, 8 : 9, :]
        edge[1, q : q + 1, :] = uvt[q, 7 + ROWS : 8 + ROWS, :]
    outer = [
        send(rim_t, rim_got.at[0], 8, (east, gy)),
        send(rim_t, rim_got.at[1], 9, (west, gy)),
        send(edge.at[1], edge_got.at[0], 10, (gx, north)),
        send(edge.at[0], edge_got.at[1], 11, (gx, south)),
    ]

    for copy in halo:
        copy.wait_recv()
    low_half = lax.rem(lanes(8), 16) < 8
    got[0:8, :] = jnp.where(low_half, corner[0], corner[1])
    for c in range(3):
        block = got_t[:, :, :, 128 * c : 128 * (c + 1)].reshape(128, 128).T
        n = min(128, ROWS - 128 * c)
        got[8 + 128 * c : 8 + 128 * c + n, :] = block[:n, :]
    got[8 + ROWS : 16 + ROWS, :] = jnp.where(low_half, corner[2], corner[3])

    chunks = [(r, STEP) for r in range(LOW, HIGH, STEP)]
    lane = lanes(STEP)
    sides = (lane < 8) | (lane >= COLS - 8)
    for r, n in chunks:
        packed = got[r - LOW : r - LOW + n, :]
        for f in range(FIELDS):
            moved = pltpu.roll(packed, COLS - (16 * f + 8), 1)
            ext[f, 1, r : r + n, :] = jnp.where(sides, moved, 1.0 if f == HELM else 0.0)

    for r, n in chunks:
        at = slice(r, r + n)
        for t, (c, e, w, nn, s) in enumerate(beside(ext.at[WET], r, n)):
            four = [jnp.minimum(c, o) for o in (e, w, nn, s)]
            total = ext[HELM, t, at, :] + four[0] + four[1] + four[2] + four[3]
            inverse = 1.0 / total
            rdiag[t, at, :] = inverse
            if t == 0:
                diag[at, :] = total
            for k in range(4):
                face[k, t, at, :] = four[k]
                gain[k, t, at, :] = four[k] * inverse
    for k, (bar, hat) in enumerate(((UB, UH), (VB, VH))):
        for r, n in chunks:
            at = slice(r, r + n)
            for t, (c, *others) in enumerate(beside(ext.at[bar], r, n)):
                spread = sum(face[i, t, at, :] * (o - c) for i, o in enumerate(others))
                flow[k, t, at, :] = ext[WET, t, at, :] * (ext[hat, t, at, :] + 0.1 * spread)

    def image(t, at, others):
        return sum(gain[i, t, at, :] * o for i, o in enumerate(others))

    for r, n in chunks:
        at = slice(r, r + n)
        x = beside(ext.at[X0], r, n)
        for t, (ef, efw) in enumerate(west_of(flow.at[0], r, n)):
            nf, nfs = flow[1, t, at, :], flow[1, t, r - 1 : r - 1 + n, :]
            force = jnp.where(ext[WET, t, at, :] > 0.0, (efw - ef) + (nfs - nf), 0.0)
            c, *others = x[t]
            basis[0, t, at, :] = force * rdiag[t, at, :] + (image(t, at, others) - c)
    for k in range(3):
        for r, n in chunks:
            at = slice(r, r + n)
            for t, (c, *others) in enumerate(beside(basis.at[k], r, n)):
                value = image(t, at, others)
                if k:
                    value = 2.0 * value - basis[k - 1, t, at, :]
                basis[k + 1, t, at, :] = value
    sums = [jnp.zeros((8, COLS), F32) for _ in range(8)]
    for b in range(BLOCKS):
        r = OFF + b * BY
        at = slice(r, r + BY)
        ((c, *others),) = beside(basis.at[3], r, BY, both=False)
        t4 = 2.0 * image(0, at, others) - basis[2, 0, at, :]
        vectors = [basis[k, 0, at, :] for k in range(3)] + [c, t4]
        for k in range(4):
            weighted = diag[at, :] * vectors[k]
            sums[2 * k] = sums[2 * k] + eights(weighted * vectors[k])
            sums[2 * k + 1] = sums[2 * k + 1] + eights(weighted * vectors[k + 1])

    rows8 = lax.broadcasted_iota(jnp.int32, (8, COLS), 0)
    mat = jnp.zeros((8, COLS), F32)
    for k in range(8):
        mat = jnp.where(rows8 == k, jnp.sum(sums[k], axis=0, keepdims=True), mat)
    total = jnp.broadcast_to(jnp.sum(mat, axis=1, keepdims=True), (8, COLS))
    row = jnp.sum(jnp.where(lanes(8) == rows8, total, 0.0), axis=0, keepdims=True)

    def level_updates():
        for copy in outer:
            copy.wait_recv()
        even = lax.rem(lax.broadcasted_iota(jnp.int32, (2 * PLANES, COLS), 0), 2) == 0
        for c in range(3):
            cols = slice(128 * c, 128 * (c + 1))
            from_w, from_e = rim_got[0, :, cols], rim_got[1, :, cols]
            up, down = pltpu.roll(from_e, 2 * PLANES - 1, 0), pltpu.roll(from_w, 1, 0)
            rim_m[0 : 2 * PLANES, :] = jnp.where(even, up, down)
            rim_back[128 * c : 128 * (c + 1), :] = rim_m[...].T
        for q in range(PLANES):
            uvt[q, 7:8, :] = edge_got[0, q : q + 1, :]
            uvt[q, 8 + ROWS : 9 + ROWS, :] = edge_got[1, q : q + 1, :]
        first, last = lanes(BY) == 0, lanes(BY) == COLS - 1

        for b in range(BLOCKS):
            r = b * BY
            rows = slice(r, r + BY)
            at = slice(OFF + r, OFF + r + BY)
            on = act[b : b + 1, :]
            ocean = land[rows, :].astype(F32)
            keep = on * ocean
            off = 1.0 - on
            cor = coriolis(b)
            faces = [face[k, 0, at, :] for k in range(4)]
            rim_row = rim_back[rows, :]

            def around(q):
                c = uvt[q, 8 + r : 8 + r + BY, :]
                side = pltpu.roll(rim_row, COLS - 1 - 2 * q, 1)
                e = jnp.where(last, side, pltpu.roll(c, COLS - 1, 1))
                w = jnp.where(first, side, pltpu.roll(c, 1, 1))
                return c, e, w, uvt[q, 9 + r : 9 + r + BY, :], uvt[q, 7 + r : 7 + r + BY, :]

            def raw(q0):
                out, keepers = [], []
                for k in range(LEVELS):
                    c, *others = around(q0 + k)
                    spread = sum(faces[i] * (o - c) for i, o in enumerate(others))
                    mix = jnp.zeros_like(c)
                    if k < LEVELS - 1:
                        mix = mix + (uvt[q0 + k + 1, 8 + r : 8 + r + BY, :] - c)
                    if k > 0:
                        mix = mix - (c - uvt[q0 + k - 1, 8 + r : 8 + r + BY, :])
                    out.append((c, 0.5 * mix + 0.5 * spread, others))
                return out

            for k, (c, tend, _) in enumerate(raw(0)):
                star = c + 0.2 * (tend + cor * uvt[LEVELS + k, 8 + r : 8 + r + BY, :])
                u_out[k, rows, :] = keep * star + off * c
            for k, (c, tend, _) in enumerate(raw(LEVELS)):
                star = c + 0.2 * (tend - cor * uvt[k, 8 + r : 8 + r + BY, :])
                v_out[k, rows, :] = keep * star + off * c
            for k, (c, tend, (e, w, nn, s)) in enumerate(raw(2 * LEVELS)):
                uk = uvt[k, 8 + r : 8 + r + BY, :]
                vk = uvt[LEVELS + k, 8 + r : 8 + r + BY, :]
                star = c + 0.2 * (tend - 0.5 * (uk * (e - w) + vk * (nn - s)))
                t_out[k, rows, :] = keep * star + off * c

    for s, kind in enumerate(RED_STAGES):
        landing = red[s]
        part[s] = row
        for j, peer in enumerate(peers(kind)):
            pltpu.make_async_remote_copy(
                src_ref=part.at[s], dst_ref=landing.at[j], send_sem=rsend_sem.at[s], recv_sem=rrecv_sem.at[s],
                device_id=peer, device_id_type=MESH,
            ).start()
        if s == 0:
            level_updates()
        every = pltpu.make_async_remote_copy(
            src_ref=landing, dst_ref=landing, send_sem=rsend_sem.at[s], recv_sem=rrecv_sem.at[s],
            device_id=(east, gy), device_id_type=MESH,
        )
        every.wait_recv()
        row = row + jnp.sum(landing[...], axis=0)

    c = coefficients([jnp.broadcast_to(row[:, k : k + 1], (1, COLS)) for k in range(8)])

    def answer(t, at):
        x = ext[X0, t, at, :]
        for k in range(4):
            x = x + c[k] * basis[k, t, at, :]
        return x

    for b in range(BLOCKS):
        rows = slice(b * BY, (b + 1) * BY)
        at = slice(OFF + b * BY, OFF + (b + 1) * BY)
        x0, x1 = answer(0, at), answer(1, at)
        up = answer(0, slice(at.start + 1, at.stop + 1))
        right = jnp.where(lanes(BY) == COLS - 1, pltpu.roll(x1, COLS - 1, 1), pltpu.roll(x0, COLS - 1, 1))
        keep = act[b : b + 1, :] * land[rows, :].astype(F32)
        p_out[rows, :] = x0
        grad_x, grad_y = keep * (right - x0), keep * (up - x0)
        for k in range(LEVELS):
            u_out[k, rows, :] = u_out[k, rows, :] - grad_x
            v_out[k, rows, :] = v_out[k, rows, :] - grad_y

    for copy in halo + outer:
        copy.wait_send()
    for s in range(len(RED_STAGES)):
        pltpu.make_async_remote_copy(
            src_ref=red[s], dst_ref=red[s], send_sem=rsend_sem.at[s], recv_sem=rrecv_sem.at[s],
            device_id=(east, gy), device_id_type=MESH,
        ).wait_send()


def emit_kernel(*refs):
    n = (len(refs) - 1) // 2
    sem = refs[-1]
    copies = [pltpu.make_async_copy(refs[i], refs[n + i], sem.at[i]) for i in range(n)]
    for copy in copies:
        copy.start()
    for copy in copies:
        copy.wait()


def on_device(*args):
    args = args[:7] + (args[7].T, args[8].T)
    vmem, hbm = pltpu.VMEM, pltpu.HBM
    three = jax.ShapeDtypeStruct((LEVELS, ROWS, COLS), F32)
    two = jax.ShapeDtypeStruct((ROWS, COLS), F32)
    shapes = (three, three, three, two)
    tiles = (2, EXT_ROWS, COLS)
    scratch = [
        vmem((PLANES, ROWS + 16, COLS), F32),
        vmem((ROWS, COLS), F32),
        vmem((ROWS, COLS), F32),
        vmem((ROWS, COLS), jnp.int32),
        vmem((NX_DEV, NBY), jnp.int32),
        vmem((NX_DEV, NBY), jnp.int32),
        vmem((BLOCKS, COLS), F32),
        vmem((BLOCKS, COLS), F32),
        vmem((FIELDS,) + tiles, F32),
        vmem((384, COLS), F32),
        vmem((8, 2, 8, 384), F32),
        vmem((8, 2, 8, 384), F32),
        vmem((ROWS + 16, COLS), F32),
        vmem((4, 8, COLS), F32),
        vmem((384, COLS), F32),
        vmem((2 * PLANES, 384), F32),
        vmem((2, 2 * PLANES, 384), F32),
        vmem((COLS, COLS), F32),
        vmem((384, COLS), F32),
        vmem((2, 16, COLS), F32),
        vmem((2, 16, COLS), F32),
        vmem((4,) + tiles, F32),
        vmem(tiles, F32),
        vmem((4,) + tiles, F32),
        vmem((EXT_ROWS, COLS), F32),
        vmem((2,) + tiles, F32),
        vmem((4,) + tiles, F32),
        vmem((len(RED_STAGES), 1, COLS), F32),
        pltpu.SemaphoreType.DMA((9,)),
        pltpu.SemaphoreType.DMA((12,)),
        pltpu.SemaphoreType.DMA((12,)),
        pltpu.SemaphoreType.DMA((len(RED_STAGES),)),
        pltpu.SemaphoreType.DMA((len(RED_STAGES),)),
    ] + [vmem((COUNT[kind], 1, COLS), F32) for kind in RED_STAGES]
    out = pl.pallas_call(
        ocean_kernel,
        out_shape=shapes,
        in_specs=[pl.BlockSpec(memory_space=hbm)] * 9,
        out_specs=[pl.BlockSpec(memory_space=vmem)] * 4,
        scratch_shapes=scratch,
        compiler_params=pltpu.CompilerParams(
            collective_id=0, has_side_effects=True, vmem_limit_bytes=VMEM_LIMIT
        ),
        name="ocean",
    )(*args)
    return pl.pallas_call(
        emit_kernel,
        out_shape=shapes,
        in_specs=[pl.BlockSpec(memory_space=vmem)] * 4,
        out_specs=[pl.BlockSpec(memory_space=hbm)] * 4,
        scratch_shapes=[pltpu.SemaphoreType.DMA((4,))],
        compiler_params=pltpu.CompilerParams(vmem_limit_bytes=8 * 1024 * 1024),
        name="emit",
    )(*out)


def solution(mesh):
    wide, flat = P(None, "gy", "gx"), P("gy", "gx")
    return jax.shard_map(
        on_device,
        mesh=mesh,
        in_specs=(wide, wide, wide, flat, flat, flat, flat, P(), P()),
        out_specs=(wide, wide, wide, flat),
        check_vma=False,
    )
```

```python
import functools

import jax
import jax.numpy as jnp
from jax import lax
from jax.experimental import pallas as pl
from jax.experimental.pallas import tpu as pltpu
from jax.sharding import PartitionSpec as P

MESH = pl.DeviceIdType.MESH
F32 = jnp.float32

LEVELS, ROWS, COLS, BY, NY = 4, 320, 128, 40, 2560
BLOCKS, NBY = ROWS // BY, 64
THICK = [(2 * k + 1) / (LEVELS * LEVELS) for k in range(LEVELS)]

OFF = 16
EXT_ROWS = ROWS + 2 * OFF
LOW, HIGH = OFF - 8, OFF + ROWS + 8
STEP = 48
FIELDS = 7
WET, HELM, X0, UB, UH, VB, VH = range(FIELDS)
PLANES = 3 * LEVELS
NX_DEV, NY_DEV = 16, 8

VMEM_LIMIT = 24 * 1024 * 1024
RED_STAGES = ("all",)


def peers(kind):
    gx, gy = lax.axis_index("gx"), lax.axis_index("gy")
    if kind == "halo":
        return [
            (lax.rem(gx + i, NX_DEV), lax.rem(gy + j, NY_DEV))
            for i in (0, 1, NX_DEV - 1)
            for j in (0, 1, NY_DEV - 1)
            if i or j
        ]
    if kind == "plane":
        base = gx // 4 * 4
        return [
            (base + lax.rem(lax.rem(gx, 4) + i, 4), lax.rem(gy + j, NY_DEV))
            for i in range(4)
            for j in range(NY_DEV)
            if i or j
        ]
    if kind == "z":
        return [(lax.rem(gx + 4 * j, NX_DEV), gy) for j in range(1, 4)]
    return [
        (lax.rem(gx + i, NX_DEV), lax.rem(gy + j, NY_DEV))
        for i in range(NX_DEV)
        for j in range(NY_DEV)
        if i or j
    ]


COUNT = {"all": 127, "plane": 31, "z": 3}


def lanes(rows):
    return lax.broadcasted_iota(jnp.int32, (rows, COLS), 1)


def beside(ref, r, n, both=True):
    lane = lanes(n)
    first, last = lane == 0, lane == COLS - 1
    c0, c1 = ref[0, r : r + n, :], ref[1, r : r + n, :]
    e0, e1 = pltpu.roll(c0, COLS - 1, 1), pltpu.roll(c1, COLS - 1, 1)
    w0, w1 = pltpu.roll(c0, 1, 1), pltpu.roll(c1, 1, 1)
    out = [
        (
            c0,
            jnp.where(last, e1, e0),
            jnp.where(first, w1, w0),
            ref[0, r + 1 : r + 1 + n, :],
            ref[0, r - 1 : r - 1 + n, :],
        )
    ]
    if both:
        out.append(
            (
                c1,
                jnp.where(last, e0, e1),
                jnp.where(first, w0, w1),
                ref[1, r + 1 : r + 1 + n, :],
                ref[1, r - 1 : r - 1 + n, :],
            )
        )
    return out


def west_of(ref, r, n):
    first = lanes(n) == 0
    c0, c1 = ref[0, r : r + n, :], ref[1, r : r + n, :]
    w0, w1 = pltpu.roll(c0, 1, 1), pltpu.roll(c1, 1, 1)
    return (c0, jnp.where(first, w1, w0)), (c1, jnp.where(first, w0, w1))


def eights(x):
    return jnp.sum(x.reshape(x.shape[0] // 8, 8, COLS), axis=0)


def coefficients(sums):
    m = [sums[0], sums[1]]
    for k in range(2, 8):
        m.append(2.0 * sums[k] - m[k % 2])
    g = [[0.5 * (m[i + j] + m[abs(i - j)]) for j in range(5) if i + j < 8] for i in range(4)]

    def image(i, j):
        if j == 0:
            return g[i][1]
        return 0.5 * (g[i][j + 1] + g[i][j - 1])

    a = [[g[i][j] - image(i, j) for j in range(i + 1)] for i in range(4)]
    low = [[None] * 4 for _ in range(4)]
    inv, piv = [], []
    for j in range(4):
        pivot = a[j][j]
        for k in range(j):
            pivot = pivot - low[j][k] * low[j][k] * piv[k]
        good = pivot > 1e-6 * a[j][j]
        piv.append(jnp.where(good, pivot, 0.0))
        inv.append(jnp.where(good, 1.0 / jnp.where(good, pivot, 1.0), 0.0))
        for i in range(j + 1, 4):
            s = a[i][j]
            for k in range(j):
                s = s - low[i][k] * low[j][k] * piv[k]
            low[i][j] = s * inv[j]
    y = []
    for i in range(4):
        s = m[i]
        for k in range(i):
            s = s - low[i][k] * y[k]
        y.append(s)
    c = [None] * 4
    for i in reversed(range(4)):
        s = y[i] * inv[i]
        for k in range(i + 1, 4):
            s = s - low[k][i] * c[k]
        c[i] = s
    return c


def ocean_kernel(
    u_hbm, v_hbm, t_hbm, p_hbm, depth_hbm, helm_hbm, land_hbm, clinic_hbm, tropic_hbm,
    u_out, v_out, t_out, p_out,
    uvt, pold, depth, land, cmap, tmap, act, dom,
    ext, pack, pack_t, got_t, got, corner,
    rim, rim_t, rim_got, rim_m, rim_back, edge, edge_got,
    face, rdiag, gain, diag, flow, basis, part,
    in_sem, send_sem, recv_sem, rsend_sem, rrecv_sem, *red,
):
    gx, gy = lax.axis_index("gx"), lax.axis_index("gy")
    east, west = lax.rem(gx + 1, NX_DEV), lax.rem(gx + NX_DEV - 1, NX_DEV)
    north, south = lax.rem(gy + 1, NY_DEV), lax.rem(gy + NY_DEV - 1, NY_DEV)
    own = pl.ds(OFF, ROWS)

    loads = [
        pltpu.make_async_copy(u_hbm, uvt.at[0:4, 8 : 8 + ROWS, :], in_sem.at[0]),
        pltpu.make_async_copy(v_hbm, uvt.at[4:8, 8 : 8 + ROWS, :], in_sem.at[1]),
        pltpu.make_async_copy(p_hbm, pold, in_sem.at[2]),
        pltpu.make_async_copy(depth_hbm, depth, in_sem.at[3]),
        pltpu.make_async_copy(land_hbm, land, in_sem.at[4]),
        pltpu.make_async_copy(clinic_hbm, cmap, in_sem.at[5]),
        pltpu.make_async_copy(tropic_hbm, tmap, in_sem.at[6]),
        pltpu.make_async_copy(helm_hbm, ext.at[HELM, 0, OFF : OFF + ROWS, :], in_sem.at[7]),
        pltpu.make_async_copy(t_hbm, uvt.at[8:12, 8 : 8 + ROWS, :], in_sem.at[8]),
    ]
    for load in loads:
        load.start()

    barrier = pltpu.get_barrier_semaphore()
    greeted = []
    for kind in RED_STAGES if RED_STAGES == ("all",) else RED_STAGES + ("halo",):
        greeted += peers(kind)
    for peer in greeted:
        pl.semaphore_signal(barrier, inc=1, device_id=peer, device_id_type=MESH)

    pack[ROWS:, :] = jnp.zeros((pack.shape[0] - ROWS, COLS), F32)
    for load in loads[:8]:
        load.wait()

    shape = (NX_DEV, NBY)
    mine = lax.broadcasted_iota(jnp.int32, shape, 0) == gx
    shape = (BLOCKS, NBY)
    wanted = lax.broadcasted_iota(jnp.int32, shape, 1) == lax.broadcasted_iota(jnp.int32, shape, 0) + gy * BLOCKS

    def per_block(flags):
        line = jnp.sum(jnp.where(mine, flags, 0.0), axis=0, keepdims=True)
        column = jnp.sum(jnp.where(wanted, line, 0.0), axis=1, keepdims=True)
        return jnp.broadcast_to(column, (BLOCKS, COLS))

    act[...] = per_block(cmap[...].astype(F32))
    dom[...] = per_block(jnp.where(tmap[...] >= 0, 1.0, 0.0))

    def coriolis(b):
        row = lax.broadcasted_iota(jnp.int32, (BY, COLS), 0) + (gy * ROWS + b * BY)
        return 0.2 + 0.6 * ((row.astype(F32) + 0.5) / NY)

    group = lanes(BY) // 16
    for b in range(BLOCKS):
        r = b * BY
        rows = slice(r, r + BY)
        solve = land[rows, :].astype(F32) * dom[b : b + 1, :]
        wet = depth[rows, :] * solve
        u = [uvt[k, 8 + r : 8 + r + BY, :] for k in range(LEVELS)]
        v = [uvt[LEVELS + k, 8 + r : 8 + r + BY, :] for k in range(LEVELS)]
        u_bar = sum(THICK[k] * u[k] for k in range(LEVELS))
        v_bar = sum(THICK[k] * v[k] for k in range(LEVELS))
        cor = 0.2 * coriolis(b)
        mix = 0.1 * (THICK[1] - THICK[0])
        u_hat = u_bar + mix * (u[0] - u[3]) + cor * v_bar
        v_hat = v_bar + mix * (v[0] - v[3]) - cor * u_bar
        fields = [wet, ext[HELM, 0, OFF + r : OFF + r + BY, :], solve * pold[rows, :], u_bar, u_hat, v_bar, v_hat]
        packed = None
        for f, value in enumerate(fields):
            if f != HELM:
                ext[f, 0, OFF + r : OFF + r + BY, :] = value
            moved = pltpu.roll(value, 8 + 16 * f, 1)
            packed = moved if packed is None else jnp.where(group == f, moved, packed)
        pack[rows, :] = packed
    for c in range(3):
        pack_t[:, :, :, 128 * c : 128 * (c + 1)] = pack[128 * c : 128 * (c + 1), :].T.reshape(8, 2, 8, COLS)

    def send(src, dst, k, to):
        copy = pltpu.make_async_remote_copy(
            src_ref=src, dst_ref=dst, send_sem=send_sem.at[k], recv_sem=recv_sem.at[k], device_id=to, device_id_type=MESH
        )
        copy.start()
        return copy

    pl.semaphore_wait(barrier, len(greeted))
    halo = [
        send(pack_t.at[0:7, 0], got_t.at[0:7, 0], 0, (east, gy)),
        send(pack_t.at[0:7, 1], got_t.at[0:7, 1], 1, (west, gy)),
        send(ext.at[:, 0, OFF + ROWS - 8 : OFF + ROWS, :], ext.at[:, 0, LOW:OFF, :], 2, (gx, north)),
        send(ext.at[:, 0, OFF : OFF + 8, :], ext.at[:, 0, OFF + ROWS : HIGH, :], 3, (gx, south)),
        send(pack.at[ROWS - 8 : ROWS, :], corner.at[0], 4, (east, north)),
        send(pack.at[ROWS - 8 : ROWS, :], corner.at[1], 5, (west, north)),
        send(pack.at[0:8, :], corner.at[2], 6, (east, south)),
        send(pack.at[0:8, :], corner.at[3], 7, (west, south)),
    ]

    loads[8].wait()
    pair = lanes(BY) // 2
    for b in range(BLOCKS):
        r = b * BY
        packed = None
        for q in range(PLANES):
            moved = pltpu.roll(uvt[q, 8 + r : 8 + r + BY, :], 2 * q + 1, 1)
            packed = moved if packed is None else jnp.where(pair == q, moved, packed)
        rim[r : r + BY, :] = packed
    rim[ROWS:, :] = jnp.zeros((rim.shape[0] - ROWS, COLS), F32)
    for c in range(3):
        rim_t[:, 128 * c : 128 * (c + 1)] = rim[128 * c : 128 * (c + 1), :].T[: 2 * PLANES, :]
    for q in range(PLANES):
        edge[0, q : q + 1, :] = uvt[q, 8 : 9, :]
        edge[1, q : q + 1, :] = uvt[q, 7 + ROWS : 8 + ROWS, :]
    outer = [
        send(rim_t, rim_got.at[0], 8, (east, gy)),
        send(rim_t, rim_got.at[1], 9, (west, gy)),
        send(edge.at[1], edge_got.at[0], 10, (gx, north)),
        send(edge.at[0], edge_got.at[1], 11, (gx, south)),
    ]

    for copy in halo:
        copy.wait_recv()
    low_half = lax.rem(lanes(8), 16) < 8
    got[0:8, :] = jnp.where(low_half, corner[0], corner[1])
    for c in range(3):
        block = got_t[:, :, :, 128 * c : 128 * (c + 1)].reshape(128, 128).T
        n = min(128, ROWS - 128 * c)
        got[8 + 128 * c : 8 + 128 * c + n, :] = block[:n, :]
    got[8 + ROWS : 16 + ROWS, :] = jnp.where(low_half, corner[2], corner[3])

    chunks = [(r, STEP) for r in range(LOW, HIGH, STEP)]
    lane = lanes(STEP)
    sides = (lane < 8) | (lane >= COLS - 8)
    for r, n in chunks:
        packed = got[r - LOW : r - LOW + n, :]
        for f in range(FIELDS):
            moved = pltpu.roll(packed, COLS - (16 * f + 8), 1)
            ext[f, 1, r : r + n, :] = jnp.where(sides, moved, 1.0 if f == HELM else 0.0)

    for r, n in chunks:
        at = slice(r, r + n)
        for t, (c, e, w, nn, s) in enumerate(beside(ext.at[WET], r, n)):
            four = [jnp.minimum(c, o) for o in (e, w, nn, s)]
            total = ext[HELM, t, at, :] + four[0] + four[1] + four[2] + four[3]
            inverse = 1.0 / total
            rdiag[t, at, :] = inverse
            if t == 0:
                diag[at, :] = total
            for k in range(4):
                face[k, t, at, :] = four[k]
                gain[k, t, at, :] = four[k] * inverse
    for k, (bar, hat) in enumerate(((UB, UH), (VB, VH))):
        for r, n in chunks:
            at = slice(r, r + n)
            for t, (c, *others) in enumerate(beside(ext.at[bar], r, n)):
                spread = sum(face[i, t, at, :] * (o - c) for i, o in enumerate(others))
                flow[k, t, at, :] = ext[WET, t, at, :] * (ext[hat, t, at, :] + 0.1 * spread)

    def image(t, at, others):
        return sum(gain[i, t, at, :] * o for i, o in enumerate(others))

    for r, n in chunks:
        at = slice(r, r + n)
        x = beside(ext.at[X0], r, n)
        for t, (ef, efw) in enumerate(west_of(flow.at[0], r, n)):
            nf, nfs = flow[1, t, at, :], flow[1, t, r - 1 : r - 1 + n, :]
            force = jnp.where(ext[WET, t, at, :] > 0.0, (efw - ef) + (nfs - nf), 0.0)
            c, *others = x[t]
            basis[0, t, at, :] = force * rdiag[t, at, :] + (image(t, at, others) - c)
    for k in range(3):
        for r, n in chunks:
            at = slice(r, r + n)
            for t, (c, *others) in enumerate(beside(basis.at[k], r, n)):
                value = image(t, at, others)
                if k:
                    value = 2.0 * value - basis[k - 1, t, at, :]
                basis[k + 1, t, at, :] = value
    sums = [jnp.zeros((8, COLS), F32) for _ in range(8)]
    for b in range(BLOCKS):
        r = OFF + b * BY
        at = slice(r, r + BY)
        ((c, *others),) = beside(basis.at[3], r, BY, both=False)
        t4 = 2.0 * image(0, at, others) - basis[2, 0, at, :]
        vectors = [basis[k, 0, at, :] for k in range(3)] + [c, t4]
        for k in range(4):
            weighted = diag[at, :] * vectors[k]
            sums[2 * k] = sums[2 * k] + eights(weighted * vectors[k])
            sums[2 * k + 1] = sums[2 * k + 1] + eights(weighted * vectors[k + 1])

    rows8 = lax.broadcasted_iota(jnp.int32, (8, COLS), 0)
    mat = jnp.zeros((8, COLS), F32)
    for k in range(8):
        mat = jnp.where(rows8 == k, jnp.sum(sums[k], axis=0, keepdims=True), mat)
    total = jnp.broadcast_to(jnp.sum(mat, axis=1, keepdims=True), (8, COLS))
    row = jnp.sum(jnp.where(lanes(8) == rows8, total, 0.0), axis=0, keepdims=True)

    def level_updates():
        for copy in outer:
            copy.wait_recv()
        even = lax.rem(lax.broadcasted_iota(jnp.int32, (2 * PLANES, COLS), 0), 2) == 0
        for c in range(3):
            cols = slice(128 * c, 128 * (c + 1))
            from_w, from_e = rim_got[0, :, cols], rim_got[1, :, cols]
            up, down = pltpu.roll(from_e, 2 * PLANES - 1, 0), pltpu.roll(from_w, 1, 0)
            rim_m[0 : 2 * PLANES, :] = jnp.where(even, up, down)
            rim_back[128 * c : 128 * (c + 1), :] = rim_m[...].T
        for q in range(PLANES):
            uvt[q, 7:8, :] = edge_got[0, q : q + 1, :]
            uvt[q, 8 + ROWS : 9 + ROWS, :] = edge_got[1, q : q + 1, :]
        first, last = lanes(BY) == 0, lanes(BY) == COLS - 1

        for b in range(BLOCKS):
            r = b * BY
            rows = slice(r, r + BY)
            at = slice(OFF + r, OFF + r + BY)
            on = act[b : b + 1, :]
            ocean = land[rows, :].astype(F32)
            keep = on * ocean
            off = 1.0 - on
            cor = coriolis(b)
            faces = [face[k, 0, at, :] for k in range(4)]
            rim_row = rim_back[rows, :]

            def around(q):
                c = uvt[q, 8 + r : 8 + r + BY, :]
                side = pltpu.roll(rim_row, COLS - 1 - 2 * q, 1)
                e = jnp.where(last, side, pltpu.roll(c, COLS - 1, 1))
                w = jnp.where(first, side, pltpu.roll(c, 1, 1))
                return c, e, w, uvt[q, 9 + r : 9 + r + BY, :], uvt[q, 7 + r : 7 + r + BY, :]

            def raw(q0):
                out, keepers = [], []
                for k in range(LEVELS):
                    c, *others = around(q0 + k)
                    spread = sum(faces[i] * (o - c) for i, o in enumerate(others))
                    mix = jnp.zeros_like(c)
                    if k < LEVELS - 1:
                        mix = mix + (uvt[q0 + k + 1, 8 + r : 8 + r + BY, :] - c)
                    if k > 0:
                        mix = mix - (c - uvt[q0 + k - 1, 8 + r : 8 + r + BY, :])
                    out.append((c, 0.5 * mix + 0.5 * spread, others))
                return out

            for k, (c, tend, _) in enumerate(raw(0)):
                star = c + 0.2 * (tend + cor * uvt[LEVELS + k, 8 + r : 8 + r + BY, :])
                u_out[k, rows, :] = keep * star + off * c
            for k, (c, tend, _) in enumerate(raw(LEVELS)):
                star = c + 0.2 * (tend - cor * uvt[k, 8 + r : 8 + r + BY, :])
                v_out[k, rows, :] = keep * star + off * c
            for k, (c, tend, (e, w, nn, s)) in enumerate(raw(2 * LEVELS)):
                uk = uvt[k, 8 + r : 8 + r + BY, :]
                vk = uvt[LEVELS + k, 8 + r : 8 + r + BY, :]
                star = c + 0.2 * (tend - 0.5 * (uk * (e - w) + vk * (nn - s)))
                t_out[k, rows, :] = keep * star + off * c

    for s, kind in enumerate(RED_STAGES):
        landing = red[s]
        part[s] = row
        for j, peer in enumerate(peers(kind)):
            pltpu.make_async_remote_copy(
                src_ref=part.at[s], dst_ref=landing.at[j], send_sem=rsend_sem.at[s], recv_sem=rrecv_sem.at[s],
                device_id=peer, device_id_type=MESH,
            ).start()
        if s == 0:
            level_updates()
        every = pltpu.make_async_remote_copy(
            src_ref=landing, dst_ref=landing, send_sem=rsend_sem.at[s], recv_sem=rrecv_sem.at[s],
            device_id=(east, gy), device_id_type=MESH,
        )
        every.wait_recv()
        row = row + jnp.sum(landing[...], axis=0)

    c = coefficients([jnp.broadcast_to(row[:, k : k + 1], (1, COLS)) for k in range(8)])

    def answer(t, at):
        x = ext[X0, t, at, :]
        for k in range(4):
            x = x + c[k] * basis[k, t, at, :]
        return x

    for b in range(BLOCKS):
        rows = slice(b * BY, (b + 1) * BY)
        at = slice(OFF + b * BY, OFF + (b + 1) * BY)
        x0, x1 = answer(0, at), answer(1, at)
        up = answer(0, slice(at.start + 1, at.stop + 1))
        right = jnp.where(lanes(BY) == COLS - 1, pltpu.roll(x1, COLS - 1, 1), pltpu.roll(x0, COLS - 1, 1))
        keep = act[b : b + 1, :] * land[rows, :].astype(F32)
        p_out[rows, :] = x0
        grad_x, grad_y = keep * (right - x0), keep * (up - x0)
        for k in range(LEVELS):
            u_out[k, rows, :] = u_out[k, rows, :] - grad_x
            v_out[k, rows, :] = v_out[k, rows, :] - grad_y

    for copy in halo + outer:
        copy.wait_send()
    for s in range(len(RED_STAGES)):
        pltpu.make_async_remote_copy(
            src_ref=red[s], dst_ref=red[s], send_sem=rsend_sem.at[s], recv_sem=rrecv_sem.at[s],
            device_id=(east, gy), device_id_type=MESH,
        ).wait_send()


def emit_kernel(*refs):
    n = (len(refs) - 1) // 2
    sem = refs[-1]
    copies = [pltpu.make_async_copy(refs[i], refs[n + i], sem.at[i]) for i in range(n)]
    for copy in copies:
        copy.start()
    for copy in copies:
        copy.wait()


def on_device(*args):
    args = args[:7] + (args[7].T, args[8].T)
    args = [pltpu.with_memory_space_constraint(x, pltpu.HBM) for x in args]
    vmem, hbm = pltpu.VMEM, pltpu.HBM
    three = jax.ShapeDtypeStruct((LEVELS, ROWS, COLS), F32)
    two = jax.ShapeDtypeStruct((ROWS, COLS), F32)
    shapes = (three, three, three, two)
    tiles = (2, EXT_ROWS, COLS)
    scratch = [
        vmem((PLANES, ROWS + 16, COLS), F32),
        vmem((ROWS, COLS), F32),
        vmem((ROWS, COLS), F32),
        vmem((ROWS, COLS), jnp.int32),
        vmem((NX_DEV, NBY), jnp.int32),
        vmem((NX_DEV, NBY), jnp.int32),
        vmem((BLOCKS, COLS), F32),
        vmem((BLOCKS, COLS), F32),
        vmem((FIELDS,) + tiles, F32),
        vmem((384, COLS), F32),
        vmem((8, 2, 8, 384), F32),
        vmem((8, 2, 8, 384), F32),
        vmem((ROWS + 16, COLS), F32),
        vmem((4, 8, COLS), F32),
        vmem((384, COLS), F32),
        vmem((2 * PLANES, 384), F32),
        vmem((2, 2 * PLANES, 384), F32),
        vmem((COLS, COLS), F32),
        vmem((384, COLS), F32),
        vmem((2, 16, COLS), F32),
        vmem((2, 16, COLS), F32),
        vmem((4,) + tiles, F32),
        vmem(tiles, F32),
        vmem((4,) + tiles, F32),
        vmem((EXT_ROWS, COLS), F32),
        vmem((2,) + tiles, F32),
        vmem((4,) + tiles, F32),
        vmem((len(RED_STAGES), 1, COLS), F32),
        pltpu.SemaphoreType.DMA((9,)),
        pltpu.SemaphoreType.DMA((12,)),
        pltpu.SemaphoreType.DMA((12,)),
        pltpu.SemaphoreType.DMA((len(RED_STAGES),)),
        pltpu.SemaphoreType.DMA((len(RED_STAGES),)),
    ] + [vmem((COUNT[kind], 1, COLS), F32) for kind in RED_STAGES]
    out = pl.pallas_call(
        ocean_kernel,
        out_shape=[vmem(x.shape, x.dtype) for x in shapes],
        in_specs=[pl.BlockSpec(memory_space=hbm)] * 9,
        out_specs=[pl.BlockSpec(memory_space=vmem)] * 4,
        scratch_shapes=scratch,
        compiler_params=pltpu.CompilerParams(
            collective_id=0, has_side_effects=True, vmem_limit_bytes=VMEM_LIMIT
        ),
        name="ocean",
    )(*args)
    return pl.pallas_call(
        emit_kernel,
        out_shape=shapes,
        in_specs=[pl.BlockSpec(memory_space=vmem)] * 4,
        out_specs=[pl.BlockSpec(memory_space=hbm)] * 4,
        scratch_shapes=[pltpu.SemaphoreType.DMA((4,))],
        compiler_params=pltpu.CompilerParams(vmem_limit_bytes=8 * 1024 * 1024),
        name="emit",
    )(*out)


def solution(mesh):
    wide, flat = P(None, "gy", "gx"), P("gy", "gx")
    return jax.shard_map(
        on_device,
        mesh=mesh,
        in_specs=(wide, wide, wide, flat, flat, flat, flat, P(), P()),
        out_specs=(wide, wide, wide, flat),
        check_vma=False,
    )
```

```python
import functools

import jax
import jax.numpy as jnp
from jax import lax
from jax.experimental import pallas as pl
from jax.experimental.pallas import tpu as pltpu
from jax.sharding import PartitionSpec as P

MESH = pl.DeviceIdType.MESH
F32 = jnp.float32

LEVELS, ROWS, COLS, BY, NY = 4, 320, 128, 40, 2560
BLOCKS, NBY = ROWS // BY, 64
THICK = [(2 * k + 1) / (LEVELS * LEVELS) for k in range(LEVELS)]

OFF = 16
EXT_ROWS = ROWS + 2 * OFF
LOW, HIGH = OFF - 8, OFF + ROWS + 8
STEP = 48
FIELDS = 7
WET, HELM, X0, UB, UH, VB, VH = range(FIELDS)
PLANES = 3 * LEVELS
NX_DEV, NY_DEV = 16, 8

VMEM_LIMIT = 24 * 1024 * 1024
RED_STAGES = ("all",)


def peers(kind):
    gx, gy = lax.axis_index("gx"), lax.axis_index("gy")
    if kind == "halo":
        return [
            (lax.rem(gx + i, NX_DEV), lax.rem(gy + j, NY_DEV))
            for i in (0, 1, NX_DEV - 1)
            for j in (0, 1, NY_DEV - 1)
            if i or j
        ]
    if kind == "ball":
        z, y, x, core = gx // 4, lax.rem(gx, 4), gy // 2, lax.rem(gy, 2)
        return [
            (lax.rem(z + i, 4) * 4 + lax.rem(y + j, 4), lax.rem(x + k, 4) * 2 + lax.rem(core + c, 2))
            for i in (0, 1, 3)
            for j in (0, 1, 3)
            for k in (0, 1, 3)
            for c in (0, 1)
            if i or j or k or c
        ]
    if kind == "plane":
        base = gx // 4 * 4
        return [
            (base + lax.rem(lax.rem(gx, 4) + i, 4), lax.rem(gy + j, NY_DEV))
            for i in range(4)
            for j in range(NY_DEV)
            if i or j
        ]
    if kind == "z":
        return [(lax.rem(gx + 4 * j, NX_DEV), gy) for j in range(1, 4)]
    return [
        (lax.rem(gx + i, NX_DEV), lax.rem(gy + j, NY_DEV))
        for i in range(NX_DEV)
        for j in range(NY_DEV)
        if i or j
    ]


COUNT = {"all": 127, "plane": 31, "z": 3}


def lanes(rows):
    return lax.broadcasted_iota(jnp.int32, (rows, COLS), 1)


def beside(ref, r, n, both=True):
    lane = lanes(n)
    first, last = lane == 0, lane == COLS - 1
    c0, c1 = ref[0, r : r + n, :], ref[1, r : r + n, :]
    e0, e1 = pltpu.roll(c0, COLS - 1, 1), pltpu.roll(c1, COLS - 1, 1)
    w0, w1 = pltpu.roll(c0, 1, 1), pltpu.roll(c1, 1, 1)
    out = [
        (
            c0,
            jnp.where(last, e1, e0),
            jnp.where(first, w1, w0),
            ref[0, r + 1 : r + 1 + n, :],
            ref[0, r - 1 : r - 1 + n, :],
        )
    ]
    if both:
        out.append(
            (
                c1,
                jnp.where(last, e0, e1),
                jnp.where(first, w0, w1),
                ref[1, r + 1 : r + 1 + n, :],
                ref[1, r - 1 : r - 1 + n, :],
            )
        )
    return out


def west_of(ref, r, n):
    first = lanes(n) == 0
    c0, c1 = ref[0, r : r + n, :], ref[1, r : r + n, :]
    w0, w1 = pltpu.roll(c0, 1, 1), pltpu.roll(c1, 1, 1)
    return (c0, jnp.where(first, w1, w0)), (c1, jnp.where(first, w0, w1))


def eights(x):
    return jnp.sum(x.reshape(x.shape[0] // 8, 8, COLS), axis=0)


def coefficients(sums):
    m = [sums[0], sums[1]]
    for k in range(2, 8):
        m.append(2.0 * sums[k] - m[k % 2])
    g = [[0.5 * (m[i + j] + m[abs(i - j)]) for j in range(5) if i + j < 8] for i in range(4)]

    def image(i, j):
        if j == 0:
            return g[i][1]
        return 0.5 * (g[i][j + 1] + g[i][j - 1])

    a = [[g[i][j] - image(i, j) for j in range(i + 1)] for i in range(4)]
    low = [[None] * 4 for _ in range(4)]
    inv, piv = [], []
    for j in range(4):
        pivot = a[j][j]
        for k in range(j):
            pivot = pivot - low[j][k] * low[j][k] * piv[k]
        good = pivot > 1e-6 * a[j][j]
        piv.append(jnp.where(good, pivot, 0.0))
        inv.append(jnp.where(good, 1.0 / jnp.where(good, pivot, 1.0), 0.0))
        for i in range(j + 1, 4):
            s = a[i][j]
            for k in range(j):
                s = s - low[i][k] * low[j][k] * piv[k]
            low[i][j] = s * inv[j]
    y = []
    for i in range(4):
        s = m[i]
        for k in range(i):
            s = s - low[i][k] * y[k]
        y.append(s)
    c = [None] * 4
    for i in reversed(range(4)):
        s = y[i] * inv[i]
        for k in range(i + 1, 4):
            s = s - low[k][i] * c[k]
        c[i] = s
    return c


def ocean_kernel(
    u_hbm, v_hbm, t_hbm, p_hbm, depth_hbm, helm_hbm, land_hbm, clinic_hbm, tropic_hbm,
    u_out, v_out, t_out, p_out,
    uvt, pold, depth, land, cmap, tmap, act, dom,
    ext, pack, pack_t, got_t, got, corner,
    rim, rim_t, rim_got, rim_m, rim_back, edge, edge_got,
    face, rdiag, gain, diag, flow, basis, part,
    in_sem, send_sem, recv_sem, rsend_sem, rrecv_sem, known, *red,
):
    gx, gy = lax.axis_index("gx"), lax.axis_index("gy")
    east, west = lax.rem(gx + 1, NX_DEV), lax.rem(gx + NX_DEV - 1, NX_DEV)
    north, south = lax.rem(gy + 1, NY_DEV), lax.rem(gy + NY_DEV - 1, NY_DEV)
    own = pl.ds(OFF, ROWS)

    loads = [
        pltpu.make_async_copy(u_hbm, uvt.at[0:4, 8 : 8 + ROWS, :], in_sem.at[0]),
        pltpu.make_async_copy(v_hbm, uvt.at[4:8, 8 : 8 + ROWS, :], in_sem.at[1]),
        pltpu.make_async_copy(p_hbm, pold, in_sem.at[2]),
        pltpu.make_async_copy(depth_hbm, depth, in_sem.at[3]),
        pltpu.make_async_copy(land_hbm, land, in_sem.at[4]),
        pltpu.make_async_copy(clinic_hbm, cmap, in_sem.at[5]),
        pltpu.make_async_copy(tropic_hbm, tmap, in_sem.at[6]),
        pltpu.make_async_copy(helm_hbm, ext.at[HELM, 0, OFF : OFF + ROWS, :], in_sem.at[7]),
        pltpu.make_async_copy(t_hbm, uvt.at[8:12, 8 : 8 + ROWS, :], in_sem.at[8]),
    ]
    for load in loads:
        load.start()

    barrier = pltpu.get_barrier_semaphore()
    greeted = peers("ball")
    for peer in greeted:
        pl.semaphore_signal(barrier, inc=1, device_id=peer, device_id_type=MESH)

    pack[ROWS:, :] = jnp.zeros((pack.shape[0] - ROWS, COLS), F32)
    for load in loads[:8]:
        load.wait()

    shape = (NX_DEV, NBY)
    mine = lax.broadcasted_iota(jnp.int32, shape, 0) == gx
    shape = (BLOCKS, NBY)
    wanted = lax.broadcasted_iota(jnp.int32, shape, 1) == lax.broadcasted_iota(jnp.int32, shape, 0) + gy * BLOCKS

    def per_block(flags):
        line = jnp.sum(jnp.where(mine, flags, 0.0), axis=0, keepdims=True)
        column = jnp.sum(jnp.where(wanted, line, 0.0), axis=1, keepdims=True)
        return jnp.broadcast_to(column, (BLOCKS, COLS))

    act[...] = per_block(cmap[...].astype(F32))
    dom[...] = per_block(jnp.where(tmap[...] >= 0, 1.0, 0.0))

    def coriolis(b):
        row = lax.broadcasted_iota(jnp.int32, (BY, COLS), 0) + (gy * ROWS + b * BY)
        return 0.2 + 0.6 * ((row.astype(F32) + 0.5) / NY)

    group = lanes(BY) // 16
    for b in range(BLOCKS):
        r = b * BY
        rows = slice(r, r + BY)
        solve = land[rows, :].astype(F32) * dom[b : b + 1, :]
        wet = depth[rows, :] * solve
        u = [uvt[k, 8 + r : 8 + r + BY, :] for k in range(LEVELS)]
        v = [uvt[LEVELS + k, 8 + r : 8 + r + BY, :] for k in range(LEVELS)]
        u_bar = sum(THICK[k] * u[k] for k in range(LEVELS))
        v_bar = sum(THICK[k] * v[k] for k in range(LEVELS))
        cor = 0.2 * coriolis(b)
        mix = 0.1 * (THICK[1] - THICK[0])
        u_hat = u_bar + mix * (u[0] - u[3]) + cor * v_bar
        v_hat = v_bar + mix * (v[0] - v[3]) - cor * u_bar
        fields = [wet, ext[HELM, 0, OFF + r : OFF + r + BY, :], solve * pold[rows, :], u_bar, u_hat, v_bar, v_hat]
        packed = None
        for f, value in enumerate(fields):
            if f != HELM:
                ext[f, 0, OFF + r : OFF + r + BY, :] = value
            moved = pltpu.roll(value, 8 + 16 * f, 1)
            packed = moved if packed is None else jnp.where(group == f, moved, packed)
        pack[rows, :] = packed
    for c in range(3):
        pack_t[:, :, :, 128 * c : 128 * (c + 1)] = pack[128 * c : 128 * (c + 1), :].T.reshape(8, 2, 8, COLS)

    def send(src, dst, k, to):
        copy = pltpu.make_async_remote_copy(
            src_ref=src, dst_ref=dst, send_sem=send_sem.at[k], recv_sem=recv_sem.at[k], device_id=to, device_id_type=MESH
        )
        copy.start()
        return copy

    pl.semaphore_wait(barrier, len(greeted))
    for peer in greeted:
        pl.semaphore_signal(known, inc=1, device_id=peer, device_id_type=MESH)
    halo = [
        send(pack_t.at[0:7, 0], got_t.at[0:7, 0], 0, (east, gy)),
        send(pack_t.at[0:7, 1], got_t.at[0:7, 1], 1, (west, gy)),
        send(ext.at[:, 0, OFF + ROWS - 8 : OFF + ROWS, :], ext.at[:, 0, LOW:OFF, :], 2, (gx, north)),
        send(ext.at[:, 0, OFF : OFF + 8, :], ext.at[:, 0, OFF + ROWS : HIGH, :], 3, (gx, south)),
        send(pack.at[ROWS - 8 : ROWS, :], corner.at[0], 4, (east, north)),
        send(pack.at[ROWS - 8 : ROWS, :], corner.at[1], 5, (west, north)),
        send(pack.at[0:8, :], corner.at[2], 6, (east, south)),
        send(pack.at[0:8, :], corner.at[3], 7, (west, south)),
    ]

    loads[8].wait()
    pair = lanes(BY) // 2
    for b in range(BLOCKS):
        r = b * BY
        packed = None
        for q in range(PLANES):
            moved = pltpu.roll(uvt[q, 8 + r : 8 + r + BY, :], 2 * q + 1, 1)
            packed = moved if packed is None else jnp.where(pair == q, moved, packed)
        rim[r : r + BY, :] = packed
    rim[ROWS:, :] = jnp.zeros((rim.shape[0] - ROWS, COLS), F32)
    for c in range(3):
        rim_t[:, 128 * c : 128 * (c + 1)] = rim[128 * c : 128 * (c + 1), :].T[: 2 * PLANES, :]
    for q in range(PLANES):
        edge[0, q : q + 1, :] = uvt[q, 8 : 9, :]
        edge[1, q : q + 1, :] = uvt[q, 7 + ROWS : 8 + ROWS, :]
    outer = [
        send(rim_t, rim_got.at[0], 8, (east, gy)),
        send(rim_t, rim_got.at[1], 9, (west, gy)),
        send(edge.at[1], edge_got.at[0], 10, (gx, north)),
        send(edge.at[0], edge_got.at[1], 11, (gx, south)),
    ]

    for copy in halo:
        copy.wait_recv()
    low_half = lax.rem(lanes(8), 16) < 8
    got[0:8, :] = jnp.where(low_half, corner[0], corner[1])
    for c in range(3):
        block = got_t[:, :, :, 128 * c : 128 * (c + 1)].reshape(128, 128).T
        n = min(128, ROWS - 128 * c)
        got[8 + 128 * c : 8 + 128 * c + n, :] = block[:n, :]
    got[8 + ROWS : 16 + ROWS, :] = jnp.where(low_half, corner[2], corner[3])

    chunks = [(r, STEP) for r in range(LOW, HIGH, STEP)]
    lane = lanes(STEP)
    sides = (lane < 8) | (lane >= COLS - 8)
    for r, n in chunks:
        packed = got[r - LOW : r - LOW + n, :]
        for f in range(FIELDS):
            moved = pltpu.roll(packed, COLS - (16 * f + 8), 1)
            ext[f, 1, r : r + n, :] = jnp.where(sides, moved, 1.0 if f == HELM else 0.0)

    for r, n in chunks:
        at = slice(r, r + n)
        for t, (c, e, w, nn, s) in enumerate(beside(ext.at[WET], r, n)):
            four = [jnp.minimum(c, o) for o in (e, w, nn, s)]
            total = ext[HELM, t, at, :] + four[0] + four[1] + four[2] + four[3]
            inverse = 1.0 / total
            rdiag[t, at, :] = inverse
            if t == 0:
                diag[at, :] = total
            for k in range(4):
                face[k, t, at, :] = four[k]
                gain[k, t, at, :] = four[k] * inverse
    for k, (bar, hat) in enumerate(((UB, UH), (VB, VH))):
        for r, n in chunks:
            at = slice(r, r + n)
            for t, (c, *others) in enumerate(beside(ext.at[bar], r, n)):
                spread = sum(face[i, t, at, :] * (o - c) for i, o in enumerate(others))
                flow[k, t, at, :] = ext[WET, t, at, :] * (ext[hat, t, at, :] + 0.1 * spread)

    def image(t, at, others):
        return sum(gain[i, t, at, :] * o for i, o in enumerate(others))

    for r, n in chunks:
        at = slice(r, r + n)
        x = beside(ext.at[X0], r, n)
        for t, (ef, efw) in enumerate(west_of(flow.at[0], r, n)):
            nf, nfs = flow[1, t, at, :], flow[1, t, r - 1 : r - 1 + n, :]
            force = jnp.where(ext[WET, t, at, :] > 0.0, (efw - ef) + (nfs - nf), 0.0)
            c, *others = x[t]
            basis[0, t, at, :] = force * rdiag[t, at, :] + (image(t, at, others) - c)
    for k in range(3):
        for r, n in chunks:
            at = slice(r, r + n)
            for t, (c, *others) in enumerate(beside(basis.at[k], r, n)):
                value = image(t, at, others)
                if k:
                    value = 2.0 * value - basis[k - 1, t, at, :]
                basis[k + 1, t, at, :] = value
    sums = [jnp.zeros((8, COLS), F32) for _ in range(8)]
    for b in range(BLOCKS):
        r = OFF + b * BY
        at = slice(r, r + BY)
        ((c, *others),) = beside(basis.at[3], r, BY, both=False)
        t4 = 2.0 * image(0, at, others) - basis[2, 0, at, :]
        vectors = [basis[k, 0, at, :] for k in range(3)] + [c, t4]
        for k in range(4):
            weighted = diag[at, :] * vectors[k]
            sums[2 * k] = sums[2 * k] + eights(weighted * vectors[k])
            sums[2 * k + 1] = sums[2 * k + 1] + eights(weighted * vectors[k + 1])

    rows8 = lax.broadcasted_iota(jnp.int32, (8, COLS), 0)
    mat = jnp.zeros((8, COLS), F32)
    for k in range(8):
        mat = jnp.where(rows8 == k, jnp.sum(sums[k], axis=0, keepdims=True), mat)
    total = jnp.broadcast_to(jnp.sum(mat, axis=1, keepdims=True), (8, COLS))
    row = jnp.sum(jnp.where(lanes(8) == rows8, total, 0.0), axis=0, keepdims=True)

    def level_updates():
        for copy in outer:
            copy.wait_recv()
        even = lax.rem(lax.broadcasted_iota(jnp.int32, (2 * PLANES, COLS), 0), 2) == 0
        for c in range(3):
            cols = slice(128 * c, 128 * (c + 1))
            from_w, from_e = rim_got[0, :, cols], rim_got[1, :, cols]
            up, down = pltpu.roll(from_e, 2 * PLANES - 1, 0), pltpu.roll(from_w, 1, 0)
            rim_m[0 : 2 * PLANES, :] = jnp.where(even, up, down)
            rim_back[128 * c : 128 * (c + 1), :] = rim_m[...].T
        for q in range(PLANES):
            uvt[q, 7:8, :] = edge_got[0, q : q + 1, :]
            uvt[q, 8 + ROWS : 9 + ROWS, :] = edge_got[1, q : q + 1, :]
        first, last = lanes(BY) == 0, lanes(BY) == COLS - 1

        for b in range(BLOCKS):
            r = b * BY
            rows = slice(r, r + BY)
            at = slice(OFF + r, OFF + r + BY)
            on = act[b : b + 1, :]
            ocean = land[rows, :].astype(F32)
            keep = on * ocean
            off = 1.0 - on
            cor = coriolis(b)
            faces = [face[k, 0, at, :] for k in range(4)]
            rim_row = rim_back[rows, :]

            def around(q):
                c = uvt[q, 8 + r : 8 + r + BY, :]
                side = pltpu.roll(rim_row, COLS - 1 - 2 * q, 1)
                e = jnp.where(last, side, pltpu.roll(c, COLS - 1, 1))
                w = jnp.where(first, side, pltpu.roll(c, 1, 1))
                return c, e, w, uvt[q, 9 + r : 9 + r + BY, :], uvt[q, 7 + r : 7 + r + BY, :]

            def raw(q0):
                out, keepers = [], []
                for k in range(LEVELS):
                    c, *others = around(q0 + k)
                    spread = sum(faces[i] * (o - c) for i, o in enumerate(others))
                    mix = jnp.zeros_like(c)
                    if k < LEVELS - 1:
                        mix = mix + (uvt[q0 + k + 1, 8 + r : 8 + r + BY, :] - c)
                    if k > 0:
                        mix = mix - (c - uvt[q0 + k - 1, 8 + r : 8 + r + BY, :])
                    out.append((c, 0.5 * mix + 0.5 * spread, others))
                return out

            for k, (c, tend, _) in enumerate(raw(0)):
                star = c + 0.2 * (tend + cor * uvt[LEVELS + k, 8 + r : 8 + r + BY, :])
                u_out[k, rows, :] = keep * star + off * c
            for k, (c, tend, _) in enumerate(raw(LEVELS)):
                star = c + 0.2 * (tend - cor * uvt[k, 8 + r : 8 + r + BY, :])
                v_out[k, rows, :] = keep * star + off * c
            for k, (c, tend, (e, w, nn, s)) in enumerate(raw(2 * LEVELS)):
                uk = uvt[k, 8 + r : 8 + r + BY, :]
                vk = uvt[LEVELS + k, 8 + r : 8 + r + BY, :]
                star = c + 0.2 * (tend - 0.5 * (uk * (e - w) + vk * (nn - s)))
                t_out[k, rows, :] = keep * star + off * c

    pl.semaphore_wait(known, len(greeted))
    for s, kind in enumerate(RED_STAGES):
        landing = red[s]
        part[s] = row
        for j, peer in enumerate(peers(kind)):
            pltpu.make_async_remote_copy(
                src_ref=part.at[s], dst_ref=landing.at[j], send_sem=rsend_sem.at[s], recv_sem=rrecv_sem.at[s],
                device_id=peer, device_id_type=MESH,
            ).start()
        if s == 0:
            level_updates()
        every = pltpu.make_async_remote_copy(
            src_ref=landing, dst_ref=landing, send_sem=rsend_sem.at[s], recv_sem=rrecv_sem.at[s],
            device_id=(east, gy), device_id_type=MESH,
        )
        every.wait_recv()
        row = row + jnp.sum(landing[...], axis=0)

    c = coefficients([jnp.broadcast_to(row[:, k : k + 1], (1, COLS)) for k in range(8)])

    def answer(t, at):
        x = ext[X0, t, at, :]
        for k in range(4):
            x = x + c[k] * basis[k, t, at, :]
        return x

    for b in range(BLOCKS):
        rows = slice(b * BY, (b + 1) * BY)
        at = slice(OFF + b * BY, OFF + (b + 1) * BY)
        x0, x1 = answer(0, at), answer(1, at)
        up = answer(0, slice(at.start + 1, at.stop + 1))
        right = jnp.where(lanes(BY) == COLS - 1, pltpu.roll(x1, COLS - 1, 1), pltpu.roll(x0, COLS - 1, 1))
        keep = act[b : b + 1, :] * land[rows, :].astype(F32)
        p_out[rows, :] = x0
        grad_x, grad_y = keep * (right - x0), keep * (up - x0)
        for k in range(LEVELS):
            u_out[k, rows, :] = u_out[k, rows, :] - grad_x
            v_out[k, rows, :] = v_out[k, rows, :] - grad_y

    for copy in halo + outer:
        copy.wait_send()
    for s in range(len(RED_STAGES)):
        pltpu.make_async_remote_copy(
            src_ref=red[s], dst_ref=red[s], send_sem=rsend_sem.at[s], recv_sem=rrecv_sem.at[s],
            device_id=(east, gy), device_id_type=MESH,
        ).wait_send()


def emit_kernel(*refs):
    n = (len(refs) - 1) // 2
    sem = refs[-1]
    copies = [pltpu.make_async_copy(refs[i], refs[n + i], sem.at[i]) for i in range(n)]
    for copy in copies:
        copy.start()
    for copy in copies:
        copy.wait()


def on_device(*args):
    args = args[:7] + (args[7].T, args[8].T)
    args = [pltpu.with_memory_space_constraint(x, pltpu.HBM) for x in args]
    vmem, hbm = pltpu.VMEM, pltpu.HBM
    three = jax.ShapeDtypeStruct((LEVELS, ROWS, COLS), F32)
    two = jax.ShapeDtypeStruct((ROWS, COLS), F32)
    shapes = (three, three, three, two)
    tiles = (2, EXT_ROWS, COLS)
    scratch = [
        vmem((PLANES, ROWS + 16, COLS), F32),
        vmem((ROWS, COLS), F32),
        vmem((ROWS, COLS), F32),
        vmem((ROWS, COLS), jnp.int32),
        vmem((NX_DEV, NBY), jnp.int32),
        vmem((NX_DEV, NBY), jnp.int32),
        vmem((BLOCKS, COLS), F32),
        vmem((BLOCKS, COLS), F32),
        vmem((FIELDS,) + tiles, F32),
        vmem((384, COLS), F32),
        vmem((8, 2, 8, 384), F32),
        vmem((8, 2, 8, 384), F32),
        vmem((ROWS + 16, COLS), F32),
        vmem((4, 8, COLS), F32),
        vmem((384, COLS), F32),
        vmem((2 * PLANES, 384), F32),
        vmem((2, 2 * PLANES, 384), F32),
        vmem((COLS, COLS), F32),
        vmem((384, COLS), F32),
        vmem((2, 16, COLS), F32),
        vmem((2, 16, COLS), F32),
        vmem((4,) + tiles, F32),
        vmem(tiles, F32),
        vmem((4,) + tiles, F32),
        vmem((EXT_ROWS, COLS), F32),
        vmem((2,) + tiles, F32),
        vmem((4,) + tiles, F32),
        vmem((len(RED_STAGES), 1, COLS), F32),
        pltpu.SemaphoreType.DMA((9,)),
        pltpu.SemaphoreType.DMA((12,)),
        pltpu.SemaphoreType.DMA((12,)),
        pltpu.SemaphoreType.DMA((len(RED_STAGES),)),
        pltpu.SemaphoreType.DMA((len(RED_STAGES),)),
        pltpu.SemaphoreType.REGULAR,
    ] + [vmem((COUNT[kind], 1, COLS), F32) for kind in RED_STAGES]
    out = pl.pallas_call(
        ocean_kernel,
        out_shape=[vmem(x.shape, x.dtype) for x in shapes],
        in_specs=[pl.BlockSpec(memory_space=hbm)] * 9,
        out_specs=[pl.BlockSpec(memory_space=vmem)] * 4,
        scratch_shapes=scratch,
        compiler_params=pltpu.CompilerParams(
            collective_id=0, has_side_effects=True, vmem_limit_bytes=VMEM_LIMIT
        ),
        name="ocean",
    )(*args)
    return pl.pallas_call(
        emit_kernel,
        out_shape=shapes,
        in_specs=[pl.BlockSpec(memory_space=vmem)] * 4,
        out_specs=[pl.BlockSpec(memory_space=hbm)] * 4,
        scratch_shapes=[pltpu.SemaphoreType.DMA((4,))],
        compiler_params=pltpu.CompilerParams(vmem_limit_bytes=8 * 1024 * 1024),
        name="emit",
    )(*out)


def solution(mesh):
    wide, flat = P(None, "gy", "gx"), P("gy", "gx")
    return jax.shard_map(
        on_device,
        mesh=mesh,
        in_specs=(wide, wide, wide, flat, flat, flat, flat, P(), P()),
        out_specs=(wide, wide, wide, flat),
        check_vma=False,
    )
```

```python
import functools

import jax
import jax.numpy as jnp
from jax import lax
from jax.experimental import pallas as pl
from jax.experimental.pallas import tpu as pltpu
from jax.sharding import PartitionSpec as P

MESH = pl.DeviceIdType.MESH
F32 = jnp.float32

LEVELS, ROWS, COLS, BY, NY = 4, 320, 128, 40, 2560
BLOCKS, NBY = ROWS // BY, 64
THICK = [(2 * k + 1) / (LEVELS * LEVELS) for k in range(LEVELS)]

OFF = 16
EXT_ROWS = ROWS + 2 * OFF
LOW, HIGH = OFF - 8, OFF + ROWS + 8
STEP = 48
FIELDS = 7
WET, HELM, X0, UB, UH, VB, VH = range(FIELDS)
PLANES = 3 * LEVELS
NX_DEV, NY_DEV = 16, 8

VMEM_LIMIT = 24 * 1024 * 1024
TO_EAST = (6, 4, 5, 6, 5, 5, 4)
TO_WEST = (5, 4, 5, 5, 4, 5, 4)
EAST_ROWS, WEST_ROWS = 40, 32
RED_STAGES = ("all",)


def peers(kind):
    gx, gy = lax.axis_index("gx"), lax.axis_index("gy")
    if kind == "halo":
        return [
            (lax.rem(gx + i, NX_DEV), lax.rem(gy + j, NY_DEV))
            for i in (0, 1, NX_DEV - 1)
            for j in (0, 1, NY_DEV - 1)
            if i or j
        ]
    if kind == "plane":
        base = gx // 4 * 4
        return [
            (base + lax.rem(lax.rem(gx, 4) + i, 4), lax.rem(gy + j, NY_DEV))
            for i in range(4)
            for j in range(NY_DEV)
            if i or j
        ]
    if kind == "z":
        return [(lax.rem(gx + 4 * j, NX_DEV), gy) for j in range(1, 4)]
    return [
        (lax.rem(gx + i, NX_DEV), lax.rem(gy + j, NY_DEV))
        for i in range(NX_DEV)
        for j in range(NY_DEV)
        if i or j
    ]


def nearby(step):
    gx, gy = lax.axis_index("gx"), lax.axis_index("gy")
    z, y, core = gx // 4, lax.rem(gx, 4), lax.rem(gy, 2)
    return [
        (lax.rem(z + i, 4) * 4 + lax.rem(y + j, 4), gy + 2 * step if c == 0 else gy + 2 * step + 1 - 2 * core)
        for i in (0, 1, 3)
        for j in (0, 1, 3)
        for c in (0, 1)
        if i or j or c or step
    ]


COUNT = {"all": 127, "plane": 31, "z": 3}


def lanes(rows):
    return lax.broadcasted_iota(jnp.int32, (rows, COLS), 1)


def beside(ref, r, n, both=True):
    lane = lanes(n)
    first, last = lane == 0, lane == COLS - 1
    c0, c1 = ref[0, r : r + n, :], ref[1, r : r + n, :]
    e0, e1 = pltpu.roll(c0, COLS - 1, 1), pltpu.roll(c1, COLS - 1, 1)
    w0, w1 = pltpu.roll(c0, 1, 1), pltpu.roll(c1, 1, 1)
    out = [
        (
            c0,
            jnp.where(last, e1, e0),
            jnp.where(first, w1, w0),
            ref[0, r + 1 : r + 1 + n, :],
            ref[0, r - 1 : r - 1 + n, :],
        )
    ]
    if both:
        out.append(
            (
                c1,
                jnp.where(last, e0, e1),
                jnp.where(first, w0, w1),
                ref[1, r + 1 : r + 1 + n, :],
                ref[1, r - 1 : r - 1 + n, :],
            )
        )
    return out


def west_of(ref, r, n):
    first = lanes(n) == 0
    c0, c1 = ref[0, r : r + n, :], ref[1, r : r + n, :]
    w0, w1 = pltpu.roll(c0, 1, 1), pltpu.roll(c1, 1, 1)
    return (c0, jnp.where(first, w1, w0)), (c1, jnp.where(first, w0, w1))


def eights(x):
    return jnp.sum(x.reshape(x.shape[0] // 8, 8, COLS), axis=0)


def coefficients(sums):
    m = [sums[0], sums[1]]
    for k in range(2, 8):
        m.append(2.0 * sums[k] - m[k % 2])
    g = [[0.5 * (m[i + j] + m[abs(i - j)]) for j in range(5) if i + j < 8] for i in range(4)]

    def image(i, j):
        if j == 0:
            return g[i][1]
        return 0.5 * (g[i][j + 1] + g[i][j - 1])

    a = [[g[i][j] - image(i, j) for j in range(i + 1)] for i in range(4)]
    low = [[None] * 4 for _ in range(4)]
    inv, piv = [], []
    for j in range(4):
        pivot = a[j][j]
        for k in range(j):
            pivot = pivot - low[j][k] * low[j][k] * piv[k]
        good = pivot > 1e-6 * a[j][j]
        piv.append(jnp.where(good, pivot, 0.0))
        inv.append(jnp.where(good, 1.0 / jnp.where(good, pivot, 1.0), 0.0))
        for i in range(j + 1, 4):
            s = a[i][j]
            for k in range(j):
                s = s - low[i][k] * low[j][k] * piv[k]
            low[i][j] = s * inv[j]
    y = []
    for i in range(4):
        s = m[i]
        for k in range(i):
            s = s - low[i][k] * y[k]
        y.append(s)
    c = [None] * 4
    for i in reversed(range(4)):
        s = y[i] * inv[i]
        for k in range(i + 1, 4):
            s = s - low[k][i] * c[k]
        c[i] = s
    return c


def ocean_kernel(
    u_hbm, v_hbm, t_hbm, p_hbm, depth_hbm, helm_hbm, land_hbm, clinic_hbm, tropic_hbm,
    u_out, v_out, t_out, p_out,
    uvt, pold, depth, land, cmap, tmap, act, dom,
    ext, pack, pack_t, for_e, for_w, from_w, from_e, got_t, got, corner,
    rim, rim_t, rim_got, rim_m, rim_back, edge, edge_got,
    face, rdiag, gain, diag, flow, basis, part,
    in_sem, send_sem, recv_sem, rsend_sem, rrecv_sem, known, far, *red,
):
    gx, gy = lax.axis_index("gx"), lax.axis_index("gy")
    east, west = lax.rem(gx + 1, NX_DEV), lax.rem(gx + NX_DEV - 1, NX_DEV)
    north, south = lax.rem(gy + 1, NY_DEV), lax.rem(gy + NY_DEV - 1, NY_DEV)
    own = pl.ds(OFF, ROWS)

    loads = [
        pltpu.make_async_copy(u_hbm, uvt.at[0:4, 8 : 8 + ROWS, :], in_sem.at[0]),
        pltpu.make_async_copy(v_hbm, uvt.at[4:8, 8 : 8 + ROWS, :], in_sem.at[1]),
        pltpu.make_async_copy(p_hbm, pold, in_sem.at[2]),
        pltpu.make_async_copy(depth_hbm, depth, in_sem.at[3]),
        pltpu.make_async_copy(land_hbm, land, in_sem.at[4]),
        pltpu.make_async_copy(clinic_hbm, cmap, in_sem.at[5]),
        pltpu.make_async_copy(tropic_hbm, tmap, in_sem.at[6]),
        pltpu.make_async_copy(helm_hbm, ext.at[HELM, 0, OFF : OFF + ROWS, :], in_sem.at[7]),
        pltpu.make_async_copy(t_hbm, uvt.at[8:12, 8 : 8 + ROWS, :], in_sem.at[8]),
    ]
    for load in loads:
        load.start()

    barrier = pltpu.get_barrier_semaphore()
    has_n, has_s = gy < NY_DEV - 1, gy > 0
    up_x, down_x = gy < NY_DEV - 2, gy > 1

    def greet(sem):
        for step, there in ((0, None), (1, up_x), (-1, down_x)):

            def tell(step=step):
                for peer in nearby(step):
                    pl.semaphore_signal(sem, inc=1, device_id=peer, device_id_type=MESH)

            tell() if there is None else pl.when(there)(tell)

    def hear(sem):
        inner = lax.rem((gy // 2 + 1) // 2, 2)
        pl.semaphore_wait(sem, 35 + 18 * inner)

    greet(barrier)

    pack[ROWS:, :] = jnp.zeros((pack.shape[0] - ROWS, COLS), F32)
    for load in loads[:8]:
        load.wait()

    shape = (NX_DEV, NBY)
    mine = lax.broadcasted_iota(jnp.int32, shape, 0) == gx
    shape = (BLOCKS, NBY)
    wanted = lax.broadcasted_iota(jnp.int32, shape, 1) == lax.broadcasted_iota(jnp.int32, shape, 0) + gy * BLOCKS

    def per_block(flags):
        line = jnp.sum(jnp.where(mine, flags, 0.0), axis=0, keepdims=True)
        column = jnp.sum(jnp.where(wanted, line, 0.0), axis=1, keepdims=True)
        return jnp.broadcast_to(column, (BLOCKS, COLS))

    act[...] = per_block(cmap[...].astype(F32))
    dom[...] = per_block(jnp.where(tmap[...] >= 0, 1.0, 0.0))

    def coriolis(b):
        row = lax.broadcasted_iota(jnp.int32, (BY, COLS), 0) + (gy * ROWS + b * BY)
        return 0.2 + 0.6 * ((row.astype(F32) + 0.5) / NY)

    group = lanes(BY) // 16
    for b in range(BLOCKS):
        r = b * BY
        rows = slice(r, r + BY)
        solve = land[rows, :].astype(F32) * dom[b : b + 1, :]
        wet = depth[rows, :] * solve
        u = [uvt[k, 8 + r : 8 + r + BY, :] for k in range(LEVELS)]
        v = [uvt[LEVELS + k, 8 + r : 8 + r + BY, :] for k in range(LEVELS)]
        u_bar = sum(THICK[k] * u[k] for k in range(LEVELS))
        v_bar = sum(THICK[k] * v[k] for k in range(LEVELS))
        cor = 0.2 * coriolis(b)
        mix = 0.1 * (THICK[1] - THICK[0])
        u_hat = u_bar + mix * (u[0] - u[3]) + cor * v_bar
        v_hat = v_bar + mix * (v[0] - v[3]) - cor * u_bar
        fields = [wet, ext[HELM, 0, OFF + r : OFF + r + BY, :], solve * pold[rows, :], u_bar, u_hat, v_bar, v_hat]
        packed = None
        for f, value in enumerate(fields):
            if f != HELM:
                ext[f, 0, OFF + r : OFF + r + BY, :] = value
            moved = pltpu.roll(value, 8 + 16 * f, 1)
            packed = moved if packed is None else jnp.where(group == f, moved, packed)
        pack[rows, :] = packed
    for c in range(3):
        cols = slice(128 * c, 128 * (c + 1))
        pack_t[...] = pack[cols, :].T
        at_e = at_w = 0
        for f in range(FIELDS):
            ne, nw = TO_EAST[f], TO_WEST[f]
            for_e[at_e : at_e + ne, cols] = pack_t[16 * f + 8 - ne : 16 * f + 8, :]
            for_w[at_w : at_w + nw, cols] = pack_t[16 * f + 8 : 16 * f + 8 + nw, :]
            at_e, at_w = at_e + ne, at_w + nw

    routes = {
        0: (for_e, from_w, (east, gy), None),
        1: (for_w, from_e, (west, gy), None),
        2: (ext.at[:, 0, OFF + ROWS - 8 : OFF + ROWS, :], ext.at[:, 0, LOW:OFF, :], (gx, north), "n"),
        3: (ext.at[:, 0, OFF : OFF + 8, :], ext.at[:, 0, OFF + ROWS : HIGH, :], (gx, south), "s"),
        4: (pack.at[ROWS - 8 : ROWS, :], corner.at[0], (east, north), "n"),
        5: (pack.at[ROWS - 8 : ROWS, :], corner.at[1], (west, north), "n"),
        6: (pack.at[0:8, :], corner.at[2], (east, south), "s"),
        7: (pack.at[0:8, :], corner.at[3], (west, south), "s"),
        8: (rim_t, rim_got.at[0], (east, gy), None),
        9: (rim_t, rim_got.at[1], (west, gy), None),
        10: (edge.at[1], edge_got.at[0], (gx, north), "n"),
        11: (edge.at[0], edge_got.at[1], (gx, south), "s"),
    }
    HALO, OUTER = range(8), range(8, 12)

    def transfer(which, what):
        def go(keys):
            for k in keys:
                src, dst, to, _ = routes[k]
                copy = pltpu.make_async_remote_copy(
                    src_ref=src, dst_ref=dst, send_sem=send_sem.at[k], recv_sem=recv_sem.at[k],
                    device_id=to, device_id_type=MESH,
                )
                getattr(copy, what)()

        go([k for k in which if routes[k][3] is None])
        for way, other in (("n", "s"), ("s", "n")):
            there = {"n": has_n, "s": has_s}[other if what == "wait_recv" else way]
            pl.when(there)(functools.partial(go, [k for k in which if routes[k][3] == way]))

    hear(barrier)
    greet(known)
    transfer(HALO, "start")

    loads[8].wait()
    pair = lanes(BY) // 2
    for b in range(BLOCKS):
        r = b * BY
        packed = None
        for q in range(PLANES):
            moved = pltpu.roll(uvt[q, 8 + r : 8 + r + BY, :], 2 * q + 1, 1)
            packed = moved if packed is None else jnp.where(pair == q, moved, packed)
        rim[r : r + BY, :] = packed
    rim[ROWS:, :] = jnp.zeros((rim.shape[0] - ROWS, COLS), F32)
    for c in range(3):
        rim_t[:, 128 * c : 128 * (c + 1)] = rim[128 * c : 128 * (c + 1), :].T[: 2 * PLANES, :]
    for q in range(PLANES):
        edge[0, q : q + 1, :] = uvt[q, 8 : 9, :]
        edge[1, q : q + 1, :] = uvt[q, 7 + ROWS : 8 + ROWS, :]
    transfer(OUTER, "start")
    transfer(HALO, "wait_recv")
    hear(known)

    @pl.when((gy // 2 == 1) | (gy // 2 == 2))
    def _():
        pl.semaphore_signal(
            far, inc=1, device_id=(gx, gy + 4 * lax.rem(gy // 2 - 1, 2) - 2), device_id_type=MESH
        )

    low_half = lax.rem(lanes(8), 16) < 8
    nothing = jnp.where(lanes(8) // 16 == HELM, 1.0, 0.0)
    for c in range(3):
        cols = slice(128 * c, 128 * (c + 1))
        at_w = at_e = 0
        for f in range(FIELDS):
            nw, ne = TO_EAST[f], TO_WEST[f]
            got_t[16 * f + 8 - nw : 16 * f + 8, :] = from_w[at_w : at_w + nw, cols]
            got_t[16 * f + 8 : 16 * f + 8 + ne, :] = from_e[at_e : at_e + ne, cols]
            at_w, at_e = at_w + nw, at_e + ne
        block = got_t[...].T
        n = min(128, ROWS - 128 * c)
        got[8 + 128 * c : 8 + 128 * c + n, :] = block[:n, :]
    for k, there, first, halo_at in ((0, has_s, 0, LOW), (2, has_n, 8 + ROWS, OFF + ROWS)):

        @pl.when(there)
        def _(k=k, first=first):
            got[first : first + 8, :] = jnp.where(low_half, corner[k], corner[k + 1])

        @pl.when(jnp.logical_not(there))
        def _(k=k, first=first, halo_at=halo_at):
            got[first : first + 8, :] = nothing
            edge_got[k // 2] = jnp.zeros((16, COLS), F32)
            for f in range(FIELDS):
                ext[f, 0, halo_at : halo_at + 8, :] = jnp.full((8, COLS), 1.0 if f == HELM else 0.0, F32)

    chunks = [(r, STEP) for r in range(LOW, HIGH, STEP)]
    lane = lanes(STEP)
    for r, n in chunks:
        packed = got[r - LOW : r - LOW + n, :]
        for f in range(FIELDS):
            moved = pltpu.roll(packed, COLS - (16 * f + 8), 1)
            came = (lane < TO_WEST[f]) | (lane >= COLS - TO_EAST[f])
            ext[f, 1, r : r + n, :] = jnp.where(came, moved, 1.0 if f == HELM else 0.0)

    for r, n in chunks:
        at = slice(r, r + n)
        for t, (c, e, w, nn, s) in enumerate(beside(ext.at[WET], r, n)):
            four = [jnp.minimum(c, o) for o in (e, w, nn, s)]
            total = ext[HELM, t, at, :] + four[0] + four[1] + four[2] + four[3]
            inverse = 1.0 / total
            rdiag[t, at, :] = inverse
            if t == 0:
                diag[at, :] = total
            for k in range(4):
                face[k, t, at, :] = four[k]
                gain[k, t, at, :] = four[k] * inverse
    for k, (bar, hat) in enumerate(((UB, UH), (VB, VH))):
        for r, n in chunks:
            at = slice(r, r + n)
            for t, (c, *others) in enumerate(beside(ext.at[bar], r, n)):
                spread = sum(face[i, t, at, :] * (o - c) for i, o in enumerate(others))
                flow[k, t, at, :] = ext[WET, t, at, :] * (ext[hat, t, at, :] + 0.1 * spread)

    def image(t, at, others):
        return sum(gain[i, t, at, :] * o for i, o in enumerate(others))

    for r, n in chunks:
        at = slice(r, r + n)
        x = beside(ext.at[X0], r, n)
        for t, (ef, efw) in enumerate(west_of(flow.at[0], r, n)):
            nf, nfs = flow[1, t, at, :], flow[1, t, r - 1 : r - 1 + n, :]
            force = jnp.where(ext[WET, t, at, :] > 0.0, (efw - ef) + (nfs - nf), 0.0)
            c, *others = x[t]
            basis[0, t, at, :] = force * rdiag[t, at, :] + (image(t, at, others) - c)
    for k in range(3):
        for r, n in chunks:
            at = slice(r, r + n)
            for t, (c, *others) in enumerate(beside(basis.at[k], r, n)):
                value = image(t, at, others)
                if k:
                    value = 2.0 * value - basis[k - 1, t, at, :]
                basis[k + 1, t, at, :] = value
    sums = [jnp.zeros((8, COLS), F32) for _ in range(8)]
    for b in range(BLOCKS):
        r = OFF + b * BY
        at = slice(r, r + BY)
        ((c, *others),) = beside(basis.at[3], r, BY, both=False)
        t4 = 2.0 * image(0, at, others) - basis[2, 0, at, :]
        vectors = [basis[k, 0, at, :] for k in range(3)] + [c, t4]
        for k in range(4):
            weighted = diag[at, :] * vectors[k]
            sums[2 * k] = sums[2 * k] + eights(weighted * vectors[k])
            sums[2 * k + 1] = sums[2 * k + 1] + eights(weighted * vectors[k + 1])

    rows8 = lax.broadcasted_iota(jnp.int32, (8, COLS), 0)
    mat = jnp.zeros((8, COLS), F32)
    for k in range(8):
        mat = jnp.where(rows8 == k, jnp.sum(sums[k], axis=0, keepdims=True), mat)
    total = jnp.broadcast_to(jnp.sum(mat, axis=1, keepdims=True), (8, COLS))
    row = jnp.sum(jnp.where(lanes(8) == rows8, total, 0.0), axis=0, keepdims=True)

    def level_updates():
        transfer(OUTER, "wait_recv")
        even = lax.rem(lax.broadcasted_iota(jnp.int32, (2 * PLANES, COLS), 0), 2) == 0
        for c in range(3):
            cols = slice(128 * c, 128 * (c + 1))
            from_w, from_e = rim_got[0, :, cols], rim_got[1, :, cols]
            up, down = pltpu.roll(from_e, 2 * PLANES - 1, 0), pltpu.roll(from_w, 1, 0)
            rim_m[0 : 2 * PLANES, :] = jnp.where(even, up, down)
            rim_back[128 * c : 128 * (c + 1), :] = rim_m[...].T
        for q in range(PLANES):
            uvt[q, 7:8, :] = edge_got[0, q : q + 1, :]
            uvt[q, 8 + ROWS : 9 + ROWS, :] = edge_got[1, q : q + 1, :]
        first, last = lanes(BY) == 0, lanes(BY) == COLS - 1

        for b in range(BLOCKS):
            r = b * BY
            rows = slice(r, r + BY)
            at = slice(OFF + r, OFF + r + BY)
            on = act[b : b + 1, :]
            ocean = land[rows, :].astype(F32)
            keep = on * ocean
            off = 1.0 - on
            cor = coriolis(b)
            faces = [face[k, 0, at, :] for k in range(4)]
            rim_row = rim_back[rows, :]

            def around(q):
                c = uvt[q, 8 + r : 8 + r + BY, :]
                side = pltpu.roll(rim_row, COLS - 1 - 2 * q, 1)
                e = jnp.where(last, side, pltpu.roll(c, COLS - 1, 1))
                w = jnp.where(first, side, pltpu.roll(c, 1, 1))
                return c, e, w, uvt[q, 9 + r : 9 + r + BY, :], uvt[q, 7 + r : 7 + r + BY, :]

            def raw(q0):
                out, keepers = [], []
                for k in range(LEVELS):
                    c, *others = around(q0 + k)
                    spread = sum(faces[i] * (o - c) for i, o in enumerate(others))
                    mix = jnp.zeros_like(c)
                    if k < LEVELS - 1:
                        mix = mix + (uvt[q0 + k + 1, 8 + r : 8 + r + BY, :] - c)
                    if k > 0:
                        mix = mix - (c - uvt[q0 + k - 1, 8 + r : 8 + r + BY, :])
                    out.append((c, 0.5 * mix + 0.5 * spread, others))
                return out

            for k, (c, tend, _) in enumerate(raw(0)):
                star = c + 0.2 * (tend + cor * uvt[LEVELS + k, 8 + r : 8 + r + BY, :])
                u_out[k, rows, :] = keep * star + off * c
            for k, (c, tend, _) in enumerate(raw(LEVELS)):
                star = c + 0.2 * (tend - cor * uvt[k, 8 + r : 8 + r + BY, :])
                v_out[k, rows, :] = keep * star + off * c
            for k, (c, tend, (e, w, nn, s)) in enumerate(raw(2 * LEVELS)):
                uk = uvt[k, 8 + r : 8 + r + BY, :]
                vk = uvt[LEVELS + k, 8 + r : 8 + r + BY, :]
                star = c + 0.2 * (tend - 0.5 * (uk * (e - w) + vk * (nn - s)))
                t_out[k, rows, :] = keep * star + off * c

    @pl.when((gy // 2 == 0) | (gy // 2 == 3))
    def _():
        pl.semaphore_wait(far, 1)

    for s, kind in enumerate(RED_STAGES):
        landing = red[s]
        part[s] = row
        for j, peer in enumerate(peers(kind)):
            pltpu.make_async_remote_copy(
                src_ref=part.at[s], dst_ref=landing.at[j], send_sem=rsend_sem.at[s], recv_sem=rrecv_sem.at[s],
                device_id=peer, device_id_type=MESH,
            ).start()
        if s == 0:
            level_updates()
        every = pltpu.make_async_remote_copy(
            src_ref=landing, dst_ref=landing, send_sem=rsend_sem.at[s], recv_sem=rrecv_sem.at[s],
            device_id=(east, gy), device_id_type=MESH,
        )
        every.wait_recv()
        row = row + jnp.sum(landing[...], axis=0)

    c = coefficients([jnp.broadcast_to(row[:, k : k + 1], (1, COLS)) for k in range(8)])

    def answer(t, at):
        x = ext[X0, t, at, :]
        for k in range(4):
            x = x + c[k] * basis[k, t, at, :]
        return x

    for b in range(BLOCKS):
        rows = slice(b * BY, (b + 1) * BY)
        at = slice(OFF + b * BY, OFF + (b + 1) * BY)
        x0, x1 = answer(0, at), answer(1, at)
        up = answer(0, slice(at.start + 1, at.stop + 1))
        right = jnp.where(lanes(BY) == COLS - 1, pltpu.roll(x1, COLS - 1, 1), pltpu.roll(x0, COLS - 1, 1))
        keep = act[b : b + 1, :] * land[rows, :].astype(F32)
        p_out[rows, :] = x0
        grad_x, grad_y = keep * (right - x0), keep * (up - x0)
        for k in range(LEVELS):
            u_out[k, rows, :] = u_out[k, rows, :] - grad_x
            v_out[k, rows, :] = v_out[k, rows, :] - grad_y

    transfer(range(12), "wait_send")
    for s in range(len(RED_STAGES)):
        pltpu.make_async_remote_copy(
            src_ref=red[s], dst_ref=red[s], send_sem=rsend_sem.at[s], recv_sem=rrecv_sem.at[s],
            device_id=(east, gy), device_id_type=MESH,
        ).wait_send()


def emit_kernel(*refs):
    n = (len(refs) - 1) // 2
    sem = refs[-1]
    copies = [pltpu.make_async_copy(refs[i], refs[n + i], sem.at[i]) for i in range(n)]
    for copy in copies:
        copy.start()
    for copy in copies:
        copy.wait()


def on_device(*args):
    args = args[:7] + (args[7].T, args[8].T)
    args = [pltpu.with_memory_space_constraint(x, pltpu.HBM) for x in args]
    vmem, hbm = pltpu.VMEM, pltpu.HBM
    three = jax.ShapeDtypeStruct((LEVELS, ROWS, COLS), F32)
    two = jax.ShapeDtypeStruct((ROWS, COLS), F32)
    shapes = (three, three, three, two)
    tiles = (2, EXT_ROWS, COLS)
    scratch = [
        vmem((PLANES, ROWS + 16, COLS), F32),
        vmem((ROWS, COLS), F32),
        vmem((ROWS, COLS), F32),
        vmem((ROWS, COLS), jnp.int32),
        vmem((NX_DEV, NBY), jnp.int32),
        vmem((NX_DEV, NBY), jnp.int32),
        vmem((BLOCKS, COLS), F32),
        vmem((BLOCKS, COLS), F32),
        vmem((FIELDS,) + tiles, F32),
        vmem((384, COLS), F32),
        vmem((COLS, COLS), F32),
        vmem((EAST_ROWS, 384), F32),
        vmem((WEST_ROWS, 384), F32),
        vmem((EAST_ROWS, 384), F32),
        vmem((WEST_ROWS, 384), F32),
        vmem((COLS, COLS), F32),
        vmem((ROWS + 16, COLS), F32),
        vmem((4, 8, COLS), F32),
        vmem((384, COLS), F32),
        vmem((2 * PLANES, 384), F32),
        vmem((2, 2 * PLANES, 384), F32),
        vmem((COLS, COLS), F32),
        vmem((384, COLS), F32),
        vmem((2, 16, COLS), F32),
        vmem((2, 16, COLS), F32),
        vmem((4,) + tiles, F32),
        vmem(tiles, F32),
        vmem((4,) + tiles, F32),
        vmem((EXT_ROWS, COLS), F32),
        vmem((2,) + tiles, F32),
        vmem((4,) + tiles, F32),
        vmem((len(RED_STAGES), 1, COLS), F32),
        pltpu.SemaphoreType.DMA((9,)),
        pltpu.SemaphoreType.DMA((12,)),
        pltpu.SemaphoreType.DMA((12,)),
        pltpu.SemaphoreType.DMA((len(RED_STAGES),)),
        pltpu.SemaphoreType.DMA((len(RED_STAGES),)),
        pltpu.SemaphoreType.REGULAR,
        pltpu.SemaphoreType.REGULAR,
    ] + [vmem((COUNT[kind], 1, COLS), F32) for kind in RED_STAGES]
    out = pl.pallas_call(
        ocean_kernel,
        out_shape=[vmem(x.shape, x.dtype) for x in shapes],
        in_specs=[pl.BlockSpec(memory_space=hbm)] * 9,
        out_specs=[pl.BlockSpec(memory_space=vmem)] * 4,
        scratch_shapes=scratch,
        compiler_params=pltpu.CompilerParams(
            collective_id=0, has_side_effects=True, vmem_limit_bytes=VMEM_LIMIT
        ),
        name="ocean",
    )(*args)
    return pl.pallas_call(
        emit_kernel,
        out_shape=shapes,
        in_specs=[pl.BlockSpec(memory_space=vmem)] * 4,
        out_specs=[pl.BlockSpec(memory_space=hbm)] * 4,
        scratch_shapes=[pltpu.SemaphoreType.DMA((4,))],
        compiler_params=pltpu.CompilerParams(vmem_limit_bytes=8 * 1024 * 1024),
        name="emit",
    )(*out)


def solution(mesh):
    wide, flat = P(None, "gy", "gx"), P("gy", "gx")
    return jax.shard_map(
        on_device,
        mesh=mesh,
        in_specs=(wide, wide, wide, flat, flat, flat, flat, P(), P()),
        out_specs=(wide, wide, wide, flat),
        check_vma=False,
    )
```

```python
import functools

import jax
import jax.numpy as jnp
from jax import lax
from jax.experimental import pallas as pl
from jax.experimental.pallas import tpu as pltpu
from jax.sharding import PartitionSpec as P

MESH = pl.DeviceIdType.MESH
F32 = jnp.float32

LEVELS, ROWS, COLS, BY, NY = 4, 320, 128, 40, 2560
BLOCKS, NBY = ROWS // BY, 64
THICK = [(2 * k + 1) / (LEVELS * LEVELS) for k in range(LEVELS)]

OFF = 16
EXT_ROWS = ROWS + 2 * OFF
LOW, HIGH = OFF - 8, OFF + ROWS + 8
STEP = 48
FIELDS = 7
WET, HELM, X0, UB, UH, VB, VH = range(FIELDS)
PLANES = 3 * LEVELS
NX_DEV, NY_DEV = 16, 8

VMEM_LIMIT = 24 * 1024 * 1024
TO_EAST = (6, 4, 5, 6, 5, 5, 4)
TO_WEST = (5, 4, 5, 5, 4, 5, 4)
EAST_ROWS, WEST_ROWS = 40, 32
EMIT = 80
HALVES = ((20, 24), (16, 16))
RED_STAGES = ("all",)


def peers(kind):
    gx, gy = lax.axis_index("gx"), lax.axis_index("gy")
    if kind == "halo":
        return [
            (lax.rem(gx + i, NX_DEV), lax.rem(gy + j, NY_DEV))
            for i in (0, 1, NX_DEV - 1)
            for j in (0, 1, NY_DEV - 1)
            if i or j
        ]
    if kind == "plane":
        base = gx // 4 * 4
        return [
            (base + lax.rem(lax.rem(gx, 4) + i, 4), lax.rem(gy + j, NY_DEV))
            for i in range(4)
            for j in range(NY_DEV)
            if i or j
        ]
    if kind == "z":
        return [(lax.rem(gx + 4 * j, NX_DEV), gy) for j in range(1, 4)]
    return [
        (lax.rem(gx + i, NX_DEV), lax.rem(gy + j, NY_DEV))
        for i in range(NX_DEV)
        for j in range(NY_DEV)
        if i or j
    ]


def nearby(step):
    gx, gy = lax.axis_index("gx"), lax.axis_index("gy")
    z, y, core = gx // 4, lax.rem(gx, 4), lax.rem(gy, 2)
    return [
        (lax.rem(z + i, 4) * 4 + lax.rem(y + j, 4), gy + 2 * step if c == 0 else gy + 2 * step + 1 - 2 * core)
        for i in (0, 1, 3)
        for j in (0, 1, 3)
        for c in (0, 1)
        if i or j or c or step
    ]


COUNT = {"all": 127, "plane": 31, "z": 3}


def lanes(rows):
    return lax.broadcasted_iota(jnp.int32, (rows, COLS), 1)


def beside(ref, r, n, both=True):
    lane = lanes(n)
    first, last = lane == 0, lane == COLS - 1
    c0, c1 = ref[0, r : r + n, :], ref[1, r : r + n, :]
    e0, e1 = pltpu.roll(c0, COLS - 1, 1), pltpu.roll(c1, COLS - 1, 1)
    w0, w1 = pltpu.roll(c0, 1, 1), pltpu.roll(c1, 1, 1)
    out = [
        (
            c0,
            jnp.where(last, e1, e0),
            jnp.where(first, w1, w0),
            ref[0, r + 1 : r + 1 + n, :],
            ref[0, r - 1 : r - 1 + n, :],
        )
    ]
    if both:
        out.append(
            (
                c1,
                jnp.where(last, e0, e1),
                jnp.where(first, w0, w1),
                ref[1, r + 1 : r + 1 + n, :],
                ref[1, r - 1 : r - 1 + n, :],
            )
        )
    return out


def west_of(ref, r, n):
    first = lanes(n) == 0
    c0, c1 = ref[0, r : r + n, :], ref[1, r : r + n, :]
    w0, w1 = pltpu.roll(c0, 1, 1), pltpu.roll(c1, 1, 1)
    return (c0, jnp.where(first, w1, w0)), (c1, jnp.where(first, w0, w1))


def eights(x):
    return jnp.sum(x.reshape(x.shape[0] // 8, 8, COLS), axis=0)


def coefficients(sums):
    m = [sums[0], sums[1]]
    for k in range(2, 8):
        m.append(2.0 * sums[k] - m[k % 2])
    g = [[0.5 * (m[i + j] + m[abs(i - j)]) for j in range(5) if i + j < 8] for i in range(4)]

    def image(i, j):
        if j == 0:
            return g[i][1]
        return 0.5 * (g[i][j + 1] + g[i][j - 1])

    a = [[g[i][j] - image(i, j) for j in range(i + 1)] for i in range(4)]
    low = [[None] * 4 for _ in range(4)]
    inv, piv = [], []
    for j in range(4):
        pivot = a[j][j]
        for k in range(j):
            pivot = pivot - low[j][k] * low[j][k] * piv[k]
        good = pivot > 1e-6 * a[j][j]
        piv.append(jnp.where(good, pivot, 0.0))
        inv.append(jnp.where(good, 1.0 / jnp.where(good, pivot, 1.0), 0.0))
        for i in range(j + 1, 4):
            s = a[i][j]
            for k in range(j):
                s = s - low[i][k] * low[j][k] * piv[k]
            low[i][j] = s * inv[j]
    y = []
    for i in range(4):
        s = m[i]
        for k in range(i):
            s = s - low[i][k] * y[k]
        y.append(s)
    c = [None] * 4
    for i in reversed(range(4)):
        s = y[i] * inv[i]
        for k in range(i + 1, 4):
            s = s - low[k][i] * c[k]
        c[i] = s
    return c


def ocean_kernel(
    u_hbm, v_hbm, t_hbm, p_hbm, depth_hbm, helm_hbm, land_hbm, clinic_hbm, tropic_hbm,
    u_out, v_out, t_out, basis, guess, kept, sums_out,
    uvt, pold, depth, land, cmap, tmap, act, dom,
    ext, pack, pack_t, for_e, for_w, from_w, from_e, tail, got_t, got, corner,
    rim, rim_t, rim_got, rim_m, rim_back, edge, edge_got,
    face, rdiag, gain, diag, flow, part,
    in_sem, send_sem, recv_sem, rsend_sem, rrecv_sem, known, far, *red,
):
    gx, gy = lax.axis_index("gx"), lax.axis_index("gy")
    east, west = lax.rem(gx + 1, NX_DEV), lax.rem(gx + NX_DEV - 1, NX_DEV)
    north, south = lax.rem(gy + 1, NY_DEV), lax.rem(gy + NY_DEV - 1, NY_DEV)
    own = pl.ds(OFF, ROWS)

    loads = [
        pltpu.make_async_copy(u_hbm, uvt.at[0:4, 8 : 8 + ROWS, :], in_sem.at[0]),
        pltpu.make_async_copy(v_hbm, uvt.at[4:8, 8 : 8 + ROWS, :], in_sem.at[1]),
        pltpu.make_async_copy(p_hbm, pold, in_sem.at[2]),
        pltpu.make_async_copy(depth_hbm, depth, in_sem.at[3]),
        pltpu.make_async_copy(land_hbm, land, in_sem.at[4]),
        pltpu.make_async_copy(clinic_hbm, cmap, in_sem.at[5]),
        pltpu.make_async_copy(tropic_hbm, tmap, in_sem.at[6]),
        pltpu.make_async_copy(helm_hbm, ext.at[HELM, 0, OFF : OFF + ROWS, :], in_sem.at[7]),
        pltpu.make_async_copy(t_hbm, uvt.at[8:12, 8 : 8 + ROWS, :], in_sem.at[8]),
    ]
    for load in loads:
        load.start()

    barrier = pltpu.get_barrier_semaphore()
    has_n, has_s = gy < NY_DEV - 1, gy > 0
    up_x, down_x = gy < NY_DEV - 2, gy > 1

    def greet(sem):
        for step, there in ((0, None), (1, up_x), (-1, down_x)):

            def tell(step=step):
                for peer in nearby(step):
                    pl.semaphore_signal(sem, inc=1, device_id=peer, device_id_type=MESH)

            tell() if there is None else pl.when(there)(tell)

    def hear(sem):
        inner = lax.rem((gy // 2 + 1) // 2, 2)
        pl.semaphore_wait(sem, 35 + 18 * inner)

    greet(barrier)

    pack[ROWS:, :] = jnp.zeros((pack.shape[0] - ROWS, COLS), F32)
    for load in loads[:8]:
        load.wait()

    shape = (NX_DEV, NBY)
    mine = lax.broadcasted_iota(jnp.int32, shape, 0) == gx
    shape = (BLOCKS, NBY)
    wanted = lax.broadcasted_iota(jnp.int32, shape, 1) == lax.broadcasted_iota(jnp.int32, shape, 0) + gy * BLOCKS

    def per_block(flags):
        line = jnp.sum(jnp.where(mine, flags, 0.0), axis=0, keepdims=True)
        column = jnp.sum(jnp.where(wanted, line, 0.0), axis=1, keepdims=True)
        return jnp.broadcast_to(column, (BLOCKS, COLS))

    act[...] = per_block(cmap[...].astype(F32))
    dom[...] = per_block(jnp.where(tmap[...] >= 0, 1.0, 0.0))

    def coriolis(b):
        row = lax.broadcasted_iota(jnp.int32, (BY, COLS), 0) + (gy * ROWS + b * BY)
        return 0.2 + 0.6 * ((row.astype(F32) + 0.5) / NY)

    group = lanes(BY) // 16
    for b in range(BLOCKS):
        r = b * BY
        rows = slice(r, r + BY)
        solve = land[rows, :].astype(F32) * dom[b : b + 1, :]
        wet = depth[rows, :] * solve
        u = [uvt[k, 8 + r : 8 + r + BY, :] for k in range(LEVELS)]
        v = [uvt[LEVELS + k, 8 + r : 8 + r + BY, :] for k in range(LEVELS)]
        u_bar = sum(THICK[k] * u[k] for k in range(LEVELS))
        v_bar = sum(THICK[k] * v[k] for k in range(LEVELS))
        cor = 0.2 * coriolis(b)
        mix = 0.1 * (THICK[1] - THICK[0])
        u_hat = u_bar + mix * (u[0] - u[3]) + cor * v_bar
        v_hat = v_bar + mix * (v[0] - v[3]) - cor * u_bar
        fields = [wet, ext[HELM, 0, OFF + r : OFF + r + BY, :], solve * pold[rows, :], u_bar, u_hat, v_bar, v_hat]
        packed = None
        for f, value in enumerate(fields):
            if f != HELM:
                ext[f, 0, OFF + r : OFF + r + BY, :] = value
            moved = pltpu.roll(value, 8 + 16 * f, 1)
            packed = moved if packed is None else jnp.where(group == f, moved, packed)
        pack[rows, :] = packed
    for c in range(3):
        pack_t[...] = pack[128 * c : 128 * (c + 1), :].T
        e_ref, w_ref = (tail.at[0], tail.at[1]) if c == 2 else (for_e, for_w)
        at_e, at_w = (0, 0) if c == 2 else (EAST_ROWS * c, WEST_ROWS * c)
        for f in range(FIELDS):
            ne, nw = TO_EAST[f], TO_WEST[f]
            e_ref[at_e : at_e + ne, :] = pack_t[16 * f + 8 - ne : 16 * f + 8, :]
            w_ref[at_w : at_w + nw, :] = pack_t[16 * f + 8 : 16 * f + 8 + nw, :]
            at_e, at_w = at_e + ne, at_w + nw
    for i, (ref, whole) in enumerate(((for_e, EAST_ROWS), (for_w, WEST_ROWS))):
        half, size = HALVES[i]
        moved = pltpu.roll(tail[i, half : half + size, :], COLS // 2, 1)
        ref[2 * whole :, :] = jnp.where(lanes(size) < COLS // 2, tail[i, 0:size, :], moved)

    routes = {
        0: (for_e, from_w, (east, gy), None),
        1: (for_w, from_e, (west, gy), None),
        2: (ext.at[:, 0, OFF + ROWS - 8 : OFF + ROWS, :], ext.at[:, 0, LOW:OFF, :], (gx, north), "n"),
        3: (ext.at[:, 0, OFF : OFF + 8, :], ext.at[:, 0, OFF + ROWS : HIGH, :], (gx, south), "s"),
        4: (pack.at[ROWS - 8 : ROWS, :], corner.at[0], (east, north), "n"),
        5: (pack.at[ROWS - 8 : ROWS, :], corner.at[1], (west, north), "n"),
        6: (pack.at[0:8, :], corner.at[2], (east, south), "s"),
        7: (pack.at[0:8, :], corner.at[3], (west, south), "s"),
        8: (rim_t, rim_got.at[0], (east, gy), None),
        9: (rim_t, rim_got.at[1], (west, gy), None),
        10: (edge.at[1], edge_got.at[0], (gx, north), "n"),
        11: (edge.at[0], edge_got.at[1], (gx, south), "s"),
    }
    HALO, OUTER = range(8), range(8, 12)

    def transfer(which, what):
        def go(keys):
            for k in keys:
                src, dst, to, _ = routes[k]
                copy = pltpu.make_async_remote_copy(
                    src_ref=src, dst_ref=dst, send_sem=send_sem.at[k], recv_sem=recv_sem.at[k],
                    device_id=to, device_id_type=MESH,
                )
                getattr(copy, what)()

        go([k for k in which if routes[k][3] is None])
        for way, other in (("n", "s"), ("s", "n")):
            there = {"n": has_n, "s": has_s}[other if what == "wait_recv" else way]
            pl.when(there)(functools.partial(go, [k for k in which if routes[k][3] == way]))

    hear(barrier)
    transfer((0, 1), "start")
    greet(known)
    transfer(HALO[2:], "start")

    loads[8].wait()
    pair = lanes(BY) // 2
    for b in range(BLOCKS):
        r = b * BY
        packed = None
        for q in range(PLANES):
            moved = pltpu.roll(uvt[q, 8 + r : 8 + r + BY, :], 2 * q + 1, 1)
            packed = moved if packed is None else jnp.where(pair == q, moved, packed)
        rim[r : r + BY, :] = packed
    rim[ROWS:, :] = jnp.zeros((rim.shape[0] - ROWS, COLS), F32)
    for c in range(3):
        rim_t[:, 128 * c : 128 * (c + 1)] = rim[128 * c : 128 * (c + 1), :].T[: 2 * PLANES, :]
    for q in range(PLANES):
        edge[0, q : q + 1, :] = uvt[q, 8 : 9, :]
        edge[1, q : q + 1, :] = uvt[q, 7 + ROWS : 8 + ROWS, :]
    transfer(OUTER, "start")
    transfer(HALO, "wait_recv")
    hear(known)

    @pl.when((gy // 2 == 1) | (gy // 2 == 2))
    def _():
        pl.semaphore_signal(
            far, inc=1, device_id=(gx, gy + 4 * lax.rem(gy // 2 - 1, 2) - 2), device_id_type=MESH
        )

    low_half = lax.rem(lanes(8), 16) < 8
    nothing = jnp.where(lanes(8) // 16 == HELM, 1.0, 0.0)
    for i, (ref, whole) in enumerate(((from_w, EAST_ROWS), (from_e, WEST_ROWS))):
        half, size = HALVES[i]
        shared = ref[2 * whole :, :]
        tail[i, 0:size, :] = shared
        tail[i, half : half + size, :] = pltpu.roll(shared, COLS // 2, 1)
    for c in range(3):
        w_ref, e_ref = (tail.at[0], tail.at[1]) if c == 2 else (from_w, from_e)
        at_w, at_e = (0, 0) if c == 2 else (EAST_ROWS * c, WEST_ROWS * c)
        for f in range(FIELDS):
            nw, ne = TO_EAST[f], TO_WEST[f]
            got_t[16 * f + 8 - nw : 16 * f + 8, :] = w_ref[at_w : at_w + nw, :]
            got_t[16 * f + 8 : 16 * f + 8 + ne, :] = e_ref[at_e : at_e + ne, :]
            at_w, at_e = at_w + nw, at_e + ne
        block = got_t[...].T
        n = min(128, ROWS - 128 * c)
        got[8 + 128 * c : 8 + 128 * c + n, :] = block[:n, :]
    for k, there, first, halo_at in ((0, has_s, 0, LOW), (2, has_n, 8 + ROWS, OFF + ROWS)):

        @pl.when(there)
        def _(k=k, first=first):
            got[first : first + 8, :] = jnp.where(low_half, corner[k], corner[k + 1])

        @pl.when(jnp.logical_not(there))
        def _(k=k, first=first, halo_at=halo_at):
            got[first : first + 8, :] = nothing
            edge_got[k // 2] = jnp.zeros((16, COLS), F32)
            for f in range(FIELDS):
                ext[f, 0, halo_at : halo_at + 8, :] = jnp.full((8, COLS), 1.0 if f == HELM else 0.0, F32)

    chunks = [(r, STEP) for r in range(LOW, HIGH, STEP)]
    lane = lanes(STEP)
    for r, n in chunks:
        packed = got[r - LOW : r - LOW + n, :]
        for f in range(FIELDS):
            moved = pltpu.roll(packed, COLS - (16 * f + 8), 1)
            came = (lane < TO_WEST[f]) | (lane >= COLS - TO_EAST[f])
            ext[f, 1, r : r + n, :] = jnp.where(came, moved, 1.0 if f == HELM else 0.0)

    for r, n in chunks:
        at = slice(r, r + n)
        for t, (c, e, w, nn, s) in enumerate(beside(ext.at[WET], r, n)):
            four = [jnp.minimum(c, o) for o in (e, w, nn, s)]
            total = ext[HELM, t, at, :] + four[0] + four[1] + four[2] + four[3]
            inverse = 1.0 / total
            rdiag[t, at, :] = inverse
            if t == 0:
                diag[at, :] = total
            for k in range(4):
                face[k, t, at, :] = four[k]
                gain[k, t, at, :] = four[k] * inverse
    for k, (bar, hat) in enumerate(((UB, UH), (VB, VH))):
        for r, n in chunks:
            at = slice(r, r + n)
            for t, (c, *others) in enumerate(beside(ext.at[bar], r, n)):
                spread = sum(face[i, t, at, :] * (o - c) for i, o in enumerate(others))
                flow[k, t, at, :] = ext[WET, t, at, :] * (ext[hat, t, at, :] + 0.1 * spread)

    def image(t, at, others):
        return sum(gain[i, t, at, :] * o for i, o in enumerate(others))

    for r, n in chunks:
        at = slice(r, r + n)
        x = beside(ext.at[X0], r, n)
        for t, (ef, efw) in enumerate(west_of(flow.at[0], r, n)):
            nf, nfs = flow[1, t, at, :], flow[1, t, r - 1 : r - 1 + n, :]
            force = jnp.where(ext[WET, t, at, :] > 0.0, (efw - ef) + (nfs - nf), 0.0)
            c, *others = x[t]
            guess[t, at, :] = c
            basis[0, t, at, :] = force * rdiag[t, at, :] + (image(t, at, others) - c)
    for k in range(3):
        for r, n in chunks:
            at = slice(r, r + n)
            for t, (c, *others) in enumerate(beside(basis.at[k], r, n)):
                value = image(t, at, others)
                if k:
                    value = 2.0 * value - basis[k - 1, t, at, :]
                basis[k + 1, t, at, :] = value
    sums = [jnp.zeros((8, COLS), F32) for _ in range(8)]
    for b in range(BLOCKS):
        r = OFF + b * BY
        at = slice(r, r + BY)
        vectors = [basis[k, 0, at, :] for k in range(4)]
        c = vectors[3]
        right = jnp.where(
            lanes(BY) == COLS - 1, pltpu.roll(basis[3, 1, at, :], COLS - 1, 1), pltpu.roll(c, COLS - 1, 1)
        )
        up = basis[3, 0, r + 1 : r + 1 + BY, :]
        for k in range(4):
            weighted = diag[at, :] * vectors[k]
            sums[2 * k] = sums[2 * k] + eights(weighted * vectors[k])
            if k < 3:
                sums[2 * k + 1] = sums[2 * k + 1] + eights(weighted * vectors[k + 1])
        sums[7] = sums[7] + eights(c * (face[0, 0, at, :] * right + face[2, 0, at, :] * up))
    sums[7] = 4.0 * sums[7] - sums[5]

    rows8 = lax.broadcasted_iota(jnp.int32, (8, COLS), 0)
    mat = jnp.zeros((8, COLS), F32)
    for k in range(8):
        mat = jnp.where(rows8 == k, jnp.sum(sums[k], axis=0, keepdims=True), mat)
    total = jnp.broadcast_to(jnp.sum(mat, axis=1, keepdims=True), (8, COLS))
    row = jnp.sum(jnp.where(lanes(8) == rows8, total, 0.0), axis=0, keepdims=True)

    def level_updates():
        transfer(OUTER, "wait_recv")
        even = lax.rem(lax.broadcasted_iota(jnp.int32, (2 * PLANES, COLS), 0), 2) == 0
        for c in range(3):
            cols = slice(128 * c, 128 * (c + 1))
            from_w, from_e = rim_got[0, :, cols], rim_got[1, :, cols]
            up, down = pltpu.roll(from_e, 2 * PLANES - 1, 0), pltpu.roll(from_w, 1, 0)
            rim_m[0 : 2 * PLANES, :] = jnp.where(even, up, down)
            rim_back[128 * c : 128 * (c + 1), :] = rim_m[...].T
        for q in range(PLANES):
            uvt[q, 7:8, :] = edge_got[0, q : q + 1, :]
            uvt[q, 8 + ROWS : 9 + ROWS, :] = edge_got[1, q : q + 1, :]
        first, last = lanes(BY) == 0, lanes(BY) == COLS - 1

        for b in range(BLOCKS):
            r = b * BY
            rows = slice(r, r + BY)
            at = slice(OFF + r, OFF + r + BY)
            on = act[b : b + 1, :]
            ocean = land[rows, :].astype(F32)
            keep = on * ocean
            kept[rows, :] = keep
            off = 1.0 - on
            cor = coriolis(b)
            faces = [face[k, 0, at, :] for k in range(4)]
            rim_row = rim_back[rows, :]

            def around(q):
                c = uvt[q, 8 + r : 8 + r + BY, :]
                side = pltpu.roll(rim_row, COLS - 1 - 2 * q, 1)
                e = jnp.where(last, side, pltpu.roll(c, COLS - 1, 1))
                w = jnp.where(first, side, pltpu.roll(c, 1, 1))
                return c, e, w, uvt[q, 9 + r : 9 + r + BY, :], uvt[q, 7 + r : 7 + r + BY, :]

            def raw(q0):
                out, keepers = [], []
                for k in range(LEVELS):
                    c, *others = around(q0 + k)
                    spread = sum(faces[i] * (o - c) for i, o in enumerate(others))
                    mix = jnp.zeros_like(c)
                    if k < LEVELS - 1:
                        mix = mix + (uvt[q0 + k + 1, 8 + r : 8 + r + BY, :] - c)
                    if k > 0:
                        mix = mix - (c - uvt[q0 + k - 1, 8 + r : 8 + r + BY, :])
                    out.append((c, 0.5 * mix + 0.5 * spread, others))
                return out

            for k, (c, tend, _) in enumerate(raw(0)):
                star = c + 0.2 * (tend + cor * uvt[LEVELS + k, 8 + r : 8 + r + BY, :])
                u_out[k, rows, :] = keep * star + off * c
            for k, (c, tend, _) in enumerate(raw(LEVELS)):
                star = c + 0.2 * (tend - cor * uvt[k, 8 + r : 8 + r + BY, :])
                v_out[k, rows, :] = keep * star + off * c
            for k, (c, tend, (e, w, nn, s)) in enumerate(raw(2 * LEVELS)):
                uk = uvt[k, 8 + r : 8 + r + BY, :]
                vk = uvt[LEVELS + k, 8 + r : 8 + r + BY, :]
                star = c + 0.2 * (tend - 0.5 * (uk * (e - w) + vk * (nn - s)))
                t_out[k, rows, :] = keep * star + off * c

    @pl.when((gy // 2 == 0) | (gy // 2 == 3))
    def _():
        pl.semaphore_wait(far, 1)

    for s, kind in enumerate(RED_STAGES):
        landing = red[s]
        part[s] = row
        for j, peer in enumerate(peers(kind)):
            pltpu.make_async_remote_copy(
                src_ref=part.at[s], dst_ref=landing.at[j], send_sem=rsend_sem.at[s], recv_sem=rrecv_sem.at[s],
                device_id=peer, device_id_type=MESH,
            ).start()
        if s == 0:
            level_updates()
        every = pltpu.make_async_remote_copy(
            src_ref=landing, dst_ref=landing, send_sem=rsend_sem.at[s], recv_sem=rrecv_sem.at[s],
            device_id=(east, gy), device_id_type=MESH,
        )
        every.wait_recv()
        row = row + jnp.sum(landing[...], axis=0)

    sums_out[...] = row
    transfer(range(12), "wait_send")
    for s in range(len(RED_STAGES)):
        pltpu.make_async_remote_copy(
            src_ref=red[s], dst_ref=red[s], send_sem=rsend_sem.at[s], recv_sem=rrecv_sem.at[s],
            device_id=(east, gy), device_id_type=MESH,
        ).wait_send()


def emit_kernel(u_ref, v_ref, t_ref, basis, guess, kept, sums, u_hbm, v_hbm, t_hbm, p_hbm, u_new, v_new, p_new, sem):
    copies = [pltpu.make_async_copy(t_ref, t_hbm, sem.at[0])]
    copies[0].start()
    row = sums[...]
    c = coefficients([jnp.broadcast_to(row[:, k : k + 1], (1, COLS)) for k in range(8)])

    def answer(t, at):
        x = guess[t, at, :]
        for k in range(4):
            x = x + c[k] * basis[k, t, at, :]
        return x

    last = lanes(EMIT) == COLS - 1
    for b in range(ROWS // EMIT):
        rows = slice(b * EMIT, (b + 1) * EMIT)
        at = slice(OFF + rows.start, OFF + rows.stop)
        x0, x1 = answer(0, at), answer(1, at)
        up = answer(0, slice(at.start + 1, at.stop + 1))
        right = jnp.where(last, pltpu.roll(x1, COLS - 1, 1), pltpu.roll(x0, COLS - 1, 1))
        keep = kept[rows, :]
        p_new[rows, :] = x0
        grad_x, grad_y = keep * (right - x0), keep * (up - x0)
        for k in range(LEVELS):
            u_new[k, rows, :] = u_ref[k, rows, :] - grad_x
            v_new[k, rows, :] = v_ref[k, rows, :] - grad_y
        for i, (src, dst) in enumerate(
            (
                (u_new.at[:, rows, :], u_hbm.at[:, rows, :]),
                (v_new.at[:, rows, :], v_hbm.at[:, rows, :]),
                (p_new.at[rows, :], p_hbm.at[rows, :]),
            )
        ):
            copy = pltpu.make_async_copy(src, dst, sem.at[1 + 3 * b + i])
            copy.start()
            copies.append(copy)
    for copy in copies:
        copy.wait()


def on_device(*args):
    args = args[:7] + (args[7].T, args[8].T)
    args = [pltpu.with_memory_space_constraint(x, pltpu.HBM) for x in args]
    vmem, hbm = pltpu.VMEM, pltpu.HBM
    three = jax.ShapeDtypeStruct((LEVELS, ROWS, COLS), F32)
    two = jax.ShapeDtypeStruct((ROWS, COLS), F32)
    shapes = (three, three, three, two)
    tiles = (2, EXT_ROWS, COLS)
    scratch = [
        vmem((PLANES, ROWS + 16, COLS), F32),
        vmem((ROWS, COLS), F32),
        vmem((ROWS, COLS), F32),
        vmem((ROWS, COLS), jnp.int32),
        vmem((NX_DEV, NBY), jnp.int32),
        vmem((NX_DEV, NBY), jnp.int32),
        vmem((BLOCKS, COLS), F32),
        vmem((BLOCKS, COLS), F32),
        vmem((FIELDS,) + tiles, F32),
        vmem((384, COLS), F32),
        vmem((COLS, COLS), F32),
        vmem((2 * EAST_ROWS + HALVES[0][1], COLS), F32),
        vmem((2 * WEST_ROWS + HALVES[1][1], COLS), F32),
        vmem((2 * EAST_ROWS + HALVES[0][1], COLS), F32),
        vmem((2 * WEST_ROWS + HALVES[1][1], COLS), F32),
        vmem((2, 48, COLS), F32),
        vmem((COLS, COLS), F32),
        vmem((ROWS + 16, COLS), F32),
        vmem((4, 8, COLS), F32),
        vmem((384, COLS), F32),
        vmem((2 * PLANES, 384), F32),
        vmem((2, 2 * PLANES, 384), F32),
        vmem((COLS, COLS), F32),
        vmem((384, COLS), F32),
        vmem((2, 16, COLS), F32),
        vmem((2, 16, COLS), F32),
        vmem((4,) + tiles, F32),
        vmem(tiles, F32),
        vmem((4,) + tiles, F32),
        vmem((EXT_ROWS, COLS), F32),
        vmem((2,) + tiles, F32),
        vmem((len(RED_STAGES), 1, COLS), F32),
        pltpu.SemaphoreType.DMA((9,)),
        pltpu.SemaphoreType.DMA((12,)),
        pltpu.SemaphoreType.DMA((12,)),
        pltpu.SemaphoreType.DMA((len(RED_STAGES),)),
        pltpu.SemaphoreType.DMA((len(RED_STAGES),)),
        pltpu.SemaphoreType.REGULAR,
        pltpu.SemaphoreType.REGULAR,
    ] + [vmem((COUNT[kind], 1, COLS), F32) for kind in RED_STAGES]
    out = pl.pallas_call(
        ocean_kernel,
        out_shape=[vmem(x.shape, F32) for x in (three, three, three)]
        + [vmem((4,) + tiles, F32), vmem(tiles, F32), vmem((ROWS, COLS), F32), vmem((1, COLS), F32)],
        in_specs=[pl.BlockSpec(memory_space=hbm)] * 9,
        out_specs=[pl.BlockSpec(memory_space=vmem)] * 7,
        scratch_shapes=scratch,
        compiler_params=pltpu.CompilerParams(
            collective_id=0, has_side_effects=True, vmem_limit_bytes=VMEM_LIMIT
        ),
        name="ocean",
    )(*args)
    return pl.pallas_call(
        emit_kernel,
        out_shape=shapes,
        in_specs=[pl.BlockSpec(memory_space=vmem)] * 7,
        out_specs=[pl.BlockSpec(memory_space=hbm)] * 4,
        scratch_shapes=[vmem(three.shape, F32), vmem(three.shape, F32), vmem(two.shape, F32)]
        + [pltpu.SemaphoreType.DMA((1 + 3 * (ROWS // EMIT),))],
        compiler_params=pltpu.CompilerParams(vmem_limit_bytes=8 * 1024 * 1024),
        name="emit",
    )(*out)


def solution(mesh):
    wide, flat = P(None, "gy", "gx"), P("gy", "gx")
    return jax.shard_map(
        on_device,
        mesh=mesh,
        in_specs=(wide, wide, wide, flat, flat, flat, flat, P(), P()),
        out_specs=(wide, wide, wide, flat),
        check_vma=False,
    )
```

```python
import functools

import jax
import jax.numpy as jnp
from jax import lax
from jax.experimental import pallas as pl
from jax.experimental.pallas import tpu as pltpu
from jax.sharding import PartitionSpec as P

MESH = pl.DeviceIdType.MESH
F32 = jnp.float32

LEVELS, ROWS, COLS, BY, NY = 4, 320, 128, 40, 2560
BLOCKS, NBY = ROWS // BY, 64
THICK = [(2 * k + 1) / (LEVELS * LEVELS) for k in range(LEVELS)]

OFF = 16
EXT_ROWS = ROWS + 2 * OFF
LOW, HIGH = OFF - 8, OFF + ROWS + 8
STEP = 48
FIELDS = 7
WET, HELM, X0, UB, UH, VB, VH = range(FIELDS)
PLANES = 3 * LEVELS
NX_DEV, NY_DEV = 16, 8

VMEM_LIMIT = 24 * 1024 * 1024
TO_EAST = (6, 4, 5, 6, 5, 5, 4)
TO_WEST = (5, 4, 5, 5, 4, 5, 4)
EAST_ROWS, WEST_ROWS = 40, 32
EMIT = 80
HALVES = ((20, 24), (16, 16))
RED_STAGES = ("all",)


def peers(kind):
    gx, gy = lax.axis_index("gx"), lax.axis_index("gy")
    if kind == "halo":
        return [
            (lax.rem(gx + i, NX_DEV), lax.rem(gy + j, NY_DEV))
            for i in (0, 1, NX_DEV - 1)
            for j in (0, 1, NY_DEV - 1)
            if i or j
        ]
    if kind == "plane":
        base = gx // 4 * 4
        return [
            (base + lax.rem(lax.rem(gx, 4) + i, 4), lax.rem(gy + j, NY_DEV))
            for i in range(4)
            for j in range(NY_DEV)
            if i or j
        ]
    if kind == "z":
        return [(lax.rem(gx + 4 * j, NX_DEV), gy) for j in range(1, 4)]
    return [
        (lax.rem(gx + i, NX_DEV), lax.rem(gy + j, NY_DEV))
        for i in range(NX_DEV)
        for j in range(NY_DEV)
        if i or j
    ]


BESIDE = ((0, 1), (1, 1), (0, 3), (3, 3), (0, 0))
APART = ((1, 0), (3, 0), (1, 3), (3, 1))


def nearby(step, ways):
    gx, gy = lax.axis_index("gx"), lax.axis_index("gy")
    z, y, core = gx // 4, lax.rem(gx, 4), lax.rem(gy, 2)
    return [
        (lax.rem(z + i, 4) * 4 + lax.rem(y + j, 4), gy + 2 * step if c == 0 else gy + 2 * step + 1 - 2 * core)
        for i, j in ways
        for c in (0, 1)
        if i or j or c or step
    ]


COUNT = {"all": 127, "plane": 31, "z": 3}


def lanes(rows):
    return lax.broadcasted_iota(jnp.int32, (rows, COLS), 1)


def beside(ref, r, n, turned=None):
    lane = lanes(n)
    first, last = lane == 0, lane == COLS - 1
    c0, c1 = ref[0, r : r + n, :], ref[1, r : r + n, :]
    if turned is None:
        e0, w0 = pltpu.roll(c0, COLS - 1, 1), pltpu.roll(c0, 1, 1)
    else:
        e0, w0 = turned[0, r : r + n, :], turned[1, r : r + n, :]
    e1, w1 = pltpu.roll(c1, COLS - 1, 1), pltpu.roll(c1, 1, 1)
    return [
        (
            c,
            jnp.where(last, other_e, own_e),
            jnp.where(first, other_w, own_w),
            ref[t, r + 1 : r + 1 + n, :],
            ref[t, r - 1 : r - 1 + n, :],
        )
        for t, (c, own_e, other_e, own_w, other_w) in enumerate(((c0, e0, e1, w0, w1), (c1, e1, e0, w1, w0)))
    ]


def west_of(ref, r, n):
    first = lanes(n) == 0
    c0, c1 = ref[0, r : r + n, :], ref[1, r : r + n, :]
    w0, w1 = pltpu.roll(c0, 1, 1), pltpu.roll(c1, 1, 1)
    return (c0, jnp.where(first, w1, w0)), (c1, jnp.where(first, w0, w1))


def eights(x):
    return jnp.sum(x.reshape(x.shape[0] // 8, 8, COLS), axis=0)


def coefficients(sums):
    m = [sums[0], sums[1]]
    for k in range(2, 8):
        m.append(2.0 * sums[k] - m[k % 2])
    g = [[0.5 * (m[i + j] + m[abs(i - j)]) for j in range(5) if i + j < 8] for i in range(4)]

    def image(i, j):
        if j == 0:
            return g[i][1]
        return 0.5 * (g[i][j + 1] + g[i][j - 1])

    a = [[g[i][j] - image(i, j) for j in range(i + 1)] for i in range(4)]
    low = [[None] * 4 for _ in range(4)]
    inv, piv = [], []
    for j in range(4):
        pivot = a[j][j]
        for k in range(j):
            pivot = pivot - low[j][k] * low[j][k] * piv[k]
        good = pivot > 1e-6 * a[j][j]
        piv.append(jnp.where(good, pivot, 0.0))
        inv.append(jnp.where(good, 1.0 / jnp.where(good, pivot, 1.0), 0.0))
        for i in range(j + 1, 4):
            s = a[i][j]
            for k in range(j):
                s = s - low[i][k] * low[j][k] * piv[k]
            low[i][j] = s * inv[j]
    y = []
    for i in range(4):
        s = m[i]
        for k in range(i):
            s = s - low[i][k] * y[k]
        y.append(s)
    c = [None] * 4
    for i in reversed(range(4)):
        s = y[i] * inv[i]
        for k in range(i + 1, 4):
            s = s - low[k][i] * c[k]
        c[i] = s
    return c


def ocean_kernel(
    u_hbm, v_hbm, t_hbm, p_hbm, depth_hbm, helm_hbm, land_hbm, clinic_hbm, tropic_hbm,
    u_out, v_out, t_out, basis, guess, kept, sums_out,
    uvt, pold, depth, land, cmap, tmap, act, dom,
    ext, pack, pack_t, for_e, for_w, from_w, from_e, tail, got_t, got, corner,
    rim, rim_t, rim_got, rim_m, rim_back, edge, edge_got,
    face, rdiag, gain, diag, flow, turned, part,
    in_sem, send_sem, recv_sem, rsend_sem, rrecv_sem, known, far, *red,
):
    gx, gy = lax.axis_index("gx"), lax.axis_index("gy")
    east, west = lax.rem(gx + 1, NX_DEV), lax.rem(gx + NX_DEV - 1, NX_DEV)
    north, south = lax.rem(gy + 1, NY_DEV), lax.rem(gy + NY_DEV - 1, NY_DEV)
    own = pl.ds(OFF, ROWS)

    loads = [
        pltpu.make_async_copy(u_hbm, uvt.at[0:4, 8 : 8 + ROWS, :], in_sem.at[0]),
        pltpu.make_async_copy(v_hbm, uvt.at[4:8, 8 : 8 + ROWS, :], in_sem.at[1]),
        pltpu.make_async_copy(p_hbm, pold, in_sem.at[2]),
        pltpu.make_async_copy(depth_hbm, depth, in_sem.at[3]),
        pltpu.make_async_copy(land_hbm, land, in_sem.at[4]),
        pltpu.make_async_copy(clinic_hbm, cmap, in_sem.at[5]),
        pltpu.make_async_copy(tropic_hbm, tmap, in_sem.at[6]),
        pltpu.make_async_copy(helm_hbm, ext.at[HELM, 0, OFF : OFF + ROWS, :], in_sem.at[7]),
        pltpu.make_async_copy(t_hbm, uvt.at[8:12, 8 : 8 + ROWS, :], in_sem.at[8]),
    ]
    barrier = pltpu.get_barrier_semaphore()
    has_n, has_s = gy < NY_DEV - 1, gy > 0
    up_x, down_x = gy < NY_DEV - 2, gy > 1

    def greet(sem):
        for ways in (BESIDE, APART):
            for step, there in ((0, None), (1, up_x), (-1, down_x)):

                def tell(step=step, ways=ways):
                    for peer in nearby(step, ways):
                        pl.semaphore_signal(sem, inc=1, device_id=peer, device_id_type=MESH)

                tell() if there is None else pl.when(there)(tell)

    def hear(sem):
        inner = lax.rem((gy // 2 + 1) // 2, 2)
        pl.semaphore_wait(sem, 35 + 18 * inner)

    greet(barrier)
    for load in loads:
        load.start()

    pack[ROWS:, :] = jnp.zeros((pack.shape[0] - ROWS, COLS), F32)
    for load in loads[:8]:
        load.wait()

    shape = (NX_DEV, NBY)
    mine = lax.broadcasted_iota(jnp.int32, shape, 0) == gx
    shape = (BLOCKS, NBY)
    wanted = lax.broadcasted_iota(jnp.int32, shape, 1) == lax.broadcasted_iota(jnp.int32, shape, 0) + gy * BLOCKS

    def per_block(flags):
        line = jnp.sum(jnp.where(mine, flags, 0.0), axis=0, keepdims=True)
        column = jnp.sum(jnp.where(wanted, line, 0.0), axis=1, keepdims=True)
        return jnp.broadcast_to(column, (BLOCKS, COLS))

    act[...] = per_block(cmap[...].astype(F32))
    dom[...] = per_block(jnp.where(tmap[...] >= 0, 1.0, 0.0))

    def coriolis(b):
        row = lax.broadcasted_iota(jnp.int32, (BY, COLS), 0) + (gy * ROWS + b * BY)
        return 0.2 + 0.6 * ((row.astype(F32) + 0.5) / NY)

    group = lanes(BY) // 16
    for b in range(BLOCKS):
        r = b * BY
        rows = slice(r, r + BY)
        solve = land[rows, :].astype(F32) * dom[b : b + 1, :]
        wet = depth[rows, :] * solve
        u = [uvt[k, 8 + r : 8 + r + BY, :] for k in range(LEVELS)]
        v = [uvt[LEVELS + k, 8 + r : 8 + r + BY, :] for k in range(LEVELS)]
        u_bar = sum(THICK[k] * u[k] for k in range(LEVELS))
        v_bar = sum(THICK[k] * v[k] for k in range(LEVELS))
        cor = 0.2 * coriolis(b)
        mix = 0.1 * (THICK[1] - THICK[0])
        u_hat = u_bar + mix * (u[0] - u[3]) + cor * v_bar
        v_hat = v_bar + mix * (v[0] - v[3]) - cor * u_bar
        fields = [wet, ext[HELM, 0, OFF + r : OFF + r + BY, :], solve * pold[rows, :], u_bar, u_hat, v_bar, v_hat]
        packed = None
        for f, value in enumerate(fields):
            if f != HELM:
                ext[f, 0, OFF + r : OFF + r + BY, :] = value
            moved = pltpu.roll(value, 8 + 16 * f, 1)
            packed = moved if packed is None else jnp.where(group == f, moved, packed)
        pack[rows, :] = packed
    for c in range(3):
        pack_t[...] = pack[128 * c : 128 * (c + 1), :].T
        e_ref, w_ref = (tail.at[0], tail.at[1]) if c == 2 else (for_e, for_w)
        at_e, at_w = (0, 0) if c == 2 else (EAST_ROWS * c, WEST_ROWS * c)
        for f in range(FIELDS):
            ne, nw = TO_EAST[f], TO_WEST[f]
            e_ref[at_e : at_e + ne, :] = pack_t[16 * f + 8 - ne : 16 * f + 8, :]
            w_ref[at_w : at_w + nw, :] = pack_t[16 * f + 8 : 16 * f + 8 + nw, :]
            at_e, at_w = at_e + ne, at_w + nw
    for i, (ref, whole) in enumerate(((for_e, EAST_ROWS), (for_w, WEST_ROWS))):
        half, size = HALVES[i]
        moved = pltpu.roll(tail[i, half : half + size, :], COLS // 2, 1)
        ref[2 * whole :, :] = jnp.where(lanes(size) < COLS // 2, tail[i, 0:size, :], moved)

    routes = {
        0: (for_e, from_w, (east, gy), None),
        1: (for_w, from_e, (west, gy), None),
        2: (ext.at[:, 0, OFF + ROWS - 8 : OFF + ROWS, :], ext.at[:, 0, LOW:OFF, :], (gx, north), "n"),
        3: (ext.at[:, 0, OFF : OFF + 8, :], ext.at[:, 0, OFF + ROWS : HIGH, :], (gx, south), "s"),
        4: (pack.at[ROWS - 8 : ROWS, :], corner.at[0], (east, north), "n"),
        5: (pack.at[ROWS - 8 : ROWS, :], corner.at[1], (west, north), "n"),
        6: (pack.at[0:8, :], corner.at[2], (east, south), "s"),
        7: (pack.at[0:8, :], corner.at[3], (west, south), "s"),
        8: (rim_t, rim_got.at[0], (east, gy), None),
        9: (rim_t, rim_got.at[1], (west, gy), None),
        10: (edge.at[1], edge_got.at[0], (gx, north), "n"),
        11: (edge.at[0], edge_got.at[1], (gx, south), "s"),
    }
    HALO, OUTER = range(8), range(8, 12)

    def transfer(which, what):
        def go(keys):
            for k in keys:
                src, dst, to, _ = routes[k]
                copy = pltpu.make_async_remote_copy(
                    src_ref=src, dst_ref=dst, send_sem=send_sem.at[k], recv_sem=recv_sem.at[k],
                    device_id=to, device_id_type=MESH,
                )
                getattr(copy, what)()

        go([k for k in which if routes[k][3] is None])
        for way, other in (("n", "s"), ("s", "n")):
            there = {"n": has_n, "s": has_s}[other if what == "wait_recv" else way]
            pl.when(there)(functools.partial(go, [k for k in which if routes[k][3] == way]))

    hear(barrier)
    transfer((0, 1), "start")
    greet(known)
    transfer(HALO[2:], "start")

    loads[8].wait()
    pair = lanes(BY) // 2
    for b in range(BLOCKS):
        r = b * BY
        packed = None
        for q in range(PLANES):
            moved = pltpu.roll(uvt[q, 8 + r : 8 + r + BY, :], 2 * q + 1, 1)
            packed = moved if packed is None else jnp.where(pair == q, moved, packed)
        rim[r : r + BY, :] = packed
    rim[ROWS:, :] = jnp.zeros((rim.shape[0] - ROWS, COLS), F32)
    for c in range(3):
        rim_t[:, 128 * c : 128 * (c + 1)] = rim[128 * c : 128 * (c + 1), :].T[: 2 * PLANES, :]
    for q in range(PLANES):
        edge[0, q : q + 1, :] = uvt[q, 8 : 9, :]
        edge[1, q : q + 1, :] = uvt[q, 7 + ROWS : 8 + ROWS, :]
    transfer(OUTER, "start")

    def turn(start, size):
        at = slice(start, start + size)
        for i, f in enumerate((WET, UB, VB, X0)):
            value = ext[f, 0, at, :]
            turned[2 * i, at, :] = pltpu.roll(value, COLS - 1, 1)
            if f != X0:
                turned[2 * i + 1, at, :] = pltpu.roll(value, 1, 1)

    for b in range(BLOCKS):
        turn(OFF + b * BY, BY)
    transfer(HALO, "wait_recv")
    hear(known)

    @pl.when((gy // 2 == 1) | (gy // 2 == 2))
    def _():
        pl.semaphore_signal(
            far, inc=1, device_id=(gx, gy + 4 * lax.rem(gy // 2 - 1, 2) - 2), device_id_type=MESH
        )

    low_half = lax.rem(lanes(8), 16) < 8
    nothing = jnp.where(lanes(8) // 16 == HELM, 1.0, 0.0)
    for i, (ref, whole) in enumerate(((from_w, EAST_ROWS), (from_e, WEST_ROWS))):
        half, size = HALVES[i]
        shared = ref[2 * whole :, :]
        tail[i, 0:size, :] = shared
        tail[i, half : half + size, :] = pltpu.roll(shared, COLS // 2, 1)
    for c in range(3):
        w_ref, e_ref = (tail.at[0], tail.at[1]) if c == 2 else (from_w, from_e)
        at_w, at_e = (0, 0) if c == 2 else (EAST_ROWS * c, WEST_ROWS * c)
        for f in range(FIELDS):
            nw, ne = TO_EAST[f], TO_WEST[f]
            got_t[16 * f + 8 - nw : 16 * f + 8, :] = w_ref[at_w : at_w + nw, :]
            got_t[16 * f + 8 : 16 * f + 8 + ne, :] = e_ref[at_e : at_e + ne, :]
            at_w, at_e = at_w + nw, at_e + ne
        block = got_t[...].T
        n = min(128, ROWS - 128 * c)
        got[8 + 128 * c : 8 + 128 * c + n, :] = block[:n, :]
    for k, there, first, halo_at in ((0, has_s, 0, LOW), (2, has_n, 8 + ROWS, OFF + ROWS)):

        @pl.when(there)
        def _(k=k, first=first):
            got[first : first + 8, :] = jnp.where(low_half, corner[k], corner[k + 1])

        @pl.when(jnp.logical_not(there))
        def _(k=k, first=first, halo_at=halo_at):
            got[first : first + 8, :] = nothing
            edge_got[k // 2] = jnp.zeros((16, COLS), F32)
            for f in range(FIELDS):
                ext[f, 0, halo_at : halo_at + 8, :] = jnp.full((8, COLS), 1.0 if f == HELM else 0.0, F32)

    chunks = [(r, STEP) for r in range(LOW, HIGH, STEP)]
    lane = lanes(STEP)
    for r, n in chunks:
        packed = got[r - LOW : r - LOW + n, :]
        for f in range(FIELDS):
            moved = pltpu.roll(packed, COLS - (16 * f + 8), 1)
            came = (lane < TO_WEST[f]) | (lane >= COLS - TO_EAST[f])
            ext[f, 1, r : r + n, :] = jnp.where(came, moved, 1.0 if f == HELM else 0.0)

    turn(LOW, 8)
    turn(OFF + ROWS, 8)

    for r, n in chunks:
        at = slice(r, r + n)
        for t, (c, e, w, nn, s) in enumerate(beside(ext.at[WET], r, n, turned.at[0:2])):
            four = [jnp.minimum(c, o) for o in (e, w, nn, s)]
            total = ext[HELM, t, at, :] + four[0] + four[1] + four[2] + four[3]
            inverse = 1.0 / total
            rdiag[t, at, :] = inverse
            if t == 0:
                diag[at, :] = total
            for k in range(4):
                face[k, t, at, :] = four[k]
                gain[k, t, at, :] = four[k] * inverse
    for r, n in chunks:
        at = slice(r, r + n)
        last = lanes(n) == COLS - 1
        x0, x1 = ext[X0, 0, at, :], ext[X0, 1, at, :]
        e0, e1 = turned[6, at, :], pltpu.roll(x1, COLS - 1, 1)
        slope_e = jnp.where(last, e1, e0) - x0, jnp.where(last, e0, e1) - x1
        for t, x in enumerate((x0, x1)):
            guess[t, at, :] = x
            slopes = slope_e[t], ext[X0, t, r + 1 : r + 1 + n, :] - x
            for k, face_at in ((0, 0), (1, 2)):
                flow[k, t, at, :] = face[face_at, t, at, :] * slopes[k]
    for k, (bar, hat) in enumerate(((UB, UH), (VB, VH))):
        for r, n in chunks:
            at = slice(r, r + n)
            for t, (c, *others) in enumerate(beside(ext.at[bar], r, n, turned.at[2 * k + 2 : 2 * k + 4])):
                spread = sum(face[i, t, at, :] * (o - c) for i, o in enumerate(others))
                flow[k, t, at, :] = ext[WET, t, at, :] * (ext[hat, t, at, :] + 0.1 * spread) - flow[k, t, at, :]

    def image(t, at, others):
        return sum(gain[i, t, at, :] * o for i, o in enumerate(others))

    for r, n in chunks:
        at = slice(r, r + n)
        for t, (ef, efw) in enumerate(west_of(flow.at[0], r, n)):
            nf, nfs = flow[1, t, at, :], flow[1, t, r - 1 : r - 1 + n, :]
            residual = (efw - ef) + (nfs - nf) - ext[HELM, t, at, :] * ext[X0, t, at, :]
            basis[0, t, at, :] = jnp.where(ext[WET, t, at, :] > 0.0, residual * rdiag[t, at, :], 0.0)
    for k in range(3):
        for r, n in chunks:
            at = slice(r, r + n)
            for t, (c, *others) in enumerate(beside(basis.at[k], r, n)):
                value = image(t, at, others)
                if k:
                    value = 2.0 * value - basis[k - 1, t, at, :]
                basis[k + 1, t, at, :] = value
    sums = [jnp.zeros((8, COLS), F32) for _ in range(8)]
    for b in range(BLOCKS):
        r = OFF + b * BY
        at = slice(r, r + BY)
        vectors = [basis[k, 0, at, :] for k in range(4)]
        c = vectors[3]
        right = jnp.where(
            lanes(BY) == COLS - 1, pltpu.roll(basis[3, 1, at, :], COLS - 1, 1), pltpu.roll(c, COLS - 1, 1)
        )
        up = basis[3, 0, r + 1 : r + 1 + BY, :]
        for k in range(4):
            weighted = diag[at, :] * vectors[k]
            sums[2 * k] = sums[2 * k] + eights(weighted * vectors[k])
            if k < 3:
                sums[2 * k + 1] = sums[2 * k + 1] + eights(weighted * vectors[k + 1])
        sums[7] = sums[7] + eights(c * (face[0, 0, at, :] * right + face[2, 0, at, :] * up))
    sums[7] = 4.0 * sums[7] - sums[5]

    rows8 = lax.broadcasted_iota(jnp.int32, (8, COLS), 0)
    mat = jnp.zeros((8, COLS), F32)
    for k in range(8):
        mat = jnp.where(rows8 == k, jnp.sum(sums[k], axis=0, keepdims=True), mat)
    total = jnp.broadcast_to(jnp.sum(mat, axis=1, keepdims=True), (8, COLS))
    row = jnp.sum(jnp.where(lanes(8) == rows8, total, 0.0), axis=0, keepdims=True)

    def level_updates():
        transfer(OUTER, "wait_recv")
        even = lax.rem(lax.broadcasted_iota(jnp.int32, (2 * PLANES, COLS), 0), 2) == 0
        for c in range(3):
            cols = slice(128 * c, 128 * (c + 1))
            from_w, from_e = rim_got[0, :, cols], rim_got[1, :, cols]
            up, down = pltpu.roll(from_e, 2 * PLANES - 1, 0), pltpu.roll(from_w, 1, 0)
            rim_m[0 : 2 * PLANES, :] = jnp.where(even, up, down)
            rim_back[128 * c : 128 * (c + 1), :] = rim_m[...].T
        for q in range(PLANES):
            uvt[q, 7:8, :] = edge_got[0, q : q + 1, :]
            uvt[q, 8 + ROWS : 9 + ROWS, :] = edge_got[1, q : q + 1, :]
        first, last = lanes(BY) == 0, lanes(BY) == COLS - 1

        for b in range(BLOCKS):
            r = b * BY
            rows = slice(r, r + BY)
            at = slice(OFF + r, OFF + r + BY)
            on = act[b : b + 1, :]
            ocean = land[rows, :].astype(F32)
            keep = on * ocean
            kept[rows, :] = keep
            off = 1.0 - on
            cor = coriolis(b)
            faces = [face[k, 0, at, :] for k in range(4)]
            rim_row = rim_back[rows, :]

            def around(q):
                c = uvt[q, 8 + r : 8 + r + BY, :]
                side = pltpu.roll(rim_row, COLS - 1 - 2 * q, 1)
                e = jnp.where(last, side, pltpu.roll(c, COLS - 1, 1))
                w = jnp.where(first, side, pltpu.roll(c, 1, 1))
                return c, e, w, uvt[q, 9 + r : 9 + r + BY, :], uvt[q, 7 + r : 7 + r + BY, :]

            def raw(q0):
                out, keepers = [], []
                for k in range(LEVELS):
                    c, *others = around(q0 + k)
                    spread = sum(faces[i] * (o - c) for i, o in enumerate(others))
                    mix = jnp.zeros_like(c)
                    if k < LEVELS - 1:
                        mix = mix + (uvt[q0 + k + 1, 8 + r : 8 + r + BY, :] - c)
                    if k > 0:
                        mix = mix - (c - uvt[q0 + k - 1, 8 + r : 8 + r + BY, :])
                    out.append((c, 0.5 * mix + 0.5 * spread, others))
                return out

            for k, (c, tend, _) in enumerate(raw(0)):
                star = c + 0.2 * (tend + cor * uvt[LEVELS + k, 8 + r : 8 + r + BY, :])
                u_out[k, rows, :] = keep * star + off * c
            for k, (c, tend, _) in enumerate(raw(LEVELS)):
                star = c + 0.2 * (tend - cor * uvt[k, 8 + r : 8 + r + BY, :])
                v_out[k, rows, :] = keep * star + off * c
            for k, (c, tend, (e, w, nn, s)) in enumerate(raw(2 * LEVELS)):
                uk = uvt[k, 8 + r : 8 + r + BY, :]
                vk = uvt[LEVELS + k, 8 + r : 8 + r + BY, :]
                star = c + 0.2 * (tend - 0.5 * (uk * (e - w) + vk * (nn - s)))
                t_out[k, rows, :] = keep * star + off * c

    @pl.when((gy // 2 == 0) | (gy // 2 == 3))
    def _():
        pl.semaphore_wait(far, 1)

    for s, kind in enumerate(RED_STAGES):
        landing = red[s]
        part[s] = row
        for j, peer in enumerate(peers(kind)):
            pltpu.make_async_remote_copy(
                src_ref=part.at[s], dst_ref=landing.at[j], send_sem=rsend_sem.at[s], recv_sem=rrecv_sem.at[s],
                device_id=peer, device_id_type=MESH,
            ).start()
        if s == 0:
            level_updates()
        every = pltpu.make_async_remote_copy(
            src_ref=landing, dst_ref=landing, send_sem=rsend_sem.at[s], recv_sem=rrecv_sem.at[s],
            device_id=(east, gy), device_id_type=MESH,
        )
        every.wait_recv()
        row = row + jnp.sum(landing[...], axis=0)

    sums_out[...] = row
    transfer(range(12), "wait_send")
    for s in range(len(RED_STAGES)):
        pltpu.make_async_remote_copy(
            src_ref=red[s], dst_ref=red[s], send_sem=rsend_sem.at[s], recv_sem=rrecv_sem.at[s],
            device_id=(east, gy), device_id_type=MESH,
        ).wait_send()


def emit_kernel(u_ref, v_ref, t_ref, basis, guess, kept, sums, u_hbm, v_hbm, t_hbm, p_hbm, u_new, v_new, p_new, sem):
    copies = [pltpu.make_async_copy(t_ref, t_hbm, sem.at[0])]
    copies[0].start()
    row = sums[...]
    c = coefficients([jnp.broadcast_to(row[:, k : k + 1], (1, COLS)) for k in range(8)])

    def answer(t, at):
        x = guess[t, at, :]
        for k in range(4):
            x = x + c[k] * basis[k, t, at, :]
        return x

    last = lanes(EMIT) == COLS - 1
    for b in range(ROWS // EMIT):
        rows = slice(b * EMIT, (b + 1) * EMIT)
        at = slice(OFF + rows.start, OFF + rows.stop)
        x0, x1 = answer(0, at), answer(1, at)
        up = answer(0, slice(at.start + 1, at.stop + 1))
        right = jnp.where(last, pltpu.roll(x1, COLS - 1, 1), pltpu.roll(x0, COLS - 1, 1))
        keep = kept[rows, :]
        p_new[rows, :] = x0
        grad_x, grad_y = keep * (right - x0), keep * (up - x0)
        for k in range(LEVELS):
            u_new[k, rows, :] = u_ref[k, rows, :] - grad_x
            v_new[k, rows, :] = v_ref[k, rows, :] - grad_y
        for i, (src, dst) in enumerate(
            (
                (u_new.at[:, rows, :], u_hbm.at[:, rows, :]),
                (v_new.at[:, rows, :], v_hbm.at[:, rows, :]),
                (p_new.at[rows, :], p_hbm.at[rows, :]),
            )
        ):
            copy = pltpu.make_async_copy(src, dst, sem.at[1 + 3 * b + i])
            copy.start()
            copies.append(copy)
    for copy in copies:
        copy.wait()


def on_device(*args):
    args = args[:7] + (args[7].T, args[8].T)
    args = [pltpu.with_memory_space_constraint(x, pltpu.HBM) for x in args]
    vmem, hbm = pltpu.VMEM, pltpu.HBM
    three = jax.ShapeDtypeStruct((LEVELS, ROWS, COLS), F32)
    two = jax.ShapeDtypeStruct((ROWS, COLS), F32)
    shapes = (three, three, three, two)
    tiles = (2, EXT_ROWS, COLS)
    scratch = [
        vmem((PLANES, ROWS + 16, COLS), F32),
        vmem((ROWS, COLS), F32),
        vmem((ROWS, COLS), F32),
        vmem((ROWS, COLS), jnp.int32),
        vmem((NX_DEV, NBY), jnp.int32),
        vmem((NX_DEV, NBY), jnp.int32),
        vmem((BLOCKS, COLS), F32),
        vmem((BLOCKS, COLS), F32),
        vmem((FIELDS,) + tiles, F32),
        vmem((384, COLS), F32),
        vmem((COLS, COLS), F32),
        vmem((2 * EAST_ROWS + HALVES[0][1], COLS), F32),
        vmem((2 * WEST_ROWS + HALVES[1][1], COLS), F32),
        vmem((2 * EAST_ROWS + HALVES[0][1], COLS), F32),
        vmem((2 * WEST_ROWS + HALVES[1][1], COLS), F32),
        vmem((2, 48, COLS), F32),
        vmem((COLS, COLS), F32),
        vmem((ROWS + 16, COLS), F32),
        vmem((4, 8, COLS), F32),
        vmem((384, COLS), F32),
        vmem((2 * PLANES, 384), F32),
        vmem((2, 2 * PLANES, 384), F32),
        vmem((COLS, COLS), F32),
        vmem((384, COLS), F32),
        vmem((2, 16, COLS), F32),
        vmem((2, 16, COLS), F32),
        vmem((4,) + tiles, F32),
        vmem(tiles, F32),
        vmem((4,) + tiles, F32),
        vmem((EXT_ROWS, COLS), F32),
        vmem((2,) + tiles, F32),
        vmem((7, EXT_ROWS, COLS), F32),
        vmem((len(RED_STAGES), 1, COLS), F32),
        pltpu.SemaphoreType.DMA((9,)),
        pltpu.SemaphoreType.DMA((12,)),
        pltpu.SemaphoreType.DMA((12,)),
        pltpu.SemaphoreType.DMA((len(RED_STAGES),)),
        pltpu.SemaphoreType.DMA((len(RED_STAGES),)),
        pltpu.SemaphoreType.REGULAR,
        pltpu.SemaphoreType.REGULAR,
    ] + [vmem((COUNT[kind], 1, COLS), F32) for kind in RED_STAGES]
    out = pl.pallas_call(
        ocean_kernel,
        out_shape=[vmem(x.shape, F32) for x in (three, three, three)]
        + [vmem((4,) + tiles, F32), vmem(tiles, F32), vmem((ROWS, COLS), F32), vmem((1, COLS), F32)],
        in_specs=[pl.BlockSpec(memory_space=hbm)] * 9,
        out_specs=[pl.BlockSpec(memory_space=vmem)] * 7,
        scratch_shapes=scratch,
        compiler_params=pltpu.CompilerParams(
            collective_id=0, has_side_effects=True, vmem_limit_bytes=VMEM_LIMIT
        ),
        name="ocean",
    )(*args)
    return pl.pallas_call(
        emit_kernel,
        out_shape=shapes,
        in_specs=[pl.BlockSpec(memory_space=vmem)] * 7,
        out_specs=[pl.BlockSpec(memory_space=hbm)] * 4,
        scratch_shapes=[vmem(three.shape, F32), vmem(three.shape, F32), vmem(two.shape, F32)]
        + [pltpu.SemaphoreType.DMA((1 + 3 * (ROWS // EMIT),))],
        compiler_params=pltpu.CompilerParams(vmem_limit_bytes=8 * 1024 * 1024),
        name="emit",
    )(*out)


def solution(mesh):
    wide, flat = P(None, "gy", "gx"), P("gy", "gx")
    return jax.shard_map(
        on_device,
        mesh=mesh,
        in_specs=(wide, wide, wide, flat, flat, flat, flat, P(), P()),
        out_specs=(wide, wide, wide, flat),
        check_vma=False,
    )
```

```python
import functools

import jax
import jax.numpy as jnp
from jax import lax
from jax.experimental import pallas as pl
from jax.experimental.pallas import tpu as pltpu
from jax.sharding import PartitionSpec as P

MESH = pl.DeviceIdType.MESH
F32 = jnp.float32

LEVELS, ROWS, COLS, BY, NY = 4, 320, 128, 40, 2560
BLOCKS, NBY = ROWS // BY, 64
THICK = [(2 * k + 1) / (LEVELS * LEVELS) for k in range(LEVELS)]

OFF = 16
EXT_ROWS = ROWS + 2 * OFF
LOW, HIGH = OFF - 8, OFF + ROWS + 8
STEP = 48
FIELDS = 7
WET, HELM, X0, UB, UH, VB, VH = range(FIELDS)
PLANES = 3 * LEVELS
NX_DEV, NY_DEV = 16, 8

VMEM_LIMIT = 24 * 1024 * 1024
TO_EAST = (6, 4, 5, 6, 5, 5, 4)
TO_WEST = (5, 4, 5, 5, 4, 5, 4)
EAST_ROWS, WEST_ROWS = 40, 32
EMIT = 160
HALVES = ((20, 24), (16, 16))
RED_STAGES = ("all",)


def peers(kind):
    gx, gy = lax.axis_index("gx"), lax.axis_index("gy")
    if kind == "halo":
        return [
            (lax.rem(gx + i, NX_DEV), lax.rem(gy + j, NY_DEV))
            for i in (0, 1, NX_DEV - 1)
            for j in (0, 1, NY_DEV - 1)
            if i or j
        ]
    if kind == "plane":
        base = gx // 4 * 4
        return [
            (base + lax.rem(lax.rem(gx, 4) + i, 4), lax.rem(gy + j, NY_DEV))
            for i in range(4)
            for j in range(NY_DEV)
            if i or j
        ]
    if kind == "z":
        return [(lax.rem(gx + 4 * j, NX_DEV), gy) for j in range(1, 4)]
    return [
        (lax.rem(gx + i, NX_DEV), lax.rem(gy + j, NY_DEV))
        for i in range(NX_DEV)
        for j in range(NY_DEV)
        if i or j
    ]


BESIDE = ((0, 1), (1, 1), (0, 3), (3, 3), (0, 0))
APART = ((1, 0), (3, 0), (1, 3), (3, 1))


def nearby(step, ways):
    gx, gy = lax.axis_index("gx"), lax.axis_index("gy")
    z, y, core = gx // 4, lax.rem(gx, 4), lax.rem(gy, 2)
    return [
        (lax.rem(z + i, 4) * 4 + lax.rem(y + j, 4), gy + 2 * step if c == 0 else gy + 2 * step + 1 - 2 * core)
        for i, j in ways
        for c in (0, 1)
        if i or j or c or step
    ]


COUNT = {"all": 127, "plane": 31, "z": 3}


def lanes(rows):
    return lax.broadcasted_iota(jnp.int32, (rows, COLS), 1)


def beside(ref, r, n, turned=None):
    lane = lanes(n)
    first, last = lane == 0, lane == COLS - 1
    c0, c1 = ref[0, r : r + n, :], ref[1, r : r + n, :]
    if turned is None:
        e0, w0 = pltpu.roll(c0, COLS - 1, 1), pltpu.roll(c0, 1, 1)
    else:
        e0, w0 = turned[0, r : r + n, :], turned[1, r : r + n, :]
    e1, w1 = pltpu.roll(c1, COLS - 1, 1), pltpu.roll(c1, 1, 1)
    return [
        (
            c,
            jnp.where(last, other_e, own_e),
            jnp.where(first, other_w, own_w),
            ref[t, r + 1 : r + 1 + n, :],
            ref[t, r - 1 : r - 1 + n, :],
        )
        for t, (c, own_e, other_e, own_w, other_w) in enumerate(((c0, e0, e1, w0, w1), (c1, e1, e0, w1, w0)))
    ]


def west_of(ref, r, n):
    first = lanes(n) == 0
    c0, c1 = ref[0, r : r + n, :], ref[1, r : r + n, :]
    w0, w1 = pltpu.roll(c0, 1, 1), pltpu.roll(c1, 1, 1)
    return (c0, jnp.where(first, w1, w0)), (c1, jnp.where(first, w0, w1))


def eights(x):
    return jnp.sum(x.reshape(x.shape[0] // 8, 8, COLS), axis=0)


def coefficients(sums):
    m = [sums[0], sums[1]]
    for k in range(2, 8):
        m.append(2.0 * sums[k] - m[k % 2])
    g = [[0.5 * (m[i + j] + m[abs(i - j)]) for j in range(5) if i + j < 8] for i in range(4)]

    def image(i, j):
        if j == 0:
            return g[i][1]
        return 0.5 * (g[i][j + 1] + g[i][j - 1])

    a = [[g[i][j] - image(i, j) for j in range(i + 1)] for i in range(4)]
    low = [[None] * 4 for _ in range(4)]
    inv, piv = [], []
    for j in range(4):
        pivot = a[j][j]
        for k in range(j):
            pivot = pivot - low[j][k] * low[j][k] * piv[k]
        good = pivot > 1e-6 * a[j][j]
        piv.append(jnp.where(good, pivot, 0.0))
        inv.append(jnp.where(good, 1.0 / jnp.where(good, pivot, 1.0), 0.0))
        for i in range(j + 1, 4):
            s = a[i][j]
            for k in range(j):
                s = s - low[i][k] * low[j][k] * piv[k]
            low[i][j] = s * inv[j]
    y = []
    for i in range(4):
        s = m[i]
        for k in range(i):
            s = s - low[i][k] * y[k]
        y.append(s)
    c = [None] * 4
    for i in reversed(range(4)):
        s = y[i] * inv[i]
        for k in range(i + 1, 4):
            s = s - low[k][i] * c[k]
        c[i] = s
    return c


def ocean_kernel(
    u_hbm, v_hbm, t_hbm, p_hbm, depth_hbm, helm_hbm, land_hbm, clinic_hbm, tropic_hbm,
    u_out, v_out, t_out, basis, guess, kept, sums_out,
    uvt, pold, depth, land, cmap, tmap, act, dom,
    ext, pack, pack_t, for_e, for_w, from_w, from_e, tail, got_t, got, corner,
    rim, rim_t, rim_got, rim_m, rim_back, edge, edge_got,
    face, rdiag, gain, diag, flow, turned, part,
    in_sem, send_sem, recv_sem, rsend_sem, rrecv_sem, known, far, *red,
):
    gx, gy = lax.axis_index("gx"), lax.axis_index("gy")
    east, west = lax.rem(gx + 1, NX_DEV), lax.rem(gx + NX_DEV - 1, NX_DEV)
    north, south = lax.rem(gy + 1, NY_DEV), lax.rem(gy + NY_DEV - 1, NY_DEV)
    own = pl.ds(OFF, ROWS)

    loads = [
        pltpu.make_async_copy(u_hbm, uvt.at[0:4, 8 : 8 + ROWS, :], in_sem.at[0]),
        pltpu.make_async_copy(v_hbm, uvt.at[4:8, 8 : 8 + ROWS, :], in_sem.at[1]),
        pltpu.make_async_copy(p_hbm, pold, in_sem.at[2]),
        pltpu.make_async_copy(depth_hbm, depth, in_sem.at[3]),
        pltpu.make_async_copy(land_hbm, land, in_sem.at[4]),
        pltpu.make_async_copy(clinic_hbm, cmap, in_sem.at[5]),
        pltpu.make_async_copy(tropic_hbm, tmap, in_sem.at[6]),
        pltpu.make_async_copy(helm_hbm, ext.at[HELM, 0, OFF : OFF + ROWS, :], in_sem.at[7]),
        pltpu.make_async_copy(t_hbm, uvt.at[8:12, 8 : 8 + ROWS, :], in_sem.at[8]),
    ]
    barrier = pltpu.get_barrier_semaphore()
    has_n, has_s = gy < NY_DEV - 1, gy > 0
    up_x, down_x = gy < NY_DEV - 2, gy > 1

    def greet(sem):
        for ways in (BESIDE, APART):
            for step, there in ((0, None), (1, up_x), (-1, down_x)):

                def tell(step=step, ways=ways):
                    for peer in nearby(step, ways):
                        pl.semaphore_signal(sem, inc=1, device_id=peer, device_id_type=MESH)

                tell() if there is None else pl.when(there)(tell)

    def hear(sem):
        inner = lax.rem((gy // 2 + 1) // 2, 2)
        pl.semaphore_wait(sem, 35 + 18 * inner)

    greet(barrier)
    for load in loads:
        load.start()

    pack[ROWS:, :] = jnp.zeros((pack.shape[0] - ROWS, COLS), F32)
    for load in loads[:8]:
        load.wait()

    shape = (NX_DEV, NBY)
    mine = lax.broadcasted_iota(jnp.int32, shape, 0) == gx
    shape = (BLOCKS, NBY)
    wanted = lax.broadcasted_iota(jnp.int32, shape, 1) == lax.broadcasted_iota(jnp.int32, shape, 0) + gy * BLOCKS

    def per_block(flags):
        line = jnp.sum(jnp.where(mine, flags, 0.0), axis=0, keepdims=True)
        column = jnp.sum(jnp.where(wanted, line, 0.0), axis=1, keepdims=True)
        return jnp.broadcast_to(column, (BLOCKS, COLS))

    act[...] = per_block(cmap[...].astype(F32))
    dom[...] = per_block(jnp.where(tmap[...] >= 0, 1.0, 0.0))

    def coriolis(b):
        row = lax.broadcasted_iota(jnp.int32, (BY, COLS), 0) + (gy * ROWS + b * BY)
        return 0.2 + 0.6 * ((row.astype(F32) + 0.5) / NY)

    group = lanes(BY) // 16
    for b in range(BLOCKS):
        r = b * BY
        rows = slice(r, r + BY)
        solve = land[rows, :].astype(F32) * dom[b : b + 1, :]
        wet = depth[rows, :] * solve
        u = [uvt[k, 8 + r : 8 + r + BY, :] for k in range(LEVELS)]
        v = [uvt[LEVELS + k, 8 + r : 8 + r + BY, :] for k in range(LEVELS)]
        u_bar = sum(THICK[k] * u[k] for k in range(LEVELS))
        v_bar = sum(THICK[k] * v[k] for k in range(LEVELS))
        cor = 0.2 * coriolis(b)
        mix = 0.1 * (THICK[1] - THICK[0])
        u_hat = u_bar + mix * (u[0] - u[3]) + cor * v_bar
        v_hat = v_bar + mix * (v[0] - v[3]) - cor * u_bar
        fields = [wet, ext[HELM, 0, OFF + r : OFF + r + BY, :], solve * pold[rows, :], u_bar, u_hat, v_bar, v_hat]
        packed = None
        for f, value in enumerate(fields):
            if f != HELM:
                ext[f, 0, OFF + r : OFF + r + BY, :] = value
            moved = pltpu.roll(value, 8 + 16 * f, 1)
            packed = moved if packed is None else jnp.where(group == f, moved, packed)
        pack[rows, :] = packed
    for c in range(3):
        pack_t[...] = pack[128 * c : 128 * (c + 1), :].T
        e_ref, w_ref = (tail.at[0], tail.at[1]) if c == 2 else (for_e, for_w)
        at_e, at_w = (0, 0) if c == 2 else (EAST_ROWS * c, WEST_ROWS * c)
        for f in range(FIELDS):
            ne, nw = TO_EAST[f], TO_WEST[f]
            e_ref[at_e : at_e + ne, :] = pack_t[16 * f + 8 - ne : 16 * f + 8, :]
            w_ref[at_w : at_w + nw, :] = pack_t[16 * f + 8 : 16 * f + 8 + nw, :]
            at_e, at_w = at_e + ne, at_w + nw
    for i, (ref, whole) in enumerate(((for_e, EAST_ROWS), (for_w, WEST_ROWS))):
        half, size = HALVES[i]
        moved = pltpu.roll(tail[i, half : half + size, :], COLS // 2, 1)
        ref[2 * whole :, :] = jnp.where(lanes(size) < COLS // 2, tail[i, 0:size, :], moved)

    routes = {
        0: (for_e, from_w, (east, gy), None),
        1: (for_w, from_e, (west, gy), None),
        2: (ext.at[:, 0, OFF + ROWS - 8 : OFF + ROWS, :], ext.at[:, 0, LOW:OFF, :], (gx, north), "n"),
        3: (ext.at[:, 0, OFF : OFF + 8, :], ext.at[:, 0, OFF + ROWS : HIGH, :], (gx, south), "s"),
        4: (pack.at[ROWS - 8 : ROWS, :], corner.at[0], (east, north), "n"),
        5: (pack.at[ROWS - 8 : ROWS, :], corner.at[1], (west, north), "n"),
        6: (pack.at[0:8, :], corner.at[2], (east, south), "s"),
        7: (pack.at[0:8, :], corner.at[3], (west, south), "s"),
        8: (rim_t, rim_got.at[0], (east, gy), None),
        9: (rim_t, rim_got.at[1], (west, gy), None),
        10: (edge.at[1], edge_got.at[0], (gx, north), "n"),
        11: (edge.at[0], edge_got.at[1], (gx, south), "s"),
    }
    HALO, OUTER = range(8), range(8, 12)

    def transfer(which, what):
        def go(keys):
            for k in keys:
                src, dst, to, _ = routes[k]
                copy = pltpu.make_async_remote_copy(
                    src_ref=src, dst_ref=dst, send_sem=send_sem.at[k], recv_sem=recv_sem.at[k],
                    device_id=to, device_id_type=MESH,
                )
                getattr(copy, what)()

        go([k for k in which if routes[k][3] is None])
        for way, other in (("n", "s"), ("s", "n")):
            there = {"n": has_n, "s": has_s}[other if what == "wait_recv" else way]
            pl.when(there)(functools.partial(go, [k for k in which if routes[k][3] == way]))

    hear(barrier)
    transfer((4, 5, 6, 7), "start")
    transfer((0, 1), "start")
    transfer((2, 3), "start")
    greet(known)

    loads[8].wait()
    pair = lanes(BY) // 2
    for b in range(BLOCKS):
        r = b * BY
        packed = None
        for q in range(PLANES):
            moved = pltpu.roll(uvt[q, 8 + r : 8 + r + BY, :], 2 * q + 1, 1)
            packed = moved if packed is None else jnp.where(pair == q, moved, packed)
        rim[r : r + BY, :] = packed
    rim[ROWS:, :] = jnp.zeros((rim.shape[0] - ROWS, COLS), F32)
    for c in range(3):
        rim_t[:, 128 * c : 128 * (c + 1)] = rim[128 * c : 128 * (c + 1), :].T[: 2 * PLANES, :]
    for q in range(PLANES):
        edge[0, q : q + 1, :] = uvt[q, 8 : 9, :]
        edge[1, q : q + 1, :] = uvt[q, 7 + ROWS : 8 + ROWS, :]
    def turn(start, size):
        at = slice(start, start + size)
        for i, f in enumerate((WET, UB, VB, X0)):
            value = ext[f, 0, at, :]
            turned[2 * i, at, :] = pltpu.roll(value, COLS - 1, 1)
            if f != X0:
                turned[2 * i + 1, at, :] = pltpu.roll(value, 1, 1)

    for b in range(BLOCKS):
        turn(OFF + b * BY, BY)
    transfer((0, 1), "wait_send")
    transfer(OUTER, "start")
    transfer(HALO, "wait_recv")
    hear(known)

    @pl.when((gy // 2 == 1) | (gy // 2 == 2))
    def _():
        pl.semaphore_signal(
            far, inc=1, device_id=(gx, gy + 4 * lax.rem(gy // 2 - 1, 2) - 2), device_id_type=MESH
        )

    low_half = lax.rem(lanes(8), 16) < 8
    nothing = jnp.where(lanes(8) // 16 == HELM, 1.0, 0.0)
    for i, (ref, whole) in enumerate(((from_w, EAST_ROWS), (from_e, WEST_ROWS))):
        half, size = HALVES[i]
        shared = ref[2 * whole :, :]
        tail[i, 0:size, :] = shared
        tail[i, half : half + size, :] = pltpu.roll(shared, COLS // 2, 1)
    for c in range(3):
        w_ref, e_ref = (tail.at[0], tail.at[1]) if c == 2 else (from_w, from_e)
        at_w, at_e = (0, 0) if c == 2 else (EAST_ROWS * c, WEST_ROWS * c)
        for f in range(FIELDS):
            nw, ne = TO_EAST[f], TO_WEST[f]
            got_t[16 * f + 8 - nw : 16 * f + 8, :] = w_ref[at_w : at_w + nw, :]
            got_t[16 * f + 8 : 16 * f + 8 + ne, :] = e_ref[at_e : at_e + ne, :]
            at_w, at_e = at_w + nw, at_e + ne
        block = got_t[...].T
        n = min(128, ROWS - 128 * c)
        got[8 + 128 * c : 8 + 128 * c + n, :] = block[:n, :]
    for k, there, first, halo_at in ((0, has_s, 0, LOW), (2, has_n, 8 + ROWS, OFF + ROWS)):

        @pl.when(there)
        def _(k=k, first=first):
            got[first : first + 8, :] = jnp.where(low_half, corner[k], corner[k + 1])

        @pl.when(jnp.logical_not(there))
        def _(k=k, first=first, halo_at=halo_at):
            got[first : first + 8, :] = nothing
            edge_got[k // 2] = jnp.zeros((16, COLS), F32)
            for f in range(FIELDS):
                ext[f, 0, halo_at : halo_at + 8, :] = jnp.full((8, COLS), 1.0 if f == HELM else 0.0, F32)

    chunks = [(r, STEP) for r in range(LOW, HIGH, STEP)]
    lane = lanes(STEP)
    for r, n in chunks:
        packed = got[r - LOW : r - LOW + n, :]
        for f in range(FIELDS):
            moved = pltpu.roll(packed, COLS - (16 * f + 8), 1)
            came = (lane < TO_WEST[f]) | (lane >= COLS - TO_EAST[f])
            ext[f, 1, r : r + n, :] = jnp.where(came, moved, 1.0 if f == HELM else 0.0)

    turn(LOW, 8)
    turn(OFF + ROWS, 8)

    for r, n in chunks:
        at = slice(r, r + n)
        for t, (c, e, w, nn, s) in enumerate(beside(ext.at[WET], r, n, turned.at[0:2])):
            four = [jnp.minimum(c, o) for o in (e, w, nn, s)]
            total = ext[HELM, t, at, :] + four[0] + four[1] + four[2] + four[3]
            inverse = 1.0 / total
            rdiag[t, at, :] = inverse
            if t == 0:
                diag[at, :] = total
            for k in range(4):
                face[k, t, at, :] = four[k]
                gain[k, t, at, :] = four[k] * inverse
    for r, n in chunks:
        at = slice(r, r + n)
        last = lanes(n) == COLS - 1
        x0, x1 = ext[X0, 0, at, :], ext[X0, 1, at, :]
        e0, e1 = turned[6, at, :], pltpu.roll(x1, COLS - 1, 1)
        slope_e = jnp.where(last, e1, e0) - x0, jnp.where(last, e0, e1) - x1
        for t, x in enumerate((x0, x1)):
            guess[t, at, :] = x
            slopes = slope_e[t], ext[X0, t, r + 1 : r + 1 + n, :] - x
            for k, face_at in ((0, 0), (1, 2)):
                flow[k, t, at, :] = face[face_at, t, at, :] * slopes[k]
    for k, (bar, hat) in enumerate(((UB, UH), (VB, VH))):
        for r, n in chunks:
            at = slice(r, r + n)
            for t, (c, *others) in enumerate(beside(ext.at[bar], r, n, turned.at[2 * k + 2 : 2 * k + 4])):
                spread = sum(face[i, t, at, :] * (o - c) for i, o in enumerate(others))
                flow[k, t, at, :] = ext[WET, t, at, :] * (ext[hat, t, at, :] + 0.1 * spread) - flow[k, t, at, :]

    def image(t, at, others):
        return sum(gain[i, t, at, :] * o for i, o in enumerate(others))

    for r, n in chunks:
        at = slice(r, r + n)
        for t, (ef, efw) in enumerate(west_of(flow.at[0], r, n)):
            nf, nfs = flow[1, t, at, :], flow[1, t, r - 1 : r - 1 + n, :]
            residual = (efw - ef) + (nfs - nf) - ext[HELM, t, at, :] * ext[X0, t, at, :]
            basis[0, t, at, :] = jnp.where(ext[WET, t, at, :] > 0.0, residual * rdiag[t, at, :], 0.0)
    for k in range(3):
        for r, n in chunks:
            at = slice(r, r + n)
            for t, (c, *others) in enumerate(beside(basis.at[k], r, n)):
                value = image(t, at, others)
                if k:
                    value = 2.0 * value - basis[k - 1, t, at, :]
                basis[k + 1, t, at, :] = value
    sums = [jnp.zeros((8, COLS), F32) for _ in range(8)]
    for b in range(BLOCKS):
        r = OFF + b * BY
        at = slice(r, r + BY)
        vectors = [basis[k, 0, at, :] for k in range(4)]
        c = vectors[3]
        right = jnp.where(
            lanes(BY) == COLS - 1, pltpu.roll(basis[3, 1, at, :], COLS - 1, 1), pltpu.roll(c, COLS - 1, 1)
        )
        up = basis[3, 0, r + 1 : r + 1 + BY, :]
        for k in range(4):
            weighted = diag[at, :] * vectors[k]
            sums[2 * k] = sums[2 * k] + eights(weighted * vectors[k])
            if k < 3:
                sums[2 * k + 1] = sums[2 * k + 1] + eights(weighted * vectors[k + 1])
        sums[7] = sums[7] + eights(c * (face[0, 0, at, :] * right + face[2, 0, at, :] * up))
    sums[7] = 4.0 * sums[7] - sums[5]

    rows8 = lax.broadcasted_iota(jnp.int32, (8, COLS), 0)
    mat = jnp.zeros((8, COLS), F32)
    for k in range(8):
        mat = jnp.where(rows8 == k, jnp.sum(sums[k], axis=0, keepdims=True), mat)
    total = jnp.broadcast_to(jnp.sum(mat, axis=1, keepdims=True), (8, COLS))
    row = jnp.sum(jnp.where(lanes(8) == rows8, total, 0.0), axis=0, keepdims=True)

    def level_updates():
        transfer(OUTER, "wait_recv")
        even = lax.rem(lax.broadcasted_iota(jnp.int32, (2 * PLANES, COLS), 0), 2) == 0
        for c in range(3):
            cols = slice(128 * c, 128 * (c + 1))
            from_w, from_e = rim_got[0, :, cols], rim_got[1, :, cols]
            up, down = pltpu.roll(from_e, 2 * PLANES - 1, 0), pltpu.roll(from_w, 1, 0)
            rim_m[0 : 2 * PLANES, :] = jnp.where(even, up, down)
            rim_back[128 * c : 128 * (c + 1), :] = rim_m[...].T
        for q in range(PLANES):
            uvt[q, 7:8, :] = edge_got[0, q : q + 1, :]
            uvt[q, 8 + ROWS : 9 + ROWS, :] = edge_got[1, q : q + 1, :]
        first, last = lanes(BY) == 0, lanes(BY) == COLS - 1

        for b in range(BLOCKS):
            r = b * BY
            rows = slice(r, r + BY)
            at = slice(OFF + r, OFF + r + BY)
            on = act[b : b + 1, :]
            ocean = land[rows, :].astype(F32)
            keep = on * ocean
            kept[rows, :] = keep
            off = 1.0 - on
            cor = coriolis(b)
            faces = [face[k, 0, at, :] for k in range(4)]
            rim_row = rim_back[rows, :]

            def around(q):
                c = uvt[q, 8 + r : 8 + r + BY, :]
                side = pltpu.roll(rim_row, COLS - 1 - 2 * q, 1)
                e = jnp.where(last, side, pltpu.roll(c, COLS - 1, 1))
                w = jnp.where(first, side, pltpu.roll(c, 1, 1))
                return c, e, w, uvt[q, 9 + r : 9 + r + BY, :], uvt[q, 7 + r : 7 + r + BY, :]

            def raw(q0):
                out, keepers = [], []
                for k in range(LEVELS):
                    c, *others = around(q0 + k)
                    spread = sum(faces[i] * (o - c) for i, o in enumerate(others))
                    mix = jnp.zeros_like(c)
                    if k < LEVELS - 1:
                        mix = mix + (uvt[q0 + k + 1, 8 + r : 8 + r + BY, :] - c)
                    if k > 0:
                        mix = mix - (c - uvt[q0 + k - 1, 8 + r : 8 + r + BY, :])
                    out.append((c, 0.5 * mix + 0.5 * spread, others))
                return out

            for k, (c, tend, _) in enumerate(raw(0)):
                star = c + 0.2 * (tend + cor * uvt[LEVELS + k, 8 + r : 8 + r + BY, :])
                u_out[k, rows, :] = keep * star + off * c
            for k, (c, tend, _) in enumerate(raw(LEVELS)):
                star = c + 0.2 * (tend - cor * uvt[k, 8 + r : 8 + r + BY, :])
                v_out[k, rows, :] = keep * star + off * c
            for k, (c, tend, (e, w, nn, s)) in enumerate(raw(2 * LEVELS)):
                uk = uvt[k, 8 + r : 8 + r + BY, :]
                vk = uvt[LEVELS + k, 8 + r : 8 + r + BY, :]
                star = c + 0.2 * (tend - 0.5 * (uk * (e - w) + vk * (nn - s)))
                t_out[k, rows, :] = keep * star + off * c

    @pl.when((gy // 2 == 0) | (gy // 2 == 3))
    def _():
        pl.semaphore_wait(far, 1)

    for s, kind in enumerate(RED_STAGES):
        landing = red[s]
        part[s] = row
        for j, peer in enumerate(peers(kind)):
            pltpu.make_async_remote_copy(
                src_ref=part.at[s], dst_ref=landing.at[j], send_sem=rsend_sem.at[s], recv_sem=rrecv_sem.at[s],
                device_id=peer, device_id_type=MESH,
            ).start()
        if s == 0:
            level_updates()
        every = pltpu.make_async_remote_copy(
            src_ref=landing, dst_ref=landing, send_sem=rsend_sem.at[s], recv_sem=rrecv_sem.at[s],
            device_id=(east, gy), device_id_type=MESH,
        )
        every.wait_recv()
        parts = [jnp.sum(landing[j : min(j + 16, COUNT[kind])], axis=0) for j in range(0, COUNT[kind], 16)]
        while len(parts) > 1:
            parts = [sum(parts[j : j + 2]) for j in range(0, len(parts), 2)]
        row = row + parts[0]

    sums_out[...] = row
    transfer(range(2, 12), "wait_send")
    for s in range(len(RED_STAGES)):
        pltpu.make_async_remote_copy(
            src_ref=red[s], dst_ref=red[s], send_sem=rsend_sem.at[s], recv_sem=rrecv_sem.at[s],
            device_id=(east, gy), device_id_type=MESH,
        ).wait_send()


def emit_kernel(u_ref, v_ref, t_ref, basis, guess, kept, sums, u_hbm, v_hbm, t_hbm, p_hbm, u_new, v_new, p_new, sem):
    copies = [pltpu.make_async_copy(t_ref, t_hbm, sem.at[0])]
    copies[0].start()
    row = sums[...]
    c = coefficients([jnp.broadcast_to(row[:, k : k + 1], (1, COLS)) for k in range(8)])

    def answer(t, at):
        x = guess[t, at, :]
        for k in range(4):
            x = x + c[k] * basis[k, t, at, :]
        return x

    last = lanes(EMIT) == COLS - 1
    for b in range(ROWS // EMIT):
        rows = slice(b * EMIT, (b + 1) * EMIT)
        at = slice(OFF + rows.start, OFF + rows.stop)
        x0, x1 = answer(0, at), answer(1, at)
        up = answer(0, slice(at.start + 1, at.stop + 1))
        right = jnp.where(last, pltpu.roll(x1, COLS - 1, 1), pltpu.roll(x0, COLS - 1, 1))
        keep = kept[rows, :]
        p_new[rows, :] = x0
        grad_x, grad_y = keep * (right - x0), keep * (up - x0)
        for k in range(LEVELS):
            u_new[k, rows, :] = u_ref[k, rows, :] - grad_x
            v_new[k, rows, :] = v_ref[k, rows, :] - grad_y
        for i, (src, dst) in enumerate(
            (
                (u_new.at[:, rows, :], u_hbm.at[:, rows, :]),
                (v_new.at[:, rows, :], v_hbm.at[:, rows, :]),
                (p_new.at[rows, :], p_hbm.at[rows, :]),
            )
        ):
            copy = pltpu.make_async_copy(src, dst, sem.at[1 + 3 * b + i])
            copy.start()
            copies.append(copy)
    for copy in copies:
        copy.wait()


def on_device(*args):
    args = args[:7] + (args[7].T, args[8].T)
    args = [pltpu.with_memory_space_constraint(x, pltpu.HBM) for x in args]
    vmem, hbm = pltpu.VMEM, pltpu.HBM
    three = jax.ShapeDtypeStruct((LEVELS, ROWS, COLS), F32)
    two = jax.ShapeDtypeStruct((ROWS, COLS), F32)
    shapes = (three, three, three, two)
    tiles = (2, EXT_ROWS, COLS)
    scratch = [
        vmem((PLANES, ROWS + 16, COLS), F32),
        vmem((ROWS, COLS), F32),
        vmem((ROWS, COLS), F32),
        vmem((ROWS, COLS), jnp.int32),
        vmem((NX_DEV, NBY), jnp.int32),
        vmem((NX_DEV, NBY), jnp.int32),
        vmem((BLOCKS, COLS), F32),
        vmem((BLOCKS, COLS), F32),
        vmem((FIELDS,) + tiles, F32),
        vmem((384, COLS), F32),
        vmem((COLS, COLS), F32),
        vmem((2 * EAST_ROWS + HALVES[0][1], COLS), F32),
        vmem((2 * WEST_ROWS + HALVES[1][1], COLS), F32),
        vmem((2 * EAST_ROWS + HALVES[0][1], COLS), F32),
        vmem((2 * WEST_ROWS + HALVES[1][1], COLS), F32),
        vmem((2, 48, COLS), F32),
        vmem((COLS, COLS), F32),
        vmem((ROWS + 16, COLS), F32),
        vmem((4, 8, COLS), F32),
        vmem((384, COLS), F32),
        vmem((2 * PLANES, 384), F32),
        vmem((2, 2 * PLANES, 384), F32),
        vmem((COLS, COLS), F32),
        vmem((384, COLS), F32),
        vmem((2, 16, COLS), F32),
        vmem((2, 16, COLS), F32),
        vmem((4,) + tiles, F32),
        vmem(tiles, F32),
        vmem((4,) + tiles, F32),
        vmem((EXT_ROWS, COLS), F32),
        vmem((2,) + tiles, F32),
        vmem((7, EXT_ROWS, COLS), F32),
        vmem((len(RED_STAGES), 1, COLS), F32),
        pltpu.SemaphoreType.DMA((9,)),
        pltpu.SemaphoreType.DMA((12,)),
        pltpu.SemaphoreType.DMA((12,)),
        pltpu.SemaphoreType.DMA((len(RED_STAGES),)),
        pltpu.SemaphoreType.DMA((len(RED_STAGES),)),
        pltpu.SemaphoreType.REGULAR,
        pltpu.SemaphoreType.REGULAR,
    ] + [vmem((COUNT[kind], 1, COLS), F32) for kind in RED_STAGES]
    out = pl.pallas_call(
        ocean_kernel,
        out_shape=[vmem(x.shape, F32) for x in (three, three, three)]
        + [vmem((4,) + tiles, F32), vmem(tiles, F32), vmem((ROWS, COLS), F32), vmem((1, COLS), F32)],
        in_specs=[pl.BlockSpec(memory_space=hbm)] * 9,
        out_specs=[pl.BlockSpec(memory_space=vmem)] * 7,
        scratch_shapes=scratch,
        compiler_params=pltpu.CompilerParams(
            collective_id=0, has_side_effects=True, vmem_limit_bytes=VMEM_LIMIT
        ),
        name="ocean",
    )(*args)
    return pl.pallas_call(
        emit_kernel,
        out_shape=shapes,
        in_specs=[pl.BlockSpec(memory_space=vmem)] * 7,
        out_specs=[pl.BlockSpec(memory_space=hbm)] * 4,
        scratch_shapes=[vmem(three.shape, F32), vmem(three.shape, F32), vmem(two.shape, F32)]
        + [pltpu.SemaphoreType.DMA((1 + 3 * (ROWS // EMIT),))],
        compiler_params=pltpu.CompilerParams(vmem_limit_bytes=8 * 1024 * 1024),
        name="emit",
    )(*out)


def solution(mesh):
    wide, flat = P(None, "gy", "gx"), P("gy", "gx")
    return jax.shard_map(
        on_device,
        mesh=mesh,
        in_specs=(wide, wide, wide, flat, flat, flat, flat, P(), P()),
        out_specs=(wide, wide, wide, flat),
        check_vma=False,
    )
```

```python
import functools

import jax
import jax.numpy as jnp
from jax import lax
from jax.experimental import pallas as pl
from jax.experimental.pallas import tpu as pltpu
from jax.sharding import PartitionSpec as P

MESH = pl.DeviceIdType.MESH
F32 = jnp.float32

LEVELS, ROWS, COLS, BY, NY = 4, 320, 128, 40, 2560
BLOCKS, NBY = ROWS // BY, 64
THICK = [(2 * k + 1) / (LEVELS * LEVELS) for k in range(LEVELS)]

OFF = 16
EXT_ROWS = ROWS + 2 * OFF
LOW, HIGH = OFF - 8, OFF + ROWS + 8
STEP = 48
FIELDS = 7
WET, HELM, X0, UB, UH, VB, VH = range(FIELDS)
PLANES = 3 * LEVELS
NX_DEV, NY_DEV = 16, 8

VMEM_LIMIT = 24 * 1024 * 1024
TO_EAST = (6, 4, 5, 6, 5, 5, 4)
TO_WEST = (5, 4, 5, 5, 4, 5, 4)
EAST_ROWS, WEST_ROWS = 40, 32
EMIT = 160
HALVES = ((20, 24), (16, 16))
RED_STAGES = ("all",)


def peers(kind):
    gx, gy = lax.axis_index("gx"), lax.axis_index("gy")
    if kind == "halo":
        return [
            (lax.rem(gx + i, NX_DEV), lax.rem(gy + j, NY_DEV))
            for i in (0, 1, NX_DEV - 1)
            for j in (0, 1, NY_DEV - 1)
            if i or j
        ]
    if kind == "plane":
        base = gx // 4 * 4
        return [
            (base + lax.rem(lax.rem(gx, 4) + i, 4), lax.rem(gy + j, NY_DEV))
            for i in range(4)
            for j in range(NY_DEV)
            if i or j
        ]
    if kind == "z":
        return [(lax.rem(gx + 4 * j, NX_DEV), gy) for j in range(1, 4)]
    return [
        (lax.rem(gx + i, NX_DEV), lax.rem(gy + j, NY_DEV))
        for i in range(NX_DEV)
        for j in range(NY_DEV)
        if i or j
    ]


BESIDE = ((0, 1), (1, 1), (0, 3), (3, 3), (0, 0))
APART = ((1, 0), (3, 0), (1, 3), (3, 1))


def nearby(step, ways):
    gx, gy = lax.axis_index("gx"), lax.axis_index("gy")
    z, y, core = gx // 4, lax.rem(gx, 4), lax.rem(gy, 2)
    return [
        (lax.rem(z + i, 4) * 4 + lax.rem(y + j, 4), gy + 2 * step if c == 0 else gy + 2 * step + 1 - 2 * core)
        for i, j in ways
        for c in (0, 1)
        if i or j or c or step
    ]


COUNT = {"all": 127, "plane": 31, "z": 3}


def lanes(rows):
    return lax.broadcasted_iota(jnp.int32, (rows, COLS), 1)


def beside(ref, r, n, turned=None):
    lane = lanes(n)
    first, last = lane == 0, lane == COLS - 1
    c0, c1 = ref[0, r : r + n, :], ref[1, r : r + n, :]
    if turned is None:
        e0, w0 = pltpu.roll(c0, COLS - 1, 1), pltpu.roll(c0, 1, 1)
    else:
        e0, w0 = turned[0, r : r + n, :], turned[1, r : r + n, :]
    e1, w1 = pltpu.roll(c1, COLS - 1, 1), pltpu.roll(c1, 1, 1)
    return [
        (
            c,
            jnp.where(last, other_e, own_e),
            jnp.where(first, other_w, own_w),
            ref[t, r + 1 : r + 1 + n, :],
            ref[t, r - 1 : r - 1 + n, :],
        )
        for t, (c, own_e, other_e, own_w, other_w) in enumerate(((c0, e0, e1, w0, w1), (c1, e1, e0, w1, w0)))
    ]


def west_of(ref, r, n):
    first = lanes(n) == 0
    c0, c1 = ref[0, r : r + n, :], ref[1, r : r + n, :]
    w0, w1 = pltpu.roll(c0, 1, 1), pltpu.roll(c1, 1, 1)
    return (c0, jnp.where(first, w1, w0)), (c1, jnp.where(first, w0, w1))


def eights(x):
    return jnp.sum(x.reshape(x.shape[0] // 8, 8, COLS), axis=0)


def coefficients(sums):
    m = [sums[0], sums[1]]
    for k in range(2, 8):
        m.append(2.0 * sums[k] - m[k % 2])
    g = [[0.5 * (m[i + j] + m[abs(i - j)]) for j in range(5) if i + j < 8] for i in range(4)]

    def image(i, j):
        if j == 0:
            return g[i][1]
        return 0.5 * (g[i][j + 1] + g[i][j - 1])

    a = [[g[i][j] - image(i, j) for j in range(i + 1)] for i in range(4)]
    low = [[None] * 4 for _ in range(4)]
    inv, piv = [], []
    for j in range(4):
        pivot = a[j][j]
        for k in range(j):
            pivot = pivot - low[j][k] * low[j][k] * piv[k]
        good = pivot > 1e-6 * a[j][j]
        piv.append(jnp.where(good, pivot, 0.0))
        inv.append(jnp.where(good, 1.0 / jnp.where(good, pivot, 1.0), 0.0))
        for i in range(j + 1, 4):
            s = a[i][j]
            for k in range(j):
                s = s - low[i][k] * low[j][k] * piv[k]
            low[i][j] = s * inv[j]
    y = []
    for i in range(4):
        s = m[i]
        for k in range(i):
            s = s - low[i][k] * y[k]
        y.append(s)
    c = [None] * 4
    for i in reversed(range(4)):
        s = y[i] * inv[i]
        for k in range(i + 1, 4):
            s = s - low[k][i] * c[k]
        c[i] = s
    return c


def ocean_kernel(
    u_hbm, v_hbm, t_hbm, p_hbm, depth_hbm, helm_hbm, land_hbm, clinic_hbm, tropic_hbm,
    u_out, v_out, t_out, basis, guess, kept, sums_out,
    uvt, pold, depth, land, cmap, tmap, act, dom,
    ext, pack, pack_t, for_e, for_w, from_w, from_e, tail, got_t, got, corner,
    rim, rim_t, rim_got, rim_m, rim_back, edge, edge_got,
    face, rdiag, gain, diag, flow, turned, part,
    in_sem, send_sem, recv_sem, rsend_sem, rrecv_sem, known, far, *red,
):
    gx, gy = lax.axis_index("gx"), lax.axis_index("gy")
    east, west = lax.rem(gx + 1, NX_DEV), lax.rem(gx + NX_DEV - 1, NX_DEV)
    north, south = lax.rem(gy + 1, NY_DEV), lax.rem(gy + NY_DEV - 1, NY_DEV)
    own = pl.ds(OFF, ROWS)

    loads = [
        pltpu.make_async_copy(u_hbm, uvt.at[0:4, 8 : 8 + ROWS, :], in_sem.at[0]),
        pltpu.make_async_copy(v_hbm, uvt.at[4:8, 8 : 8 + ROWS, :], in_sem.at[1]),
        pltpu.make_async_copy(p_hbm, pold, in_sem.at[2]),
        pltpu.make_async_copy(depth_hbm, depth, in_sem.at[3]),
        pltpu.make_async_copy(land_hbm, land, in_sem.at[4]),
        pltpu.make_async_copy(clinic_hbm, cmap, in_sem.at[5]),
        pltpu.make_async_copy(tropic_hbm, tmap, in_sem.at[6]),
        pltpu.make_async_copy(helm_hbm, ext.at[HELM, 0, OFF : OFF + ROWS, :], in_sem.at[7]),
        pltpu.make_async_copy(t_hbm, uvt.at[8:12, 8 : 8 + ROWS, :], in_sem.at[8]),
    ]
    barrier = pltpu.get_barrier_semaphore()
    has_n, has_s = gy < NY_DEV - 1, gy > 0
    up_x, down_x = gy < NY_DEV - 2, gy > 1

    def greet(sem):
        for ways in (BESIDE, APART):
            for step, there in ((0, None), (1, up_x), (-1, down_x)):

                def tell(step=step, ways=ways):
                    for peer in nearby(step, ways):
                        pl.semaphore_signal(sem, inc=1, device_id=peer, device_id_type=MESH)

                tell() if there is None else pl.when(there)(tell)

    def hear(sem):
        inner = lax.rem((gy // 2 + 1) // 2, 2)
        pl.semaphore_wait(sem, 35 + 18 * inner)

    greet(barrier)
    for load in loads:
        load.start()

    pack[ROWS:, :] = jnp.zeros((pack.shape[0] - ROWS, COLS), F32)
    for load in loads[:8]:
        load.wait()

    shape = (NX_DEV, NBY)
    mine = lax.broadcasted_iota(jnp.int32, shape, 0) == gx
    shape = (BLOCKS, NBY)
    wanted = lax.broadcasted_iota(jnp.int32, shape, 1) == lax.broadcasted_iota(jnp.int32, shape, 0) + gy * BLOCKS

    def per_block(flags):
        line = jnp.sum(jnp.where(mine, flags, 0.0), axis=0, keepdims=True)
        column = jnp.sum(jnp.where(wanted, line, 0.0), axis=1, keepdims=True)
        return jnp.broadcast_to(column, (BLOCKS, COLS))

    act[...] = per_block(cmap[...].astype(F32))
    dom[...] = per_block(jnp.where(tmap[...] >= 0, 1.0, 0.0))

    def coriolis(b):
        row = lax.broadcasted_iota(jnp.int32, (BY, COLS), 0) + (gy * ROWS + b * BY)
        return 0.2 + 0.6 * ((row.astype(F32) + 0.5) / NY)

    group = (lanes(BY) + 8) // 16
    for b in range(BLOCKS):
        r = b * BY
        rows = slice(r, r + BY)
        solve = land[rows, :].astype(F32) * dom[b : b + 1, :]
        wet = depth[rows, :] * solve
        u = [uvt[k, 8 + r : 8 + r + BY, :] for k in range(LEVELS)]
        v = [uvt[LEVELS + k, 8 + r : 8 + r + BY, :] for k in range(LEVELS)]
        u_bar = sum(THICK[k] * u[k] for k in range(LEVELS))
        v_bar = sum(THICK[k] * v[k] for k in range(LEVELS))
        cor = 0.2 * coriolis(b)
        mix = 0.1 * (THICK[1] - THICK[0])
        u_hat = u_bar + mix * (u[0] - u[3]) + cor * v_bar
        v_hat = v_bar + mix * (v[0] - v[3]) - cor * u_bar
        fields = [wet, ext[HELM, 0, OFF + r : OFF + r + BY, :], solve * pold[rows, :], u_bar, u_hat, v_bar, v_hat]
        packed = None
        for f, value in enumerate(fields):
            if f != HELM:
                ext[f, 0, OFF + r : OFF + r + BY, :] = value
            moved = pltpu.roll(value, 16 * f, 1) if f else value
            packed = moved if packed is None else jnp.where(group == f, moved, packed)
        pack[rows, :] = packed
    for c in range(3):
        pack_t[...] = pack[128 * c : 128 * (c + 1), :].T
        e_ref, w_ref = (tail.at[0], tail.at[1]) if c == 2 else (for_e, for_w)
        at_e, at_w = (0, 0) if c == 2 else (EAST_ROWS * c, WEST_ROWS * c)
        for f in range(FIELDS):
            ne, nw = TO_EAST[f], TO_WEST[f]
            e_ref[at_e : at_e + ne, :] = pack_t[(16 * f - 8) % 128 + 8 - ne : (16 * f - 8) % 128 + 8, :]
            w_ref[at_w : at_w + nw, :] = pack_t[16 * f : 16 * f + nw, :]
            at_e, at_w = at_e + ne, at_w + nw
    for i, (ref, whole) in enumerate(((for_e, EAST_ROWS), (for_w, WEST_ROWS))):
        half, size = HALVES[i]
        moved = pltpu.roll(tail[i, half : half + size, :], COLS // 2, 1)
        ref[2 * whole :, :] = jnp.where(lanes(size) < COLS // 2, tail[i, 0:size, :], moved)

    routes = {
        0: (for_e, from_w, (east, gy), None),
        1: (for_w, from_e, (west, gy), None),
        2: (ext.at[:, 0, OFF + ROWS - 8 : OFF + ROWS, :], ext.at[:, 0, LOW:OFF, :], (gx, north), "n"),
        3: (ext.at[:, 0, OFF : OFF + 8, :], ext.at[:, 0, OFF + ROWS : HIGH, :], (gx, south), "s"),
        4: (pack.at[ROWS - 8 : ROWS, :], corner.at[0], (east, north), "n"),
        5: (pack.at[ROWS - 8 : ROWS, :], corner.at[1], (west, north), "n"),
        6: (pack.at[0:8, :], corner.at[2], (east, south), "s"),
        7: (pack.at[0:8, :], corner.at[3], (west, south), "s"),
        8: (rim_t, rim_got.at[0], (east, gy), None),
        9: (rim_t, rim_got.at[1], (west, gy), None),
        10: (edge.at[1], edge_got.at[0], (gx, north), "n"),
        11: (edge.at[0], edge_got.at[1], (gx, south), "s"),
    }
    HALO, OUTER = range(8), range(8, 12)

    def transfer(which, what):
        def go(keys):
            for k in keys:
                src, dst, to, _ = routes[k]
                copy = pltpu.make_async_remote_copy(
                    src_ref=src, dst_ref=dst, send_sem=send_sem.at[k], recv_sem=recv_sem.at[k],
                    device_id=to, device_id_type=MESH,
                )
                getattr(copy, what)()

        go([k for k in which if routes[k][3] is None])
        for way, other in (("n", "s"), ("s", "n")):
            there = {"n": has_n, "s": has_s}[other if what == "wait_recv" else way]
            pl.when(there)(functools.partial(go, [k for k in which if routes[k][3] == way]))

    hear(barrier)
    transfer((4, 5, 6, 7), "start")
    transfer((0, 1), "start")
    transfer((2, 3), "start")
    greet(known)

    loads[8].wait()
    pair = lanes(BY) // 2
    for b in range(BLOCKS):
        r = b * BY
        packed = None
        for q in range(PLANES):
            moved = pltpu.roll(uvt[q, 8 + r : 8 + r + BY, :], 2 * q + 1, 1)
            packed = moved if packed is None else jnp.where(pair == q, moved, packed)
        rim[r : r + BY, :] = packed
    rim[ROWS:, :] = jnp.zeros((rim.shape[0] - ROWS, COLS), F32)
    for c in range(3):
        rim_t[:, 128 * c : 128 * (c + 1)] = rim[128 * c : 128 * (c + 1), :].T[: 2 * PLANES, :]
    for q in range(PLANES):
        edge[0, q : q + 1, :] = uvt[q, 8 : 9, :]
        edge[1, q : q + 1, :] = uvt[q, 7 + ROWS : 8 + ROWS, :]
    def turn(start, size):
        at = slice(start, start + size)
        for i, f in enumerate((WET, UB, VB, X0)):
            value = ext[f, 0, at, :]
            turned[2 * i, at, :] = pltpu.roll(value, COLS - 1, 1)
            if f != X0:
                turned[2 * i + 1, at, :] = pltpu.roll(value, 1, 1)

    for b in range(BLOCKS):
        turn(OFF + b * BY, BY)
    transfer((0, 1), "wait_send")
    transfer(OUTER, "start")
    transfer(HALO, "wait_recv")
    hear(known)

    @pl.when((gy // 2 == 1) | (gy // 2 == 2))
    def _():
        pl.semaphore_signal(
            far, inc=1, device_id=(gx, gy + 4 * lax.rem(gy // 2 - 1, 2) - 2), device_id_type=MESH
        )

    low_half = lax.rem(lanes(8) + 8, 16) < 8
    nothing = jnp.where((lanes(8) + 8) // 16 == HELM, 1.0, 0.0)
    for i, (ref, whole) in enumerate(((from_w, EAST_ROWS), (from_e, WEST_ROWS))):
        half, size = HALVES[i]
        shared = ref[2 * whole :, :]
        tail[i, 0:size, :] = shared
        tail[i, half : half + size, :] = pltpu.roll(shared, COLS // 2, 1)
    for c in range(3):
        w_ref, e_ref = (tail.at[0], tail.at[1]) if c == 2 else (from_w, from_e)
        at_w, at_e = (0, 0) if c == 2 else (EAST_ROWS * c, WEST_ROWS * c)
        for f in range(FIELDS):
            nw, ne = TO_EAST[f], TO_WEST[f]
            got_t[(16 * f - 8) % 128 + 8 - nw : (16 * f - 8) % 128 + 8, :] = w_ref[at_w : at_w + nw, :]
            got_t[16 * f : 16 * f + ne, :] = e_ref[at_e : at_e + ne, :]
            at_w, at_e = at_w + nw, at_e + ne
        block = got_t[...].T
        n = min(128, ROWS - 128 * c)
        got[8 + 128 * c : 8 + 128 * c + n, :] = block[:n, :]
    for k, there, first, halo_at in ((0, has_s, 0, LOW), (2, has_n, 8 + ROWS, OFF + ROWS)):

        @pl.when(there)
        def _(k=k, first=first):
            got[first : first + 8, :] = jnp.where(low_half, corner[k], corner[k + 1])

        @pl.when(jnp.logical_not(there))
        def _(k=k, first=first, halo_at=halo_at):
            got[first : first + 8, :] = nothing
            edge_got[k // 2] = jnp.zeros((16, COLS), F32)
            for f in range(FIELDS):
                ext[f, 0, halo_at : halo_at + 8, :] = jnp.full((8, COLS), 1.0 if f == HELM else 0.0, F32)

    chunks = [(r, STEP) for r in range(LOW, HIGH, STEP)]
    lane = lanes(STEP)
    for r, n in chunks:
        packed = got[r - LOW : r - LOW + n, :]
        for f in range(FIELDS):
            moved = pltpu.roll(packed, COLS - 16 * f, 1) if f else packed
            came = (lane < TO_WEST[f]) | (lane >= COLS - TO_EAST[f])
            ext[f, 1, r : r + n, :] = jnp.where(came, moved, 1.0 if f == HELM else 0.0)

    turn(LOW, 8)
    turn(OFF + ROWS, 8)

    for r, n in chunks:
        at = slice(r, r + n)
        for t, (c, e, w, nn, s) in enumerate(beside(ext.at[WET], r, n, turned.at[0:2])):
            four = [jnp.minimum(c, o) for o in (e, w, nn, s)]
            total = ext[HELM, t, at, :] + four[0] + four[1] + four[2] + four[3]
            inverse = 1.0 / total
            rdiag[t, at, :] = inverse
            if t == 0:
                diag[at, :] = total
            for k in range(4):
                face[k, t, at, :] = four[k]
                gain[k, t, at, :] = four[k] * inverse
    for r, n in chunks:
        at = slice(r, r + n)
        last = lanes(n) == COLS - 1
        x0, x1 = ext[X0, 0, at, :], ext[X0, 1, at, :]
        e0, e1 = turned[6, at, :], pltpu.roll(x1, COLS - 1, 1)
        slope_e = jnp.where(last, e1, e0) - x0, jnp.where(last, e0, e1) - x1
        for t, x in enumerate((x0, x1)):
            guess[t, at, :] = x
            slopes = slope_e[t], ext[X0, t, r + 1 : r + 1 + n, :] - x
            for k, face_at in ((0, 0), (1, 2)):
                flow[k, t, at, :] = face[face_at, t, at, :] * slopes[k]
    for k, (bar, hat) in enumerate(((UB, UH), (VB, VH))):
        for r, n in chunks:
            at = slice(r, r + n)
            for t, (c, *others) in enumerate(beside(ext.at[bar], r, n, turned.at[2 * k + 2 : 2 * k + 4])):
                spread = sum(face[i, t, at, :] * (o - c) for i, o in enumerate(others))
                flow[k, t, at, :] = ext[WET, t, at, :] * (ext[hat, t, at, :] + 0.1 * spread) - flow[k, t, at, :]

    def image(t, at, others):
        return sum(gain[i, t, at, :] * o for i, o in enumerate(others))

    for r, n in chunks:
        at = slice(r, r + n)
        for t, (ef, efw) in enumerate(west_of(flow.at[0], r, n)):
            nf, nfs = flow[1, t, at, :], flow[1, t, r - 1 : r - 1 + n, :]
            residual = (efw - ef) + (nfs - nf) - ext[HELM, t, at, :] * ext[X0, t, at, :]
            basis[0, t, at, :] = jnp.where(ext[WET, t, at, :] > 0.0, residual * rdiag[t, at, :], 0.0)
    for k in range(3):
        for r, n in chunks:
            at = slice(r, r + n)
            for t, (c, *others) in enumerate(beside(basis.at[k], r, n)):
                value = image(t, at, others)
                if k:
                    value = 2.0 * value - basis[k - 1, t, at, :]
                basis[k + 1, t, at, :] = value
    sums = [jnp.zeros((8, COLS), F32) for _ in range(8)]
    for b in range(BLOCKS):
        r = OFF + b * BY
        at = slice(r, r + BY)
        vectors = [basis[k, 0, at, :] for k in range(4)]
        c = vectors[3]
        right = jnp.where(
            lanes(BY) == COLS - 1, pltpu.roll(basis[3, 1, at, :], COLS - 1, 1), pltpu.roll(c, COLS - 1, 1)
        )
        up = basis[3, 0, r + 1 : r + 1 + BY, :]
        for k in range(4):
            weighted = diag[at, :] * vectors[k]
            sums[2 * k] = sums[2 * k] + eights(weighted * vectors[k])
            if k < 3:
                sums[2 * k + 1] = sums[2 * k + 1] + eights(weighted * vectors[k + 1])
        sums[7] = sums[7] + eights(c * (face[0, 0, at, :] * right + face[2, 0, at, :] * up))
    sums[7] = 4.0 * sums[7] - sums[5]

    rows8 = lax.broadcasted_iota(jnp.int32, (8, COLS), 0)
    mat = jnp.zeros((8, COLS), F32)
    for k in range(8):
        mat = jnp.where(rows8 == k, jnp.sum(sums[k], axis=0, keepdims=True), mat)
    total = jnp.broadcast_to(jnp.sum(mat, axis=1, keepdims=True), (8, COLS))
    row = jnp.sum(jnp.where(lanes(8) == rows8, total, 0.0), axis=0, keepdims=True)

    def level_updates():
        transfer(OUTER, "wait_recv")
        even = lax.rem(lax.broadcasted_iota(jnp.int32, (2 * PLANES, COLS), 0), 2) == 0
        for c in range(3):
            cols = slice(128 * c, 128 * (c + 1))
            from_w, from_e = rim_got[0, :, cols], rim_got[1, :, cols]
            up, down = pltpu.roll(from_e, 2 * PLANES - 1, 0), pltpu.roll(from_w, 1, 0)
            rim_m[0 : 2 * PLANES, :] = jnp.where(even, up, down)
            rim_back[128 * c : 128 * (c + 1), :] = rim_m[...].T
        for q in range(PLANES):
            uvt[q, 7:8, :] = edge_got[0, q : q + 1, :]
            uvt[q, 8 + ROWS : 9 + ROWS, :] = edge_got[1, q : q + 1, :]
        first, last = lanes(BY) == 0, lanes(BY) == COLS - 1

        for b in range(BLOCKS):
            r = b * BY
            rows = slice(r, r + BY)
            at = slice(OFF + r, OFF + r + BY)
            on = act[b : b + 1, :]
            ocean = land[rows, :].astype(F32)
            keep = on * ocean
            kept[rows, :] = keep
            off = 1.0 - on
            cor = coriolis(b)
            faces = [face[k, 0, at, :] for k in range(4)]
            rim_row = rim_back[rows, :]

            def around(q):
                c = uvt[q, 8 + r : 8 + r + BY, :]
                side = pltpu.roll(rim_row, COLS - 1 - 2 * q, 1)
                e = jnp.where(last, side, pltpu.roll(c, COLS - 1, 1))
                w = jnp.where(first, side, pltpu.roll(c, 1, 1))
                return c, e, w, uvt[q, 9 + r : 9 + r + BY, :], uvt[q, 7 + r : 7 + r + BY, :]

            def raw(q0):
                out, keepers = [], []
                for k in range(LEVELS):
                    c, *others = around(q0 + k)
                    spread = sum(faces[i] * (o - c) for i, o in enumerate(others))
                    mix = jnp.zeros_like(c)
                    if k < LEVELS - 1:
                        mix = mix + (uvt[q0 + k + 1, 8 + r : 8 + r + BY, :] - c)
                    if k > 0:
                        mix = mix - (c - uvt[q0 + k - 1, 8 + r : 8 + r + BY, :])
                    out.append((c, 0.5 * mix + 0.5 * spread, others))
                return out

            for k, (c, tend, _) in enumerate(raw(0)):
                star = c + 0.2 * (tend + cor * uvt[LEVELS + k, 8 + r : 8 + r + BY, :])
                u_out[k, rows, :] = keep * star + off * c
            for k, (c, tend, _) in enumerate(raw(LEVELS)):
                star = c + 0.2 * (tend - cor * uvt[k, 8 + r : 8 + r + BY, :])
                v_out[k, rows, :] = keep * star + off * c
            for k, (c, tend, (e, w, nn, s)) in enumerate(raw(2 * LEVELS)):
                uk = uvt[k, 8 + r : 8 + r + BY, :]
                vk = uvt[LEVELS + k, 8 + r : 8 + r + BY, :]
                star = c + 0.2 * (tend - 0.5 * (uk * (e - w) + vk * (nn - s)))
                t_out[k, rows, :] = keep * star + off * c

    @pl.when((gy // 2 == 0) | (gy // 2 == 3))
    def _():
        pl.semaphore_wait(far, 1)

    for s, kind in enumerate(RED_STAGES):
        landing = red[s]
        part[s] = row
        for j, peer in enumerate(peers(kind)):
            pltpu.make_async_remote_copy(
                src_ref=part.at[s], dst_ref=landing.at[j], send_sem=rsend_sem.at[s], recv_sem=rrecv_sem.at[s],
                device_id=peer, device_id_type=MESH,
            ).start()
        if s == 0:
            level_updates()
        every = pltpu.make_async_remote_copy(
            src_ref=landing, dst_ref=landing, send_sem=rsend_sem.at[s], recv_sem=rrecv_sem.at[s],
            device_id=(east, gy), device_id_type=MESH,
        )
        every.wait_recv()
        parts = [jnp.sum(landing[j : min(j + 16, COUNT[kind])], axis=0) for j in range(0, COUNT[kind], 16)]
        while len(parts) > 1:
            parts = [sum(parts[j : j + 2]) for j in range(0, len(parts), 2)]
        row = row + parts[0]

    sums_out[...] = row
    transfer(range(2, 12), "wait_send")
    for s in range(len(RED_STAGES)):
        pltpu.make_async_remote_copy(
            src_ref=red[s], dst_ref=red[s], send_sem=rsend_sem.at[s], recv_sem=rrecv_sem.at[s],
            device_id=(east, gy), device_id_type=MESH,
        ).wait_send()


def emit_kernel(u_ref, v_ref, t_ref, basis, guess, kept, sums, u_hbm, v_hbm, t_hbm, p_hbm, u_new, v_new, p_new, sem):
    copies = [pltpu.make_async_copy(t_ref, t_hbm, sem.at[0])]
    copies[0].start()
    row = sums[...]
    c = coefficients([jnp.broadcast_to(row[:, k : k + 1], (1, COLS)) for k in range(8)])

    def answer(t, at):
        x = guess[t, at, :]
        for k in range(4):
            x = x + c[k] * basis[k, t, at, :]
        return x

    last = lanes(EMIT) == COLS - 1
    for b in range(ROWS // EMIT):
        rows = slice(b * EMIT, (b + 1) * EMIT)
        at = slice(OFF + rows.start, OFF + rows.stop)
        x0, x1 = answer(0, at), answer(1, at)
        up = answer(0, slice(at.start + 1, at.stop + 1))
        right = jnp.where(last, pltpu.roll(x1, COLS - 1, 1), pltpu.roll(x0, COLS - 1, 1))
        keep = kept[rows, :]
        p_new[rows, :] = x0
        grad_x, grad_y = keep * (right - x0), keep * (up - x0)
        for k in range(LEVELS):
            u_new[k, rows, :] = u_ref[k, rows, :] - grad_x
            v_new[k, rows, :] = v_ref[k, rows, :] - grad_y
        for i, (src, dst) in enumerate(
            (
                (u_new.at[:, rows, :], u_hbm.at[:, rows, :]),
                (v_new.at[:, rows, :], v_hbm.at[:, rows, :]),
                (p_new.at[rows, :], p_hbm.at[rows, :]),
            )
        ):
            copy = pltpu.make_async_copy(src, dst, sem.at[1 + 3 * b + i])
            copy.start()
            copies.append(copy)
    for copy in copies:
        copy.wait()


def on_device(*args):
    args = args[:7] + (args[7].T, args[8].T)
    args = [pltpu.with_memory_space_constraint(x, pltpu.HBM) for x in args]
    vmem, hbm = pltpu.VMEM, pltpu.HBM
    three = jax.ShapeDtypeStruct((LEVELS, ROWS, COLS), F32)
    two = jax.ShapeDtypeStruct((ROWS, COLS), F32)
    shapes = (three, three, three, two)
    tiles = (2, EXT_ROWS, COLS)
    scratch = [
        vmem((PLANES, ROWS + 16, COLS), F32),
        vmem((ROWS, COLS), F32),
        vmem((ROWS, COLS), F32),
        vmem((ROWS, COLS), jnp.int32),
        vmem((NX_DEV, NBY), jnp.int32),
        vmem((NX_DEV, NBY), jnp.int32),
        vmem((BLOCKS, COLS), F32),
        vmem((BLOCKS, COLS), F32),
        vmem((FIELDS,) + tiles, F32),
        vmem((384, COLS), F32),
        vmem((COLS, COLS), F32),
        vmem((2 * EAST_ROWS + HALVES[0][1], COLS), F32),
        vmem((2 * WEST_ROWS + HALVES[1][1], COLS), F32),
        vmem((2 * EAST_ROWS + HALVES[0][1], COLS), F32),
        vmem((2 * WEST_ROWS + HALVES[1][1], COLS), F32),
        vmem((2, 48, COLS), F32),
        vmem((COLS, COLS), F32),
        vmem((ROWS + 16, COLS), F32),
        vmem((4, 8, COLS), F32),
        vmem((384, COLS), F32),
        vmem((2 * PLANES, 384), F32),
        vmem((2, 2 * PLANES, 384), F32),
        vmem((COLS, COLS), F32),
        vmem((384, COLS), F32),
        vmem((2, 16, COLS), F32),
        vmem((2, 16, COLS), F32),
        vmem((4,) + tiles, F32),
        vmem(tiles, F32),
        vmem((4,) + tiles, F32),
        vmem((EXT_ROWS, COLS), F32),
        vmem((2,) + tiles, F32),
        vmem((7, EXT_ROWS, COLS), F32),
        vmem((len(RED_STAGES), 1, COLS), F32),
        pltpu.SemaphoreType.DMA((9,)),
        pltpu.SemaphoreType.DMA((12,)),
        pltpu.SemaphoreType.DMA((12,)),
        pltpu.SemaphoreType.DMA((len(RED_STAGES),)),
        pltpu.SemaphoreType.DMA((len(RED_STAGES),)),
        pltpu.SemaphoreType.REGULAR,
        pltpu.SemaphoreType.REGULAR,
    ] + [vmem((COUNT[kind], 1, COLS), F32) for kind in RED_STAGES]
    out = pl.pallas_call(
        ocean_kernel,
        out_shape=[vmem(x.shape, F32) for x in (three, three, three)]
        + [vmem((4,) + tiles, F32), vmem(tiles, F32), vmem((ROWS, COLS), F32), vmem((1, COLS), F32)],
        in_specs=[pl.BlockSpec(memory_space=hbm)] * 9,
        out_specs=[pl.BlockSpec(memory_space=vmem)] * 7,
        scratch_shapes=scratch,
        compiler_params=pltpu.CompilerParams(
            collective_id=0, has_side_effects=True, vmem_limit_bytes=VMEM_LIMIT
        ),
        name="ocean",
    )(*args)
    return pl.pallas_call(
        emit_kernel,
        out_shape=shapes,
        in_specs=[pl.BlockSpec(memory_space=vmem)] * 7,
        out_specs=[pl.BlockSpec(memory_space=hbm)] * 4,
        scratch_shapes=[vmem(three.shape, F32), vmem(three.shape, F32), vmem(two.shape, F32)]
        + [pltpu.SemaphoreType.DMA((1 + 3 * (ROWS // EMIT),))],
        compiler_params=pltpu.CompilerParams(vmem_limit_bytes=8 * 1024 * 1024),
        name="emit",
    )(*out)


def solution(mesh):
    wide, flat = P(None, "gy", "gx"), P("gy", "gx")
    return jax.shard_map(
        on_device,
        mesh=mesh,
        in_specs=(wide, wide, wide, flat, flat, flat, flat, P(), P()),
        out_specs=(wide, wide, wide, flat),
        check_vma=False,
    )
```

```python
import functools

import jax
import jax.numpy as jnp
from jax import lax
from jax.experimental import pallas as pl
from jax.experimental.pallas import tpu as pltpu
from jax.sharding import PartitionSpec as P

MESH = pl.DeviceIdType.MESH
F32 = jnp.float32

LEVELS, ROWS, COLS, BY, NY = 4, 320, 128, 40, 2560
BLOCKS, NBY = ROWS // BY, 64
THICK = [(2 * k + 1) / (LEVELS * LEVELS) for k in range(LEVELS)]

OFF = 16
EXT_ROWS = ROWS + 2 * OFF
LOW, HIGH = OFF - 8, OFF + ROWS + 8
STEP = 48
FIELDS = 7
WET, HELM, X0, UB, UH, VB, VH = range(FIELDS)
PLANES = 3 * LEVELS
NX_DEV, NY_DEV = 16, 8

VMEM_LIMIT = 24 * 1024 * 1024
TO_EAST = (6, 4, 5, 6, 5, 5, 4)
TO_WEST = (5, 4, 5, 5, 4, 5, 4)
EAST_ROWS, WEST_ROWS = 40, 32
EMIT = 160
HALVES = ((20, 24), (16, 16))
RED_STAGES = ("all",)


def peers(kind):
    gx, gy = lax.axis_index("gx"), lax.axis_index("gy")
    if kind == "halo":
        return [
            (lax.rem(gx + i, NX_DEV), lax.rem(gy + j, NY_DEV))
            for i in (0, 1, NX_DEV - 1)
            for j in (0, 1, NY_DEV - 1)
            if i or j
        ]
    if kind == "plane":
        base = gx // 4 * 4
        return [
            (base + lax.rem(lax.rem(gx, 4) + i, 4), lax.rem(gy + j, NY_DEV))
            for i in range(4)
            for j in range(NY_DEV)
            if i or j
        ]
    if kind == "z":
        return [(lax.rem(gx + 4 * j, NX_DEV), gy) for j in range(1, 4)]
    return [
        (lax.rem(gx + i, NX_DEV), lax.rem(gy + j, NY_DEV))
        for i in (*range(1, NX_DEV), 0)
        for j in range(NY_DEV)
        if i or j
    ]


BESIDE = ((0, 1), (1, 1), (0, 3), (3, 3), (0, 0))
APART = ((1, 0), (3, 0), (1, 3), (3, 1))


def nearby(step, ways):
    gx, gy = lax.axis_index("gx"), lax.axis_index("gy")
    z, y, core = gx // 4, lax.rem(gx, 4), lax.rem(gy, 2)
    return [
        (lax.rem(z + i, 4) * 4 + lax.rem(y + j, 4), gy + 2 * step if c == 0 else gy + 2 * step + 1 - 2 * core)
        for i, j in ways
        for c in (0, 1)
        if i or j or c or step
    ]


COUNT = {"all": 127, "plane": 31, "z": 3}


def lanes(rows):
    return lax.broadcasted_iota(jnp.int32, (rows, COLS), 1)


def beside(ref, r, n, turned=None):
    lane = lanes(n)
    first, last = lane == 0, lane == COLS - 1
    c0, c1 = ref[0, r : r + n, :], ref[1, r : r + n, :]
    if turned is None:
        e0, w0 = pltpu.roll(c0, COLS - 1, 1), pltpu.roll(c0, 1, 1)
    else:
        e0, w0 = turned[0, r : r + n, :], turned[1, r : r + n, :]
    e1, w1 = pltpu.roll(c1, COLS - 1, 1), pltpu.roll(c1, 1, 1)
    return [
        (
            c,
            jnp.where(last, other_e, own_e),
            jnp.where(first, other_w, own_w),
            ref[t, r + 1 : r + 1 + n, :],
            ref[t, r - 1 : r - 1 + n, :],
        )
        for t, (c, own_e, other_e, own_w, other_w) in enumerate(((c0, e0, e1, w0, w1), (c1, e1, e0, w1, w0)))
    ]


def west_of(ref, r, n):
    first = lanes(n) == 0
    c0, c1 = ref[0, r : r + n, :], ref[1, r : r + n, :]
    w0, w1 = pltpu.roll(c0, 1, 1), pltpu.roll(c1, 1, 1)
    return (c0, jnp.where(first, w1, w0)), (c1, jnp.where(first, w0, w1))


def eights(x):
    return jnp.sum(x.reshape(x.shape[0] // 8, 8, COLS), axis=0)


def coefficients(sums):
    m = [sums[0], sums[1]]
    for k in range(2, 8):
        m.append(2.0 * sums[k] - m[k % 2])
    g = [[0.5 * (m[i + j] + m[abs(i - j)]) for j in range(5) if i + j < 8] for i in range(4)]

    def image(i, j):
        if j == 0:
            return g[i][1]
        return 0.5 * (g[i][j + 1] + g[i][j - 1])

    a = [[g[i][j] - image(i, j) for j in range(i + 1)] for i in range(4)]
    low = [[None] * 4 for _ in range(4)]
    inv, piv = [], []
    for j in range(4):
        pivot = a[j][j]
        for k in range(j):
            pivot = pivot - low[j][k] * low[j][k] * piv[k]
        good = pivot > 1e-6 * a[j][j]
        piv.append(jnp.where(good, pivot, 0.0))
        inv.append(jnp.where(good, 1.0 / jnp.where(good, pivot, 1.0), 0.0))
        for i in range(j + 1, 4):
            s = a[i][j]
            for k in range(j):
                s = s - low[i][k] * low[j][k] * piv[k]
            low[i][j] = s * inv[j]
    y = []
    for i in range(4):
        s = m[i]
        for k in range(i):
            s = s - low[i][k] * y[k]
        y.append(s)
    c = [None] * 4
    for i in reversed(range(4)):
        s = y[i] * inv[i]
        for k in range(i + 1, 4):
            s = s - low[k][i] * c[k]
        c[i] = s
    return c


def ocean_kernel(
    u_hbm, v_hbm, t_hbm, p_hbm, depth_hbm, helm_hbm, land_hbm, clinic_hbm, tropic_hbm,
    u_out, v_out, t_out, basis, guess, kept, sums_out,
    uvt, pold, depth, land, cmap, tmap, act, dom,
    ext, pack, pack_t, for_e, for_w, from_w, from_e, tail, got_t, got, corner,
    rim, rim_t, rim_got, rim_m, rim_back, edge, edge_got,
    face, rdiag, gain, diag, flow, turned, part,
    in_sem, send_sem, recv_sem, rsend_sem, rrecv_sem, known, far, *red,
):
    gx, gy = lax.axis_index("gx"), lax.axis_index("gy")
    east, west = lax.rem(gx + 1, NX_DEV), lax.rem(gx + NX_DEV - 1, NX_DEV)
    north, south = lax.rem(gy + 1, NY_DEV), lax.rem(gy + NY_DEV - 1, NY_DEV)
    own = pl.ds(OFF, ROWS)

    loads = [
        pltpu.make_async_copy(u_hbm, uvt.at[0:4, 8 : 8 + ROWS, :], in_sem.at[0]),
        pltpu.make_async_copy(v_hbm, uvt.at[4:8, 8 : 8 + ROWS, :], in_sem.at[1]),
        pltpu.make_async_copy(p_hbm, pold, in_sem.at[2]),
        pltpu.make_async_copy(depth_hbm, depth, in_sem.at[3]),
        pltpu.make_async_copy(land_hbm, land, in_sem.at[4]),
        pltpu.make_async_copy(clinic_hbm, cmap, in_sem.at[5]),
        pltpu.make_async_copy(tropic_hbm, tmap, in_sem.at[6]),
        pltpu.make_async_copy(helm_hbm, ext.at[HELM, 0, OFF : OFF + ROWS, :], in_sem.at[7]),
        pltpu.make_async_copy(t_hbm, uvt.at[8:12, 8 : 8 + ROWS, :], in_sem.at[8]),
    ]
    barrier = pltpu.get_barrier_semaphore()
    has_n, has_s = gy < NY_DEV - 1, gy > 0
    up_x, down_x = gy < NY_DEV - 2, gy > 1

    def greet(sem):
        for ways in (BESIDE, APART):
            for step, there in ((0, None), (1, up_x), (-1, down_x)):

                def tell(step=step, ways=ways):
                    for peer in nearby(step, ways):
                        pl.semaphore_signal(sem, inc=1, device_id=peer, device_id_type=MESH)

                tell() if there is None else pl.when(there)(tell)

    def hear(sem):
        inner = lax.rem((gy // 2 + 1) // 2, 2)
        pl.semaphore_wait(sem, 35 + 18 * inner)

    greet(barrier)
    for load in loads:
        load.start()

    pack[ROWS:, :] = jnp.zeros((pack.shape[0] - ROWS, COLS), F32)
    for load in loads[:8]:
        load.wait()

    shape = (NX_DEV, NBY)
    mine = lax.broadcasted_iota(jnp.int32, shape, 0) == gx
    shape = (BLOCKS, NBY)
    wanted = lax.broadcasted_iota(jnp.int32, shape, 1) == lax.broadcasted_iota(jnp.int32, shape, 0) + gy * BLOCKS

    def per_block(flags):
        line = jnp.sum(jnp.where(mine, flags, 0.0), axis=0, keepdims=True)
        column = jnp.sum(jnp.where(wanted, line, 0.0), axis=1, keepdims=True)
        return jnp.broadcast_to(column, (BLOCKS, COLS))

    act[...] = per_block(cmap[...].astype(F32))
    dom[...] = per_block(jnp.where(tmap[...] >= 0, 1.0, 0.0))

    def coriolis(b):
        row = lax.broadcasted_iota(jnp.int32, (BY, COLS), 0) + (gy * ROWS + b * BY)
        return 0.2 + 0.6 * ((row.astype(F32) + 0.5) / NY)

    group = (lanes(BY) + 8) // 16
    for b in range(BLOCKS):
        r = b * BY
        rows = slice(r, r + BY)
        solve = land[rows, :].astype(F32) * dom[b : b + 1, :]
        wet = depth[rows, :] * solve
        u = [uvt[k, 8 + r : 8 + r + BY, :] for k in range(LEVELS)]
        v = [uvt[LEVELS + k, 8 + r : 8 + r + BY, :] for k in range(LEVELS)]
        u_bar = sum(THICK[k] * u[k] for k in range(LEVELS))
        v_bar = sum(THICK[k] * v[k] for k in range(LEVELS))
        cor = 0.2 * coriolis(b)
        mix = 0.1 * (THICK[1] - THICK[0])
        u_hat = u_bar + mix * (u[0] - u[3]) + cor * v_bar
        v_hat = v_bar + mix * (v[0] - v[3]) - cor * u_bar
        fields = [wet, ext[HELM, 0, OFF + r : OFF + r + BY, :], solve * pold[rows, :], u_bar, u_hat, v_bar, v_hat]
        packed = None
        for f, value in enumerate(fields):
            if f != HELM:
                ext[f, 0, OFF + r : OFF + r + BY, :] = value
            moved = pltpu.roll(value, 16 * f, 1) if f else value
            packed = moved if packed is None else jnp.where(group == f, moved, packed)
        pack[rows, :] = packed
    for c in range(3):
        pack_t[...] = pack[128 * c : 128 * (c + 1), :].T
        e_ref, w_ref = (tail.at[0], tail.at[1]) if c == 2 else (for_e, for_w)
        at_e, at_w = (0, 0) if c == 2 else (EAST_ROWS * c, WEST_ROWS * c)
        for f in range(FIELDS):
            ne, nw = TO_EAST[f], TO_WEST[f]
            e_ref[at_e : at_e + ne, :] = pack_t[(16 * f - 8) % 128 + 8 - ne : (16 * f - 8) % 128 + 8, :]
            w_ref[at_w : at_w + nw, :] = pack_t[16 * f : 16 * f + nw, :]
            at_e, at_w = at_e + ne, at_w + nw
    for i, (ref, whole) in enumerate(((for_e, EAST_ROWS), (for_w, WEST_ROWS))):
        half, size = HALVES[i]
        moved = pltpu.roll(tail[i, half : half + size, :], COLS // 2, 1)
        ref[2 * whole :, :] = jnp.where(lanes(size) < COLS // 2, tail[i, 0:size, :], moved)

    routes = {
        0: (for_e, from_w, (east, gy), None),
        1: (for_w, from_e, (west, gy), None),
        2: (ext.at[:, 0, OFF + ROWS - 8 : OFF + ROWS, :], ext.at[:, 0, LOW:OFF, :], (gx, north), "n"),
        3: (ext.at[:, 0, OFF : OFF + 8, :], ext.at[:, 0, OFF + ROWS : HIGH, :], (gx, south), "s"),
        4: (pack.at[ROWS - 8 : ROWS, :], corner.at[0], (east, north), "n"),
        5: (pack.at[ROWS - 8 : ROWS, :], corner.at[1], (west, north), "n"),
        6: (pack.at[0:8, :], corner.at[2], (east, south), "s"),
        7: (pack.at[0:8, :], corner.at[3], (west, south), "s"),
        8: (rim_t, rim_got.at[0], (east, gy), None),
        9: (rim_t, rim_got.at[1], (west, gy), None),
        10: (edge.at[1], edge_got.at[0], (gx, north), "n"),
        11: (edge.at[0], edge_got.at[1], (gx, south), "s"),
    }
    HALO, OUTER = range(8), range(8, 12)

    def transfer(which, what):
        def go(keys):
            for k in keys:
                src, dst, to, _ = routes[k]
                copy = pltpu.make_async_remote_copy(
                    src_ref=src, dst_ref=dst, send_sem=send_sem.at[k], recv_sem=recv_sem.at[k],
                    device_id=to, device_id_type=MESH,
                )
                getattr(copy, what)()

        go([k for k in which if routes[k][3] is None])
        for way, other in (("n", "s"), ("s", "n")):
            there = {"n": has_n, "s": has_s}[other if what == "wait_recv" else way]
            pl.when(there)(functools.partial(go, [k for k in which if routes[k][3] == way]))

    hear(barrier)
    transfer((4, 5, 6, 7), "start")
    transfer((0, 1), "start")
    transfer((2, 3), "start")
    greet(known)

    loads[8].wait()
    pair = lanes(BY) // 2
    for b in range(BLOCKS):
        r = b * BY
        packed = None
        for q in range(PLANES):
            moved = pltpu.roll(uvt[q, 8 + r : 8 + r + BY, :], 2 * q + 1, 1)
            packed = moved if packed is None else jnp.where(pair == q, moved, packed)
        rim[r : r + BY, :] = packed
    rim[ROWS:, :] = jnp.zeros((rim.shape[0] - ROWS, COLS), F32)
    for c in range(3):
        rim_t[:, 128 * c : 128 * (c + 1)] = rim[128 * c : 128 * (c + 1), :].T[: 2 * PLANES, :]
    for q in range(PLANES):
        edge[0, q : q + 1, :] = uvt[q, 8 : 9, :]
        edge[1, q : q + 1, :] = uvt[q, 7 + ROWS : 8 + ROWS, :]
    def turn(start, size):
        at = slice(start, start + size)
        for i, f in enumerate((WET, UB, VB, X0)):
            value = ext[f, 0, at, :]
            turned[2 * i, at, :] = pltpu.roll(value, COLS - 1, 1)
            if f != X0:
                turned[2 * i + 1, at, :] = pltpu.roll(value, 1, 1)

    for b in range(BLOCKS):
        turn(OFF + b * BY, BY)
    transfer((0, 1), "wait_send")
    transfer(OUTER, "start")
    transfer(HALO, "wait_recv")
    hear(known)

    @pl.when((gy // 2 == 1) | (gy // 2 == 2))
    def _():
        pl.semaphore_signal(
            far, inc=1, device_id=(gx, gy + 4 * lax.rem(gy // 2 - 1, 2) - 2), device_id_type=MESH
        )

    low_half = lax.rem(lanes(8) + 8, 16) < 8
    nothing = jnp.where((lanes(8) + 8) // 16 == HELM, 1.0, 0.0)
    for i, (ref, whole) in enumerate(((from_w, EAST_ROWS), (from_e, WEST_ROWS))):
        half, size = HALVES[i]
        shared = ref[2 * whole :, :]
        tail[i, 0:size, :] = shared
        tail[i, half : half + size, :] = pltpu.roll(shared, COLS // 2, 1)
    for c in range(3):
        w_ref, e_ref = (tail.at[0], tail.at[1]) if c == 2 else (from_w, from_e)
        at_w, at_e = (0, 0) if c == 2 else (EAST_ROWS * c, WEST_ROWS * c)
        for f in range(FIELDS):
            nw, ne = TO_EAST[f], TO_WEST[f]
            got_t[(16 * f - 8) % 128 + 8 - nw : (16 * f - 8) % 128 + 8, :] = w_ref[at_w : at_w + nw, :]
            got_t[16 * f : 16 * f + ne, :] = e_ref[at_e : at_e + ne, :]
            at_w, at_e = at_w + nw, at_e + ne
        block = got_t[...].T
        n = min(128, ROWS - 128 * c)
        got[8 + 128 * c : 8 + 128 * c + n, :] = block[:n, :]
    for k, there, first, halo_at in ((0, has_s, 0, LOW), (2, has_n, 8 + ROWS, OFF + ROWS)):

        @pl.when(there)
        def _(k=k, first=first):
            got[first : first + 8, :] = jnp.where(low_half, corner[k], corner[k + 1])

        @pl.when(jnp.logical_not(there))
        def _(k=k, first=first, halo_at=halo_at):
            got[first : first + 8, :] = nothing
            edge_got[k // 2] = jnp.zeros((16, COLS), F32)
            for f in range(FIELDS):
                ext[f, 0, halo_at : halo_at + 8, :] = jnp.full((8, COLS), 1.0 if f == HELM else 0.0, F32)

    chunks = [(r, STEP) for r in range(LOW, HIGH, STEP)]
    lane = lanes(STEP)
    for r, n in chunks:
        packed = got[r - LOW : r - LOW + n, :]
        for f in range(FIELDS):
            moved = pltpu.roll(packed, COLS - 16 * f, 1) if f else packed
            came = (lane < TO_WEST[f]) | (lane >= COLS - TO_EAST[f])
            ext[f, 1, r : r + n, :] = jnp.where(came, moved, 1.0 if f == HELM else 0.0)

    turn(LOW, 8)
    turn(OFF + ROWS, 8)

    for r, n in chunks:
        at = slice(r, r + n)
        for t, (c, e, w, nn, s) in enumerate(beside(ext.at[WET], r, n, turned.at[0:2])):
            four = [jnp.minimum(c, o) for o in (e, w, nn, s)]
            total = ext[HELM, t, at, :] + four[0] + four[1] + four[2] + four[3]
            inverse = 1.0 / total
            rdiag[t, at, :] = inverse
            if t == 0:
                diag[at, :] = total
            for k in range(4):
                face[k, t, at, :] = four[k]
                gain[k, t, at, :] = four[k] * inverse
    for r, n in chunks:
        at = slice(r, r + n)
        last = lanes(n) == COLS - 1
        x0, x1 = ext[X0, 0, at, :], ext[X0, 1, at, :]
        e0, e1 = turned[6, at, :], pltpu.roll(x1, COLS - 1, 1)
        slope_e = jnp.where(last, e1, e0) - x0, jnp.where(last, e0, e1) - x1
        for t, x in enumerate((x0, x1)):
            guess[t, at, :] = x
            slopes = slope_e[t], ext[X0, t, r + 1 : r + 1 + n, :] - x
            for k, face_at in ((0, 0), (1, 2)):
                flow[k, t, at, :] = face[face_at, t, at, :] * slopes[k]
    for k, (bar, hat) in enumerate(((UB, UH), (VB, VH))):
        for r, n in chunks:
            at = slice(r, r + n)
            for t, (c, *others) in enumerate(beside(ext.at[bar], r, n, turned.at[2 * k + 2 : 2 * k + 4])):
                spread = sum(face[i, t, at, :] * (o - c) for i, o in enumerate(others))
                flow[k, t, at, :] = ext[WET, t, at, :] * (ext[hat, t, at, :] + 0.1 * spread) - flow[k, t, at, :]

    def image(t, at, others):
        return sum(gain[i, t, at, :] * o for i, o in enumerate(others))

    for r, n in chunks:
        at = slice(r, r + n)
        for t, (ef, efw) in enumerate(west_of(flow.at[0], r, n)):
            nf, nfs = flow[1, t, at, :], flow[1, t, r - 1 : r - 1 + n, :]
            residual = (efw - ef) + (nfs - nf) - ext[HELM, t, at, :] * ext[X0, t, at, :]
            basis[0, t, at, :] = jnp.where(ext[WET, t, at, :] > 0.0, residual * rdiag[t, at, :], 0.0)
    for k in range(3):
        for r, n in chunks:
            at = slice(r, r + n)
            for t, (c, *others) in enumerate(beside(basis.at[k], r, n)):
                value = image(t, at, others)
                if k:
                    value = 2.0 * value - basis[k - 1, t, at, :]
                basis[k + 1, t, at, :] = value
    sums = [jnp.zeros((8, COLS), F32) for _ in range(8)]
    for b in range(BLOCKS):
        r = OFF + b * BY
        at = slice(r, r + BY)
        vectors = [basis[k, 0, at, :] for k in range(4)]
        c = vectors[3]
        right = jnp.where(
            lanes(BY) == COLS - 1, pltpu.roll(basis[3, 1, at, :], COLS - 1, 1), pltpu.roll(c, COLS - 1, 1)
        )
        up = basis[3, 0, r + 1 : r + 1 + BY, :]
        for k in range(4):
            weighted = diag[at, :] * vectors[k]
            sums[2 * k] = sums[2 * k] + eights(weighted * vectors[k])
            if k < 3:
                sums[2 * k + 1] = sums[2 * k + 1] + eights(weighted * vectors[k + 1])
        sums[7] = sums[7] + eights(c * (face[0, 0, at, :] * right + face[2, 0, at, :] * up))
    sums[7] = 4.0 * sums[7] - sums[5]

    rows8 = lax.broadcasted_iota(jnp.int32, (8, COLS), 0)
    mat = jnp.zeros((8, COLS), F32)
    for k in range(8):
        mat = jnp.where(rows8 == k, jnp.sum(sums[k], axis=0, keepdims=True), mat)
    total = jnp.broadcast_to(jnp.sum(mat, axis=1, keepdims=True), (8, COLS))
    row = jnp.sum(jnp.where(lanes(8) == rows8, total, 0.0), axis=0, keepdims=True)

    def level_updates():
        transfer(OUTER, "wait_recv")
        even = lax.rem(lax.broadcasted_iota(jnp.int32, (2 * PLANES, COLS), 0), 2) == 0
        for c in range(3):
            cols = slice(128 * c, 128 * (c + 1))
            from_w, from_e = rim_got[0, :, cols], rim_got[1, :, cols]
            up, down = pltpu.roll(from_e, 2 * PLANES - 1, 0), pltpu.roll(from_w, 1, 0)
            rim_m[0 : 2 * PLANES, :] = jnp.where(even, up, down)
            rim_back[128 * c : 128 * (c + 1), :] = rim_m[...].T
        for q in range(PLANES):
            uvt[q, 7:8, :] = edge_got[0, q : q + 1, :]
            uvt[q, 8 + ROWS : 9 + ROWS, :] = edge_got[1, q : q + 1, :]
        first, last = lanes(BY) == 0, lanes(BY) == COLS - 1

        for b in range(BLOCKS):
            r = b * BY
            rows = slice(r, r + BY)
            at = slice(OFF + r, OFF + r + BY)
            on = act[b : b + 1, :]
            ocean = land[rows, :].astype(F32)
            keep = on * ocean
            kept[rows, :] = keep
            off = 1.0 - on
            cor = coriolis(b)
            faces = [face[k, 0, at, :] for k in range(4)]
            rim_row = rim_back[rows, :]

            def around(q):
                c = uvt[q, 8 + r : 8 + r + BY, :]
                side = pltpu.roll(rim_row, COLS - 1 - 2 * q, 1)
                e = jnp.where(last, side, pltpu.roll(c, COLS - 1, 1))
                w = jnp.where(first, side, pltpu.roll(c, 1, 1))
                return c, e, w, uvt[q, 9 + r : 9 + r + BY, :], uvt[q, 7 + r : 7 + r + BY, :]

            def raw(q0):
                out, keepers = [], []
                for k in range(LEVELS):
                    c, *others = around(q0 + k)
                    spread = sum(faces[i] * (o - c) for i, o in enumerate(others))
                    mix = jnp.zeros_like(c)
                    if k < LEVELS - 1:
                        mix = mix + (uvt[q0 + k + 1, 8 + r : 8 + r + BY, :] - c)
                    if k > 0:
                        mix = mix - (c - uvt[q0 + k - 1, 8 + r : 8 + r + BY, :])
                    out.append((c, 0.5 * mix + 0.5 * spread, others))
                return out

            for k, (c, tend, _) in enumerate(raw(0)):
                star = c + 0.2 * (tend + cor * uvt[LEVELS + k, 8 + r : 8 + r + BY, :])
                u_out[k, rows, :] = keep * star + off * c
            for k, (c, tend, _) in enumerate(raw(LEVELS)):
                star = c + 0.2 * (tend - cor * uvt[k, 8 + r : 8 + r + BY, :])
                v_out[k, rows, :] = keep * star + off * c
            for k, (c, tend, (e, w, nn, s)) in enumerate(raw(2 * LEVELS)):
                uk = uvt[k, 8 + r : 8 + r + BY, :]
                vk = uvt[LEVELS + k, 8 + r : 8 + r + BY, :]
                star = c + 0.2 * (tend - 0.5 * (uk * (e - w) + vk * (nn - s)))
                t_out[k, rows, :] = keep * star + off * c

    @pl.when((gy // 2 == 0) | (gy // 2 == 3))
    def _():
        pl.semaphore_wait(far, 1)

    for s, kind in enumerate(RED_STAGES):
        landing = red[s]
        part[s] = row
        for j, peer in enumerate(peers(kind)):
            pltpu.make_async_remote_copy(
                src_ref=part.at[s], dst_ref=landing.at[j], send_sem=rsend_sem.at[s], recv_sem=rrecv_sem.at[s],
                device_id=peer, device_id_type=MESH,
            ).start()
        if s == 0:
            level_updates()
        every = pltpu.make_async_remote_copy(
            src_ref=landing, dst_ref=landing, send_sem=rsend_sem.at[s], recv_sem=rrecv_sem.at[s],
            device_id=(east, gy), device_id_type=MESH,
        )
        every.wait_recv()
        parts = [jnp.sum(landing[j : min(j + 16, COUNT[kind])], axis=0) for j in range(0, COUNT[kind], 16)]
        while len(parts) > 1:
            parts = [sum(parts[j : j + 2]) for j in range(0, len(parts), 2)]
        row = row + parts[0]

    sums_out[...] = row
    transfer(range(2, 12), "wait_send")
    for s in range(len(RED_STAGES)):
        pltpu.make_async_remote_copy(
            src_ref=red[s], dst_ref=red[s], send_sem=rsend_sem.at[s], recv_sem=rrecv_sem.at[s],
            device_id=(east, gy), device_id_type=MESH,
        ).wait_send()


def emit_kernel(u_ref, v_ref, t_ref, basis, guess, kept, sums, u_hbm, v_hbm, t_hbm, p_hbm, u_new, v_new, p_new, sem):
    copies = [pltpu.make_async_copy(t_ref, t_hbm, sem.at[0])]
    copies[0].start()
    row = sums[...]
    c = coefficients([jnp.broadcast_to(row[:, k : k + 1], (1, COLS)) for k in range(8)])

    def answer(t, at):
        x = guess[t, at, :]
        for k in range(4):
            x = x + c[k] * basis[k, t, at, :]
        return x

    last = lanes(EMIT) == COLS - 1
    for b in range(ROWS // EMIT):
        rows = slice(b * EMIT, (b + 1) * EMIT)
        at = slice(OFF + rows.start, OFF + rows.stop)
        x0, x1 = answer(0, at), answer(1, at)
        up = answer(0, slice(at.start + 1, at.stop + 1))
        right = jnp.where(last, pltpu.roll(x1, COLS - 1, 1), pltpu.roll(x0, COLS - 1, 1))
        keep = kept[rows, :]
        p_new[rows, :] = x0
        grad_x, grad_y = keep * (right - x0), keep * (up - x0)
        for k in range(LEVELS):
            u_new[k, rows, :] = u_ref[k, rows, :] - grad_x
            v_new[k, rows, :] = v_ref[k, rows, :] - grad_y
        for i, (src, dst) in enumerate(
            (
                (u_new.at[:, rows, :], u_hbm.at[:, rows, :]),
                (v_new.at[:, rows, :], v_hbm.at[:, rows, :]),
                (p_new.at[rows, :], p_hbm.at[rows, :]),
            )
        ):
            copy = pltpu.make_async_copy(src, dst, sem.at[1 + 3 * b + i])
            copy.start()
            copies.append(copy)
    for copy in copies:
        copy.wait()


def on_device(*args):
    args = args[:7] + (args[7].T, args[8].T)
    args = [pltpu.with_memory_space_constraint(x, pltpu.HBM) for x in args]
    vmem, hbm = pltpu.VMEM, pltpu.HBM
    three = jax.ShapeDtypeStruct((LEVELS, ROWS, COLS), F32)
    two = jax.ShapeDtypeStruct((ROWS, COLS), F32)
    shapes = (three, three, three, two)
    tiles = (2, EXT_ROWS, COLS)
    scratch = [
        vmem((PLANES, ROWS + 16, COLS), F32),
        vmem((ROWS, COLS), F32),
        vmem((ROWS, COLS), F32),
        vmem((ROWS, COLS), jnp.int32),
        vmem((NX_DEV, NBY), jnp.int32),
        vmem((NX_DEV, NBY), jnp.int32),
        vmem((BLOCKS, COLS), F32),
        vmem((BLOCKS, COLS), F32),
        vmem((FIELDS,) + tiles, F32),
        vmem((384, COLS), F32),
        vmem((COLS, COLS), F32),
        vmem((2 * EAST_ROWS + HALVES[0][1], COLS), F32),
        vmem((2 * WEST_ROWS + HALVES[1][1], COLS), F32),
        vmem((2 * EAST_ROWS + HALVES[0][1], COLS), F32),
        vmem((2 * WEST_ROWS + HALVES[1][1], COLS), F32),
        vmem((2, 48, COLS), F32),
        vmem((COLS, COLS), F32),
        vmem((ROWS + 16, COLS), F32),
        vmem((4, 8, COLS), F32),
        vmem((384, COLS), F32),
        vmem((2 * PLANES, 384), F32),
        vmem((2, 2 * PLANES, 384), F32),
        vmem((COLS, COLS), F32),
        vmem((384, COLS), F32),
        vmem((2, 16, COLS), F32),
        vmem((2, 16, COLS), F32),
        vmem((4,) + tiles, F32),
        vmem(tiles, F32),
        vmem((4,) + tiles, F32),
        vmem((EXT_ROWS, COLS), F32),
        vmem((2,) + tiles, F32),
        vmem((7, EXT_ROWS, COLS), F32),
        vmem((len(RED_STAGES), 1, COLS), F32),
        pltpu.SemaphoreType.DMA((9,)),
        pltpu.SemaphoreType.DMA((12,)),
        pltpu.SemaphoreType.DMA((12,)),
        pltpu.SemaphoreType.DMA((len(RED_STAGES),)),
        pltpu.SemaphoreType.DMA((len(RED_STAGES),)),
        pltpu.SemaphoreType.REGULAR,
        pltpu.SemaphoreType.REGULAR,
    ] + [vmem((COUNT[kind], 1, COLS), F32) for kind in RED_STAGES]
    out = pl.pallas_call(
        ocean_kernel,
        out_shape=[vmem(x.shape, F32) for x in (three, three, three)]
        + [vmem((4,) + tiles, F32), vmem(tiles, F32), vmem((ROWS, COLS), F32), vmem((1, COLS), F32)],
        in_specs=[pl.BlockSpec(memory_space=hbm)] * 9,
        out_specs=[pl.BlockSpec(memory_space=vmem)] * 7,
        scratch_shapes=scratch,
        compiler_params=pltpu.CompilerParams(
            collective_id=0, has_side_effects=True, vmem_limit_bytes=VMEM_LIMIT
        ),
        name="ocean",
    )(*args)
    return pl.pallas_call(
        emit_kernel,
        out_shape=shapes,
        in_specs=[pl.BlockSpec(memory_space=vmem)] * 7,
        out_specs=[pl.BlockSpec(memory_space=hbm)] * 4,
        scratch_shapes=[vmem(three.shape, F32), vmem(three.shape, F32), vmem(two.shape, F32)]
        + [pltpu.SemaphoreType.DMA((1 + 3 * (ROWS // EMIT),))],
        compiler_params=pltpu.CompilerParams(vmem_limit_bytes=8 * 1024 * 1024),
        name="emit",
    )(*out)


def solution(mesh):
    wide, flat = P(None, "gy", "gx"), P("gy", "gx")
    return jax.shard_map(
        on_device,
        mesh=mesh,
        in_specs=(wide, wide, wide, flat, flat, flat, flat, P(), P()),
        out_specs=(wide, wide, wide, flat),
        check_vma=False,
    )
```
